32 devices in a mesh: rows: 8 (over z, x), ka: 4 (over y, core).
Axes of the slice: x: 2, y: 2, z: 4, core: 2. Of those that a mesh axis runs over, the one named last changes fastest.
Arguments:
- pair_repr: bfloat16 [512, 512, 128], P('rows', 'ka'), may hold values from -6 to 6
- pair_mask: int32 [512, 512], P('rows', 'ka'), may hold values 0 or 1
- ln_gain: float32 [128], replicated, may hold values from 0.1 to 1.9
- ln_bias: float32 [128], replicated, may hold values from -3 to 3
- w_proj: bfloat16 [128, 256], replicated, may hold values from -0.5 to 0.5
- w_gate: bfloat16 [128, 256], replicated, may hold values from -0.5 to 0.5
- w_out_gate: bfloat16 [128, 128], replicated, may hold values from -0.5 to 0.5
- out_gain: float32 [128], replicated, may hold values from 0.1 to 1.9
- out_bias: float32 [128], replicated, may hold values from -3 to 3
- w_out: bfloat16 [128, 128], replicated, may hold values from -0.5 to 0.5
Outputs:
- update: bfloat16 [512, 512, 128], P('rows', 'ka')
The draws below stay inside these ranges and needn't reach their ends.
All inputs are finite; a program needn't handle non-finite values. No bound on the sum of `pair_mask` on one device may be relied on, other than what follows from the above.
Results may differ from the reference program's by a relative error of at most 0.015.
Values may be sent and summed in bfloat16 or wider, within the bound.
A program may use at most 64 MiB of HBM per device.

```python
import jax
import jax.numpy as jnp
from jax import lax

C = 128
H = 128
N = 512


def place_ends(drawn, own_key, smallest, high):
    spot = [jax.random.randint(jax.random.fold_in(own_key, axis), (), 0, length) for axis, length in enumerate(drawn.shape)]
    widest = drawn.shape.index(max(drawn.shape))
    beside = spot[:widest] + [(spot[widest] + 1) % drawn.shape[widest]] + spot[widest + 1:]
    return drawn.at[tuple(spot)].set(smallest).at[tuple(beside)].set(high)


def shard_levels(own_key, extent, shards, least, high):
    def one(position, parts):
        steps = jax.random.uniform(jax.random.fold_in(jax.random.fold_in(own_key, 6), position), (parts,), jnp.float32, least / len(shards), high / len(shards))
        return jnp.repeat(jnp.exp(steps), extent[position] // parts).reshape((-1,) + (1,) * (len(extent) - position - 1))

    loudness = one(*shards[0])
    for cut in shards[1:]:
        loudness = loudness * one(*cut)
    return loudness


def bell_draw(key, dims, deviation, reach, shards=(), held_as=jnp.bfloat16):
    array = jax.random.normal(key, dims, jnp.float32) * deviation
    if len(shards) > 0:
        array = shard_levels(key, dims, shards, -0.22, 0.18) * array
    return jnp.clip(array, min=-reach, max=reach).astype(held_as)


def setup_inputs(seed: int = 0) -> dict:
    seeds = jax.random.split(jax.random.key(seed), 11)
    pair_repr = bell_draw(seeds[0], (N, N, C), 1.0, 6.0, ((0, 8), (1, 4)))
    pair_mask = place_ends((jax.random.randint(seeds[1], (N, N), 0, 4) < 3).astype(jnp.int32), jax.random.fold_in(seeds[1], 1), 0, 1)
    ln_gain = jnp.clip(1.0 + 0.18 * jax.random.normal(seeds[2], (C,), jnp.float32), 0.1, 1.9)
    ln_bias = bell_draw(seeds[3], (C,), 0.5, 3.0, (), jnp.float32)
    w_proj = bell_draw(seeds[4], (C, 2 * H), C ** -0.5, 0.5)
    w_gate = bell_draw(seeds[5], (C, 2 * H), C ** -0.5, 0.5)
    w_out_gate = bell_draw(seeds[6], (C, C), C ** -0.5, 0.5)
    out_gain = jnp.clip(1.0 + 0.18 * jax.random.normal(seeds[7], (H,), jnp.float32), 0.1, 1.9)
    out_bias = bell_draw(seeds[8], (H,), 0.5, 3.0, (), jnp.float32)
    w_out = bell_draw(seeds[9], (H, C), H ** -0.5, 0.5)
    return dict(pair_repr=pair_repr, pair_mask=pair_mask, ln_gain=ln_gain, ln_bias=ln_bias, w_proj=w_proj, w_gate=w_gate, w_out_gate=w_out_gate, out_gain=out_gain, out_bias=out_bias, w_out=w_out)


def layer_norm(values, gain_vec, bias_vec):
    center = lax.optimization_barrier(jnp.mean(values, axis=-1, keepdims=True))
    deviate = values - center
    spread = lax.optimization_barrier(jnp.mean(deviate * deviate, axis=-1, keepdims=True))
    return deviate * lax.rsqrt(spread + 1e-05) * gain_vec + bias_vec

def reference(pair_repr, pair_mask, ln_gain, ln_bias, w_proj, w_gate, w_out_gate, out_gain, out_bias, w_out):
    normed = layer_norm(pair_repr.astype(jnp.float32), ln_gain, ln_bias).astype(jnp.bfloat16)
    flat_rows = normed.reshape(N * N, C)
    projected = jnp.dot(flat_rows, w_proj, preferred_element_type=jnp.float32)
    gate_logits = jnp.dot(flat_rows, w_gate, preferred_element_type=jnp.float32)
    mask_col = pair_mask.reshape(N * N, 1).astype(jnp.float32)
    edges = (jax.nn.sigmoid(gate_logits) * projected * mask_col).astype(jnp.bfloat16).reshape(N, N, 2 * H)
    left_edge = jnp.transpose(edges[:, :, :H], (2, 0, 1)).astype(jnp.float32)
    right_edge = jnp.transpose(edges[:, :, H:], (2, 1, 0)).astype(jnp.float32)
    triangle = jnp.transpose(jnp.matmul(left_edge, right_edge), (1, 2, 0))
    tri_normed = layer_norm(triangle, out_gain, out_bias).astype(jnp.bfloat16)
    out_gate = jax.nn.sigmoid(jnp.dot(flat_rows, w_out_gate, preferred_element_type=jnp.float32))
    projected_out = jnp.dot(tri_normed.reshape(N * N, H), w_out, preferred_element_type=jnp.float32)
    return (out_gate * projected_out).astype(jnp.bfloat16).reshape(N, N, C)
```

```python
import functools

import jax
import jax.numpy as jnp
from jax import lax
from jax.experimental import pallas as pl
from jax.experimental.pallas import tpu as pltpu
from jax.sharding import PartitionSpec as P

MESH = pl.DeviceIdType.MESH
CHUNK = 16
PITCH = 24
EARLY = 2
MAKE_UNROLL = 8
GATE_UNROLL = 8
FINISH_UNROLL = 16


def layer_norm(values, gain_vec, bias_vec):
    center = jnp.mean(values, axis=-1, keepdims=True)
    deviate = values - center
    spread = jnp.mean(deviate * deviate, axis=-1, keepdims=True)
    return deviate * lax.rsqrt(spread + 1e-05) * gain_vec + bias_vec


def sigmoid(logits):
    return 0.5 + 0.5 * jnp.tanh(0.5 * logits)


def kernel(
    rows_n, ka_n, early,
    pair_hbm, mask_ref, ln_gain_ref, ln_bias_ref, w_proj_ref, w_gate_ref, w_out_gate_ref,
    out_gain_ref, out_bias_ref, w_out_ref,
    out_hbm,
    pair_ref, out_ref, edges, wide, normed, gates, left, right, tri, back, w_cat, gain_col, bias_col,
    load_sem, store_sem, recv_left, recv_early, recv_right, recv_far, recv_tri,
    send_left, send_right, send_far, send_tri,
):
    row = lax.axis_index("rows")
    col = lax.axis_index("ka")
    row_count, col_count, chans = pair_ref.shape
    hidden = w_out_ref.shape[0]
    zone = rows_n // 4
    group_rows = 2 * zone
    members = group_rows * ka_n
    hubs = zone * ka_n
    share = hidden // hubs
    late = share - early
    chunks = row_count // CHUNK

    quarter = row // zone
    lane = row % zone
    half = quarter // 2
    spot = row % group_rows
    hub_q = 1 + half
    far_q = 2 - half
    edge_q = 3 * half
    place = half * (quarter - 2) + (1 - half) * (1 - quarter)
    inner = place == 0
    member = lane * ka_n + col
    planes = wide.reshape(2 * hidden, PITCH, col_count)

    def chunk_rows(chunk):
        return pl.ds(pl.multiple_of(chunk * CHUNK, CHUNK), CHUNK)

    def load(chunk):
        rows = chunk_rows(chunk)
        return pltpu.make_async_copy(pair_hbm.at[rows], pair_ref.at[rows], load_sem.at[chunk])

    for chunk in range(chunks):
        load(chunk).start()

    barrier = pltpu.get_barrier_semaphore()

    def greet(step, carry):
        to_row = (row + step // ka_n) % rows_n
        to_col = (col + step % ka_n) % ka_n
        pl.semaphore_signal(barrier, inc=1, device_id=(to_row, to_col), device_id_type=MESH)
        return carry

    lax.fori_loop(1, rows_n * ka_n, greet, 0)

    def turned(ref):
        return ref[...].astype(jnp.float32).T.astype(jnp.bfloat16)

    w_cat[: 2 * hidden, :] = turned(w_gate_ref)
    w_cat[2 * hidden :, :] = turned(w_proj_ref)

    own_cols = pl.ds(pl.multiple_of(col * col_count, 128), col_count)

    def left_ends(chan, count, first, size, to_member):
        return (
            edges.at[pl.ds(to_member * share + chan, count), pl.ds(first, size), :],
            left.at[pl.ds(chan, count), pl.ds(spot * row_count + first, size), own_cols],
        )

    def right_ends(chan, count, first, size, to_member):
        return (
            edges.at[pl.ds(hidden + to_member * share + chan, count), pl.ds(first, size), :],
            right.at[pl.ds(chan, count), pl.ds(row * row_count + first, size), own_cols],
        )

    def send_edges(ends, chan, count, first, size, sent, landed):
        def start(to_lane, to_col):
            here, there = ends(chan, count, first, size, to_lane * ka_n + to_col)
            pltpu.make_async_remote_copy(
                src_ref=here, dst_ref=there, send_sem=sent, recv_sem=landed,
                device_id=(quarter * zone + to_lane, to_col), device_id_type=MESH,
            ).start()

        def other(step, carry):
            start((lane + step % zone) % zone, (col + step // zone) % ka_n)
            return carry

        lax.fori_loop(1, hubs, other, 0)
        here, there = ends(chan, count, first, size, member)
        pltpu.make_async_copy(here, there, landed).start()

    def make_chunk(chunk):
        load(chunk).wait()

        def one_row(local, carry):
            at = chunk * CHUNK + local
            values = pair_ref[at].astype(jnp.float32)
            plain = layer_norm(values, ln_gain_ref[...], ln_bias_ref[...]).astype(jnp.bfloat16)
            normed[at] = plain
            both = lax.dot_general(
                w_cat[...], plain, (((1,), (1,)), ((), ())), preferred_element_type=jnp.float32
            )
            mask_row = mask_ref[pl.ds(at, 1), :].astype(jnp.float32)
            made = sigmoid(both[: 2 * hidden]) * both[2 * hidden :] * mask_row
            wide[pl.ds(local, 2 * hidden, stride=PITCH), :] = made
            return carry

        lax.fori_loop(0, CHUNK, one_row, 0, unroll=MAKE_UNROLL)
        edges[:, chunk_rows(chunk), :] = planes[:, :CHUNK, :].astype(jnp.bfloat16)

    def send_early(chunk):
        first = pl.multiple_of(chunk * CHUNK, CHUNK)
        send_edges(right_ends, 0, early, first, CHUNK, send_right, recv_early.at[0, chunk])
        send_edges(left_ends, 0, early, first, CHUNK, send_left, recv_left.at[0, 0])

    def send_late(group, carry):
        chan = early + group
        send_edges(right_ends, chan, 1, 0, row_count, send_right, recv_right.at[0, group])
        send_edges(left_ends, chan, 1, 0, row_count, send_left, recv_left.at[0, 1 + group])
        return carry

    def await_part(part, landed):
        pltpu.make_async_copy(part, part, landed).wait()

    def pass_on(part, to_q, landed):
        pltpu.make_async_remote_copy(
            src_ref=part, dst_ref=part, send_sem=send_far, recv_sem=landed,
            device_id=(to_q * zone + lane, col), device_id_type=MESH,
        ).start()

    def right_rows(chan, count, first, size):
        return right.at[pl.ds(chan, count), pl.ds(pl.multiple_of(first, CHUNK), size), :]

    def left_rows(chan, count, from_q):
        first = pl.multiple_of(from_q % 2 * zone * row_count, CHUNK)
        return left.at[pl.ds(chan, count), pl.ds(first, zone * row_count), :]

    def pass_early(from_q, chunk, to_q, came, landed):
        await_part(right_rows(0, early, 0, zone * CHUNK), came)
        for to_lane in range(zone):
            first = (from_q * zone + to_lane) * row_count + chunk * CHUNK
            pass_on(right_rows(0, early, first, CHUNK), to_q, landed)

    def pass_late(from_q, group, to_q, came, landed):
        part = right_rows(early + group, 1, from_q * zone * row_count, zone * row_count)
        await_part(part, came)
        pass_on(part, to_q, landed)

    def pass_left(chan, count, group):
        part = left_rows(chan, count, quarter)
        await_part(part, recv_left.at[0, group])
        pass_on(part, hub_q, recv_left.at[1, group])

    def pass_first(chunk):
        @pl.when(inner)
        def _():
            pass_early(quarter, chunk, far_q, recv_early.at[0, chunk], recv_far.at[0])

        @pl.when(place == 1)
        def _():
            pass_early(quarter, chunk, hub_q, recv_early.at[0, chunk], recv_early.at[1, chunk])

    def cross_near(group):
        pass_late(hub_q, group, far_q, recv_right.at[0, group], recv_far.at[1 + group])

    def cross_edge(group):
        pass_late(edge_q, group, far_q, recv_right.at[1, group], recv_far.at[1 + group])

    def climb(group, carry):
        pass_late(edge_q, group, hub_q, recv_right.at[0, group], recv_right.at[1, group])
        pass_left(early + group, 1, 1 + group)
        return carry

    def triangle(chan, count, group):
        await_part(left_rows(chan, count, hub_q), recv_left.at[0, group])
        await_part(left_rows(chan, count, edge_q), recv_left.at[1, group])
        await_part(right_rows(chan, count, 0, group_rows * row_count), recv_far.at[group])

        def one_channel(at, carry):
            tri[at] = lax.dot_general(
                left[at], right[at], (((1,), (1,)), ((), ())), preferred_element_type=jnp.float32
            ).astype(jnp.bfloat16)
            return carry

        lax.fori_loop(chan, chan + count, one_channel, 0)
        slot = back.at[pl.ds(member * share + chan, count)]

        def tri_part(to_spot, to_col):
            return tri.at[
                pl.ds(chan, count),
                pl.ds(pl.multiple_of(to_spot * row_count, CHUNK), row_count),
                pl.ds(pl.multiple_of(to_col * col_count, 128), col_count),
            ]

        def give(step, carry):
            to_spot, to_col = (spot + step % group_rows) % group_rows, (col + step // group_rows) % ka_n
            pltpu.make_async_remote_copy(
                src_ref=tri_part(to_spot, to_col), dst_ref=slot,
                send_sem=send_tri, recv_sem=recv_tri,
                device_id=(half * group_rows + to_spot, to_col), device_id_type=MESH,
            ).start()
            return carry

        lax.fori_loop(1, members, give, 0)
        pltpu.make_async_copy(tri_part(spot, col), slot, recv_tri).start()

    make_chunk(0)
    pl.semaphore_wait(barrier, rows_n * ka_n - 1)
    send_early(0)

    def rest(chunk, carry):
        make_chunk(chunk)
        send_early(chunk)
        pass_first(chunk - 1)
        return carry

    lax.fori_loop(1, chunks, rest, 0)
    pass_first(chunks - 1)

    @pl.when(place == 1)
    def _():
        pass_left(0, early, 0)

    lax.fori_loop(0, late, send_late, 0)

    @pl.when(inner)
    def _():
        for chunk in range(chunks):
            pass_early(edge_q, chunk, far_q, recv_early.at[1, chunk], recv_far.at[0])
        cross_near(0)
        cross_near(1)

    @pl.when(place == 1)
    def _():
        climb(0, 0)
        climb(1, 0)

    gain_col[...] = jnp.broadcast_to(out_gain_ref[...], (col_count, hidden)).T
    bias_col[...] = jnp.broadcast_to(out_bias_ref[...], (col_count, hidden)).T

    def gate_row(at, carry):
        gates[at] = sigmoid(
            jnp.dot(normed[at], w_out_gate_ref[...], preferred_element_type=jnp.float32)
        )
        return carry

    lax.fori_loop(0, row_count, gate_row, 0, unroll=GATE_UNROLL)

    @pl.when(place == 1)
    def _():
        lax.fori_loop(2, late, climb, 0)

    @pl.when(inner)
    def _():
        cross_near(2)
        cross_edge(0)
        triangle(0, early, 0)

        def stage(group, carry):
            @pl.when(group + 2 < late)
            def _():
                cross_near(group + 2)

            cross_edge(group)
            triangle(early + group - 1, 1, group)
            return carry

        lax.fori_loop(1, late, stage, 0)
        triangle(share - 1, 1, late)

    pltpu.make_async_copy(back, back, recv_tri).wait()

    def finish(chunk, carry):
        first = pl.multiple_of(chunk * CHUNK, CHUNK)
        sums = back[:, pl.ds(first, CHUNK), :].astype(jnp.float32)
        center = jnp.mean(sums, axis=0, keepdims=True)
        deviate = sums - center
        spread = jnp.mean(deviate * deviate, axis=0, keepdims=True)
        scaled = deviate * lax.rsqrt(spread + 1e-05)
        planes[:hidden, :CHUNK, :] = scaled

        def one_row(local, inner_carry):
            at = first + local
            chans_first = wide[pl.ds(local, hidden, stride=PITCH), :]
            tri_normed = (chans_first * gain_col[...] + bias_col[...]).astype(jnp.bfloat16)
            projected = lax.dot_general(
                tri_normed, w_out_ref[...], (((0,), (0,)), ((), ())), preferred_element_type=jnp.float32
            )
            out_ref[at] = (gates[at] * projected).astype(jnp.bfloat16)
            return inner_carry

        lax.fori_loop(0, CHUNK, one_row, 0, unroll=FINISH_UNROLL)
        pltpu.make_async_copy(
            out_ref.at[chunk_rows(chunk)], out_hbm.at[chunk_rows(chunk)], store_sem
        ).start()
        return carry

    lax.fori_loop(0, chunks, finish, 0)
    pltpu.make_async_copy(out_ref, out_hbm, store_sem).wait()

    others = edges.at[pl.ds(0, (hubs - 1) * share)]
    pltpu.make_async_copy(others, others, send_left).wait()
    pltpu.make_async_copy(others, others, send_right).wait()

    passed = right.at[:, pl.ds(0, group_rows * row_count), :]
    pltpu.make_async_copy(passed, passed, send_far).wait()

    @pl.when(inner)
    def _():
        most = tri.at[:, pl.ds(0, (group_rows - 1) * row_count), :]
        pltpu.make_async_copy(most, most, send_tri).wait()
        more = tri.at[:, pl.ds(0, row_count), pl.ds(0, (ka_n - 1) * col_count)]
        pltpu.make_async_copy(more, more, send_tri).wait()


def fused(rows_n, ka_n, args):
    pair_repr, pair_mask, ln_gain, ln_bias, w_proj, w_gate, w_out_gate, out_gain, out_bias, w_out = args
    row_count, col_count, chans = pair_repr.shape
    hidden = w_out.shape[0]
    share = hidden // (rows_n // 4 * ka_n)
    late = share - EARLY
    chunks = row_count // CHUNK
    half = jnp.bfloat16
    return pl.pallas_call(
        functools.partial(kernel, rows_n, ka_n, EARLY),
        out_shape=jax.ShapeDtypeStruct(pair_repr.shape, half),
        in_specs=[pl.BlockSpec(memory_space=pl.ANY)] + [pl.BlockSpec(memory_space=pltpu.VMEM)] * 9,
        out_specs=pl.BlockSpec(memory_space=pl.ANY),
        scratch_shapes=[
            pltpu.VMEM((row_count, col_count, chans), half),
            pltpu.VMEM((row_count, col_count, chans), half),
            pltpu.VMEM((2 * hidden, row_count, col_count), half),
            pltpu.VMEM((2 * hidden * PITCH, col_count), jnp.float32),
            pltpu.VMEM((row_count, col_count, chans), half),
            pltpu.VMEM((row_count, col_count, chans), jnp.float32),
            pltpu.VMEM((share, rows_n // 2 * row_count, ka_n * col_count), half),
            pltpu.VMEM((share, rows_n * row_count, ka_n * col_count), half),
            pltpu.VMEM((share, rows_n // 2 * row_count, ka_n * col_count), half),
            pltpu.VMEM((hidden, row_count, col_count), half),
            pltpu.VMEM((4 * hidden, chans), half),
            pltpu.VMEM((hidden, col_count), jnp.float32),
            pltpu.VMEM((hidden, col_count), jnp.float32),
            pltpu.SemaphoreType.DMA((chunks,)),
            pltpu.SemaphoreType.DMA,
            pltpu.SemaphoreType.DMA((2, 1 + late)),
            pltpu.SemaphoreType.DMA((2, chunks)),
            pltpu.SemaphoreType.DMA((2, late)),
            pltpu.SemaphoreType.DMA((1 + late,)),
            pltpu.SemaphoreType.DMA,
            pltpu.SemaphoreType.DMA,
            pltpu.SemaphoreType.DMA,
            pltpu.SemaphoreType.DMA,
            pltpu.SemaphoreType.DMA,
        ],
        compiler_params=pltpu.CompilerParams(
            collective_id=0, has_side_effects=True, vmem_limit_bytes=60 * 2**20
        ),
    )(
        pair_repr, pair_mask, ln_gain[None], ln_bias[None], w_proj, w_gate, w_out_gate,
        out_gain[None], out_bias[None], w_out,
    )


def plain(args):
    pair_repr, pair_mask, ln_gain, ln_bias, w_proj, w_gate, w_out_gate, out_gain, out_bias, w_out = args
    row_count, col_count, chans = pair_repr.shape
    hidden = w_out.shape[0]
    normed = layer_norm(pair_repr.astype(jnp.float32), ln_gain, ln_bias).astype(jnp.bfloat16)
    flat_rows = normed.reshape(row_count * col_count, chans)
    projected = jnp.dot(flat_rows, w_proj, preferred_element_type=jnp.float32)
    gate_logits = jnp.dot(flat_rows, w_gate, preferred_element_type=jnp.float32)
    mask_col = pair_mask.reshape(row_count * col_count, 1).astype(jnp.float32)
    edges = (jax.nn.sigmoid(gate_logits) * projected * mask_col).astype(jnp.bfloat16)
    edges = edges.reshape(row_count, col_count, 2 * hidden)
    partial_sums = jnp.einsum(
        "ikh,jkh->ijh",
        edges[:, :, :hidden],
        lax.all_gather(edges[:, :, hidden:], "rows", axis=0, tiled=True),
        preferred_element_type=jnp.float32,
    )
    triangle = lax.psum_scatter(
        partial_sums.astype(jnp.bfloat16), "ka", scatter_dimension=1, tiled=True
    ).astype(jnp.float32)
    tri_normed = layer_norm(triangle, out_gain, out_bias).astype(jnp.bfloat16)
    out_gate = jax.nn.sigmoid(jnp.dot(flat_rows, w_out_gate, preferred_element_type=jnp.float32))
    projected_out = jnp.dot(
        tri_normed.reshape(row_count * col_count, hidden), w_out, preferred_element_type=jnp.float32
    )
    return (out_gate * projected_out).astype(jnp.bfloat16).reshape(row_count, col_count, chans)


def body(rows_n, ka_n, *args):
    row_count, col_count, chans = args[0].shape
    hidden = args[-1].shape[0]
    hubs = rows_n // 4 * ka_n
    aligned = row_count % CHUNK == 0 and col_count % 128 == 0 and chans % 128 == 0 and hidden % 128 == 0
    if aligned and rows_n % 4 == 0 and hidden % hubs == 0 and col_count == hidden:
        if hidden // hubs - EARLY > max(2, row_count // CHUNK):
            return fused(rows_n, ka_n, args)
    return plain(args)


def solution(mesh):
    placed = (P("rows", "ka", None), P("rows", "ka"), P(), P(), P(), P(), P(), P(), P(), P())
    return jax.shard_map(
        functools.partial(body, mesh.shape["rows"], mesh.shape["ka"]),
        mesh=mesh, in_specs=placed, out_specs=P("rows", "ka", None), check_vma=False,
    )
```

```python
import functools

import jax
import jax.numpy as jnp
from jax import lax
from jax.experimental import pallas as pl
from jax.experimental.pallas import tpu as pltpu
from jax.sharding import PartitionSpec as P

MESH = pl.DeviceIdType.MESH
CHUNK = 16
PITCH = 24
EARLY = 4
AHEAD = 3
MAKE_UNROLL = 8
GATE_UNROLL = 8
FINISH_UNROLL = 16


def layer_norm(values, gain_vec, bias_vec):
    center = jnp.mean(values, axis=-1, keepdims=True)
    deviate = values - center
    spread = jnp.mean(deviate * deviate, axis=-1, keepdims=True)
    return deviate * lax.rsqrt(spread + 1e-05) * gain_vec + bias_vec


def sigmoid(logits):
    return 0.5 + 0.5 * jnp.tanh(0.5 * logits)


def kernel(
    rows_n, ka_n, early,
    pair_hbm, mask_hbm, ln_gain_hbm, ln_bias_hbm, w_proj_hbm, w_gate_hbm, w_out_gate_hbm,
    out_gain_hbm, out_bias_hbm, w_out_hbm,
    out_hbm,
    mask_ref, ln_gain_ref, ln_bias_ref, w_proj_ref, w_gate_ref, w_out_gate_ref,
    out_gain_ref, out_bias_ref, w_out_ref,
    pair_ref, out_ref, edges, wide, normed, gates, left, right, tri, back, w_cat, gain_col, bias_col,
    small_sem, load_sem, store_sem, recv_left, recv_first, recv_early, recv_own, recv_right, recv_far, recv_tri,
    send_left, send_right, send_far, send_tri,
):
    row = lax.axis_index("rows")
    col = lax.axis_index("ka")
    row_count, col_count, chans = pair_ref.shape
    hidden = w_out_hbm.shape[0]
    zone = rows_n // 4
    group_rows = 2 * zone
    members = group_rows * ka_n
    hubs = zone * ka_n
    share = hidden // hubs
    late = share - early
    chunks = row_count // CHUNK
    ahead = AHEAD

    quarter = row // zone
    lane = row % zone
    half = quarter // 2
    spot = row % group_rows
    hub_q = 1 + half
    far_q = 2 - half
    edge_q = 3 * half
    place = half * (quarter - 2) + (1 - half) * (1 - quarter)
    inner = place == 0
    member = lane * ka_n + col
    planes = wide.reshape(2 * hidden, PITCH, col_count)

    def chunk_rows(chunk):
        return pl.ds(pl.multiple_of(chunk * CHUNK, CHUNK), CHUNK)

    def load(chunk):
        rows = chunk_rows(chunk)
        return pltpu.make_async_copy(pair_hbm.at[rows], pair_ref.at[rows], load_sem.at[chunk])

    smalls = [
        pltpu.make_async_copy(there, here, small_sem.at[at])
        for at, (there, here) in enumerate([
            (w_gate_hbm, w_gate_ref), (w_proj_hbm, w_proj_ref), (ln_gain_hbm, ln_gain_ref),
            (ln_bias_hbm, ln_bias_ref), (mask_hbm, mask_ref), (w_out_gate_hbm, w_out_gate_ref),
            (out_gain_hbm, out_gain_ref), (out_bias_hbm, out_bias_ref), (w_out_hbm, w_out_ref),
        ])
    ]
    smalls[0].start()
    smalls[1].start()
    load(0).start()
    for small in smalls[2:]:
        small.start()
    for chunk in range(1, chunks):
        load(chunk).start()

    barrier = pltpu.get_barrier_semaphore()

    def greet(step, carry):
        to_row = (row + step // ka_n) % rows_n
        to_col = (col + step % ka_n) % ka_n
        pl.semaphore_signal(barrier, inc=1, device_id=(to_row, to_col), device_id_type=MESH)
        return carry

    lax.fori_loop(1, rows_n * ka_n, greet, 0)

    def turned(ref):
        return ref[...].astype(jnp.float32).T.astype(jnp.bfloat16)

    smalls[0].wait()
    smalls[1].wait()
    w_cat[: 2 * hidden, :] = turned(w_gate_ref)
    w_cat[2 * hidden :, :] = turned(w_proj_ref)

    own_cols = pl.ds(pl.multiple_of(col * col_count, 128), col_count)

    def left_ends(chan, count, first, size, to_member):
        return (
            edges.at[pl.ds(to_member * share + chan, count), pl.ds(first, size), :],
            left.at[pl.ds(chan, count), pl.ds(spot * row_count + first, size), own_cols],
        )

    def right_ends(chan, count, first, size, to_member):
        return (
            edges.at[pl.ds(hidden + to_member * share + chan, count), pl.ds(first, size), :],
            right.at[pl.ds(chan, count), pl.ds(row * row_count + first, size), own_cols],
        )

    def send_edges(ends, chan, count, first, size, sent, landed, to_q=None):
        def start(to_lane, to_col):
            here, there = ends(chan, count, first, size, to_lane * ka_n + to_col)
            pltpu.make_async_remote_copy(
                src_ref=here, dst_ref=there, send_sem=sent, recv_sem=landed,
                device_id=((quarter if to_q is None else to_q) * zone + to_lane, to_col), device_id_type=MESH,
            ).start()

        def other(step, carry):
            start((lane + step % zone) % zone, (col + step // zone) % ka_n)
            return carry

        if to_q is not None:
            lax.fori_loop(0, hubs, other, 0)
            return
        lax.fori_loop(1, hubs, other, 0)
        here, there = ends(chan, count, first, size, member)
        pltpu.make_async_copy(here, there, landed).start()

    def make_chunk(chunk):
        load(chunk).wait()

        def one_row(local, carry):
            at = chunk * CHUNK + local
            values = pair_ref[at].astype(jnp.float32)
            plain = layer_norm(values, ln_gain_ref[...], ln_bias_ref[...]).astype(jnp.bfloat16)
            normed[at] = plain
            both = lax.dot_general(
                w_cat[...], plain, (((1,), (1,)), ((), ())), preferred_element_type=jnp.float32
            )
            mask_row = mask_ref[pl.ds(at, 1), :].astype(jnp.float32)
            made = sigmoid(both[: 2 * hidden]) * both[2 * hidden :] * mask_row
            wide[pl.ds(local, 2 * hidden, stride=PITCH), :] = made
            return carry

        lax.fori_loop(0, CHUNK, one_row, 0, unroll=MAKE_UNROLL)
        edges[:, chunk_rows(chunk), :] = planes[:, :CHUNK, :].astype(jnp.bfloat16)

    def send_early(chunk):
        first = pl.multiple_of(chunk * CHUNK, CHUNK)

        @pl.when(inner)
        def _():
            send_edges(right_ends, 0, early, first, CHUNK, send_far, recv_far.at[0], far_q)

        @pl.when(place == 1)
        def _():
            @pl.when(chunk == 0)
            def _():
                send_edges(right_ends, 0, early, first, CHUNK, send_far, recv_early.at[0], hub_q)

            @pl.when(chunk > 0)
            def _():
                send_edges(right_ends, 0, early, first, CHUNK, send_right, recv_first.at[0, chunk])

            send_edges(left_ends, 0, early, first, CHUNK, send_left, recv_first.at[1, chunk])

    def send_right_late(group):
        send_edges(right_ends, early + group, 1, 0, row_count, send_right, recv_right.at[0, group])

    def send_left_late(group):
        send_edges(left_ends, early + group, 1, 0, row_count, send_left, recv_left.at[0, 1 + group])

    def send_both(group, lead):
        send_right_late(group + lead)
        send_left_late(group)

    def await_part(part, landed):
        pltpu.make_async_copy(part, part, landed).wait()

    def pass_on(part, to_q, landed):
        pltpu.make_async_remote_copy(
            src_ref=part, dst_ref=part, send_sem=send_far, recv_sem=landed,
            device_id=(to_q * zone + lane, col), device_id_type=MESH,
        ).start()

    def right_rows(chan, count, first, size):
        return right.at[pl.ds(chan, count), pl.ds(pl.multiple_of(first, CHUNK), size), :]

    def left_rows(chan, count, from_q):
        first = pl.multiple_of(from_q % 2 * zone * row_count, CHUNK)
        return left.at[pl.ds(chan, count), pl.ds(first, zone * row_count), :]

    def pass_early(from_q, chunk, to_q, landed):
        for to_lane in range(zone):
            first = (from_q * zone + to_lane) * row_count + chunk * CHUNK
            pass_on(right_rows(0, early, first, CHUNK), to_q, landed)

    def pass_late(from_q, group, to_q, came, landed):
        part = right_rows(early + group, 1, from_q * zone * row_count, zone * row_count)
        await_part(part, came)
        pass_on(part, to_q, landed)

    def pass_left(chan, count, group):
        part = left_rows(chan, count, quarter)
        await_part(part, recv_left.at[0, group])
        pass_on(part, hub_q, recv_left.at[1, group])

    def climb_early(chunk):
        sizer = right_rows(0, early, 0, zone * CHUNK)

        @pl.when(chunk > 0)
        def _():
            await_part(sizer, recv_first.at[0, chunk])
            pass_early(quarter, chunk, hub_q, recv_early.at[chunk])

        await_part(sizer, recv_first.at[1, chunk])
        for to_lane in range(zone):
            first = (quarter % 2 * zone + to_lane) * row_count + chunk * CHUNK
            rows = pl.ds(pl.multiple_of(first, CHUNK), CHUNK)
            pass_on(left.at[pl.ds(0, early), rows, :], hub_q, recv_left.at[1, 0])

    def cross_early(chunk):
        await_part(right_rows(0, early, 0, zone * CHUNK), recv_early.at[chunk])
        pass_early(edge_q, chunk, far_q, recv_far.at[0])

    def cross_near(group):
        pass_late(hub_q, group, far_q, recv_right.at[0, group], recv_far.at[1 + group])

    def cross_edge(group):
        pass_late(edge_q, group, far_q, recv_right.at[1, group], recv_far.at[1 + group])

    def climb_right(group):
        pass_late(edge_q, group, hub_q, recv_right.at[0, group], recv_right.at[1, group])

    def climb_left(group):
        pass_left(early + group, 1, 1 + group)

    def climb(group, carry):
        climb_right(group)
        climb_left(group - 1)
        return carry

    def triangle(chan, count, group):
        await_part(left_rows(chan, count, hub_q), recv_left.at[0, group])
        await_part(left_rows(chan, count, edge_q), recv_left.at[1, group])
        await_part(right_rows(chan, count, 0, group_rows * row_count), recv_far.at[group])

        def one_channel(at, carry):
            tri[at] = lax.dot_general(
                left[at], right[at], (((1,), (1,)), ((), ())), preferred_element_type=jnp.float32
            ).astype(jnp.bfloat16)
            return carry

        lax.fori_loop(chan, chan + count, one_channel, 0)
        slot = back.at[pl.ds(member * share + chan, count)]

        def tri_part(to_spot, to_col):
            return tri.at[
                pl.ds(chan, count),
                pl.ds(pl.multiple_of(to_spot * row_count, CHUNK), row_count),
                pl.ds(pl.multiple_of(to_col * col_count, 128), col_count),
            ]

        def give(step, carry):
            to_spot, to_col = (spot + step % group_rows) % group_rows, (col + step // group_rows) % ka_n
            pltpu.make_async_remote_copy(
                src_ref=tri_part(to_spot, to_col), dst_ref=slot,
                send_sem=send_tri, recv_sem=recv_tri,
                device_id=(half * group_rows + to_spot, to_col), device_id_type=MESH,
            ).start()
            return carry

        lax.fori_loop(1, members, give, 0)
        pltpu.make_async_copy(tri_part(spot, col), slot, recv_tri).start()

    for small in smalls[2:]:
        small.wait()
    make_chunk(0)
    pl.semaphore_wait(barrier, rows_n * ka_n - 1)
    send_early(0)

    def rest(chunk, carry):
        make_chunk(chunk)
        send_early(chunk)

        @pl.when(place == 1)
        def _():
            climb_early(chunk - 1)

        return carry

    lax.fori_loop(1, chunks, rest, 0)

    @pl.when(place == 1)
    def _():
        climb_early(chunks - 1)
        send_right_late(0)

        def both(group, carry):
            send_both(group, 1)
            return carry

        lax.fori_loop(0, late - 1, both, 0)
        send_left_late(late - 1)
        climb_right(0)
        climb(1, 0)

    @pl.when(inner)
    def _():
        for group in range(ahead):
            send_right_late(group)
        send_edges(right_ends, 0, early, 0, row_count, send_right, recv_own)
        send_edges(left_ends, 0, early, 0, row_count, send_left, recv_left.at[0, 0])
        for chunk in range(chunks):
            cross_early(chunk)

            def both(group, carry):
                send_both(group, ahead)
                return carry

            span = late - ahead
            lax.fori_loop(span * chunk // chunks, span * (chunk + 1) // chunks, both, 0)
            if chunk < ahead:
                cross_near(chunk)
        for group in range(late - ahead, late):
            send_left_late(group)

    gain_col[...] = jnp.broadcast_to(out_gain_ref[...], (col_count, hidden)).T
    bias_col[...] = jnp.broadcast_to(out_bias_ref[...], (col_count, hidden)).T

    def gate_row(at, carry):
        gates[at] = sigmoid(
            jnp.dot(normed[at], w_out_gate_ref[...], preferred_element_type=jnp.float32)
        )
        return carry

    lax.fori_loop(0, row_count, gate_row, 0, unroll=GATE_UNROLL)

    @pl.when(place == 1)
    def _():
        lax.fori_loop(2, late, climb, 0)
        climb_left(late - 1)

    @pl.when(inner)
    def _():
        for group in range(min(chunks, ahead), ahead + 1):
            cross_near(group)
        cross_edge(0)
        await_part(right_rows(0, early, hub_q * zone * row_count, zone * row_count), recv_own)
        triangle(0, early, 0)

        def stage(group, carry):
            @pl.when(group + ahead < late)
            def _():
                cross_near(group + ahead)

            cross_edge(group)
            triangle(early + group - 1, 1, group)
            return carry

        lax.fori_loop(1, late, stage, 0)
        triangle(share - 1, 1, late)

    pltpu.make_async_copy(back, back, recv_tri).wait()

    def finish(chunk, carry):
        first = pl.multiple_of(chunk * CHUNK, CHUNK)
        sums = back[:, pl.ds(first, CHUNK), :].astype(jnp.float32)
        center = jnp.mean(sums, axis=0, keepdims=True)
        deviate = sums - center
        spread = jnp.mean(deviate * deviate, axis=0, keepdims=True)
        scaled = deviate * lax.rsqrt(spread + 1e-05)
        planes[:hidden, :CHUNK, :] = scaled

        def one_row(local, inner_carry):
            at = first + local
            chans_first = wide[pl.ds(local, hidden, stride=PITCH), :]
            tri_normed = (chans_first * gain_col[...] + bias_col[...]).astype(jnp.bfloat16)
            projected = lax.dot_general(
                tri_normed, w_out_ref[...], (((0,), (0,)), ((), ())), preferred_element_type=jnp.float32
            )
            out_ref[at] = (gates[at] * projected).astype(jnp.bfloat16)
            return inner_carry

        lax.fori_loop(0, CHUNK, one_row, 0, unroll=FINISH_UNROLL)
        pltpu.make_async_copy(
            out_ref.at[chunk_rows(chunk)], out_hbm.at[chunk_rows(chunk)], store_sem
        ).start()
        return carry

    lax.fori_loop(0, chunks, finish, 0)
    pltpu.make_async_copy(out_ref, out_hbm, store_sem).wait()

    def sent_all(first, count, rows, sem):
        part = edges.at[pl.ds(0, count), pl.ds(first, rows), :]
        await_part(part, sem)

    sent_all(0, (hubs - 1) * share, row_count, send_left)
    sent_all(0, (hubs - 1) * late, row_count, send_right)
    sent_all(CHUNK, (hubs - 1) * early, row_count - CHUNK, send_right)

    @pl.when(inner)
    def _():
        sent_all(0, (hubs - 1) * early, CHUNK, send_right)

    passed = right.at[:, pl.ds(0, group_rows * row_count), :]
    await_part(passed, send_far)

    @pl.when(inner)
    def _():
        most = tri.at[:, pl.ds(0, (group_rows - 1) * row_count), :]
        pltpu.make_async_copy(most, most, send_tri).wait()
        more = tri.at[:, pl.ds(0, row_count), pl.ds(0, (ka_n - 1) * col_count)]
        pltpu.make_async_copy(more, more, send_tri).wait()


def fused(rows_n, ka_n, args):
    pair_repr, pair_mask, ln_gain, ln_bias, w_proj, w_gate, w_out_gate, out_gain, out_bias, w_out = args
    row_count, col_count, chans = pair_repr.shape
    hidden = w_out.shape[0]
    share = hidden // (rows_n // 4 * ka_n)
    late = share - EARLY
    chunks = row_count // CHUNK
    half = jnp.bfloat16
    return pl.pallas_call(
        functools.partial(kernel, rows_n, ka_n, EARLY),
        out_shape=jax.ShapeDtypeStruct(pair_repr.shape, half),
        in_specs=[pl.BlockSpec(memory_space=pltpu.HBM)] * 10,
        out_specs=pl.BlockSpec(memory_space=pl.ANY),
        scratch_shapes=[
            pltpu.VMEM((row_count, col_count), jnp.int32),
            pltpu.VMEM((1, chans), jnp.float32),
            pltpu.VMEM((1, chans), jnp.float32),
            pltpu.VMEM((chans, 2 * hidden), half),
            pltpu.VMEM((chans, 2 * hidden), half),
            pltpu.VMEM((chans, chans), half),
            pltpu.VMEM((1, hidden), jnp.float32),
            pltpu.VMEM((1, hidden), jnp.float32),
            pltpu.VMEM((hidden, chans), half),
            pltpu.VMEM((row_count, col_count, chans), half),
            pltpu.VMEM((row_count, col_count, chans), half),
            pltpu.VMEM((2 * hidden, row_count, col_count), half),
            pltpu.VMEM((2 * hidden * PITCH, col_count), jnp.float32),
            pltpu.VMEM((row_count, col_count, chans), half),
            pltpu.VMEM((row_count, col_count, chans), jnp.float32),
            pltpu.VMEM((share, rows_n // 2 * row_count, ka_n * col_count), half),
            pltpu.VMEM((share, rows_n * row_count, ka_n * col_count), half),
            pltpu.VMEM((share, rows_n // 2 * row_count, ka_n * col_count), half),
            pltpu.VMEM((hidden, row_count, col_count), half),
            pltpu.VMEM((4 * hidden, chans), half),
            pltpu.VMEM((hidden, col_count), jnp.float32),
            pltpu.VMEM((hidden, col_count), jnp.float32),
            pltpu.SemaphoreType.DMA((9,)),
            pltpu.SemaphoreType.DMA((chunks,)),
            pltpu.SemaphoreType.DMA,
            pltpu.SemaphoreType.DMA((2, 1 + late)),
            pltpu.SemaphoreType.DMA((2, chunks)),
            pltpu.SemaphoreType.DMA((chunks,)),
            pltpu.SemaphoreType.DMA,
            pltpu.SemaphoreType.DMA((2, late)),
            pltpu.SemaphoreType.DMA((1 + late,)),
            pltpu.SemaphoreType.DMA,
            pltpu.SemaphoreType.DMA,
            pltpu.SemaphoreType.DMA,
            pltpu.SemaphoreType.DMA,
            pltpu.SemaphoreType.DMA,
        ],
        compiler_params=pltpu.CompilerParams(
            collective_id=0, has_side_effects=True, vmem_limit_bytes=42 * 2**20
        ),
    )(*[
        pltpu.with_memory_space_constraint(array, pltpu.HBM)
        for array in (
            pair_repr, pair_mask, ln_gain[None], ln_bias[None], w_proj, w_gate, w_out_gate,
            out_gain[None], out_bias[None], w_out,
        )
    ])


def plain(args):
    pair_repr, pair_mask, ln_gain, ln_bias, w_proj, w_gate, w_out_gate, out_gain, out_bias, w_out = args
    row_count, col_count, chans = pair_repr.shape
    hidden = w_out.shape[0]
    normed = layer_norm(pair_repr.astype(jnp.float32), ln_gain, ln_bias).astype(jnp.bfloat16)
    flat_rows = normed.reshape(row_count * col_count, chans)
    projected = jnp.dot(flat_rows, w_proj, preferred_element_type=jnp.float32)
    gate_logits = jnp.dot(flat_rows, w_gate, preferred_element_type=jnp.float32)
    mask_col = pair_mask.reshape(row_count * col_count, 1).astype(jnp.float32)
    edges = (jax.nn.sigmoid(gate_logits) * projected * mask_col).astype(jnp.bfloat16)
    edges = edges.reshape(row_count, col_count, 2 * hidden)
    partial_sums = jnp.einsum(
        "ikh,jkh->ijh",
        edges[:, :, :hidden],
        lax.all_gather(edges[:, :, hidden:], "rows", axis=0, tiled=True),
        preferred_element_type=jnp.float32,
    )
    triangle = lax.psum_scatter(
        partial_sums.astype(jnp.bfloat16), "ka", scatter_dimension=1, tiled=True
    ).astype(jnp.float32)
    tri_normed = layer_norm(triangle, out_gain, out_bias).astype(jnp.bfloat16)
    out_gate = jax.nn.sigmoid(jnp.dot(flat_rows, w_out_gate, preferred_element_type=jnp.float32))
    projected_out = jnp.dot(
        tri_normed.reshape(row_count * col_count, hidden), w_out, preferred_element_type=jnp.float32
    )
    return (out_gate * projected_out).astype(jnp.bfloat16).reshape(row_count, col_count, chans)


def body(rows_n, ka_n, *args):
    row_count, col_count, chans = args[0].shape
    hidden = args[-1].shape[0]
    hubs = rows_n // 4 * ka_n
    aligned = row_count % CHUNK == 0 and col_count % 128 == 0 and chans % 128 == 0 and hidden % 128 == 0
    if aligned and rows_n % 4 == 0 and hidden % hubs == 0 and col_count == hidden:
        if hidden // hubs - EARLY > AHEAD and row_count > CHUNK:
            return fused(rows_n, ka_n, args)
    return plain(args)


def solution(mesh):
    placed = (P("rows", "ka", None), P("rows", "ka"), P(), P(), P(), P(), P(), P(), P(), P())
    return jax.shard_map(
        functools.partial(body, mesh.shape["rows"], mesh.shape["ka"]),
        mesh=mesh, in_specs=placed, out_specs=P("rows", "ka", None), check_vma=False,
    )
```

```python
import functools

import jax
import jax.numpy as jnp
from jax import lax
from jax.experimental import pallas as pl
from jax.experimental.pallas import tpu as pltpu
from jax.sharding import PartitionSpec as P

MESH = pl.DeviceIdType.MESH
CHUNK = 16
PITCH = 24
EARLY = 4
SHARED = 2
AHEAD = 3
MAKE_UNROLL = 8
GATE_UNROLL = 8
FINISH_UNROLL = 16


def layer_norm(values, gain_vec, bias_vec):
    center = jnp.mean(values, axis=-1, keepdims=True)
    deviate = values - center
    spread = jnp.mean(deviate * deviate, axis=-1, keepdims=True)
    return deviate * lax.rsqrt(spread + 1e-05) * gain_vec + bias_vec


def sigmoid(logits):
    return 0.5 + 0.5 * jnp.tanh(0.5 * logits)


def kernel(
    rows_n, ka_n, early,
    pair_hbm, mask_hbm, ln_gain_hbm, ln_bias_hbm, w_proj_hbm, w_gate_hbm, w_out_gate_hbm,
    out_gain_hbm, out_bias_hbm, w_out_hbm,
    out_hbm,
    mask_ref, ln_gain_ref, ln_bias_ref, w_proj_ref, w_gate_ref, w_out_gate_ref,
    out_gain_ref, out_bias_ref, w_out_ref,
    pair_ref, out_ref, edges, wide, normed, gates, left, right, tri, back, w_cat, w_scaled, bias_row,
    mean_part, square_part,
    small_sem, load_sem, store_sem, recv_left, recv_first, recv_early, recv_own, recv_down, recv_right, recv_far, recv_tri,
    send_left, send_right, send_far, send_tri,
):
    row = lax.axis_index("rows")
    col = lax.axis_index("ka")
    row_count, col_count, chans = pair_ref.shape
    hidden = w_out_hbm.shape[0]
    zone = rows_n // 4
    group_rows = 2 * zone
    members = group_rows * ka_n
    hubs = zone * ka_n
    share = hidden // hubs
    late = share - early
    chunks = row_count // CHUNK
    ahead = AHEAD
    shared = SHARED

    quarter = row // zone
    lane = row % zone
    half = quarter // 2
    spot = row % group_rows
    hub_q = 1 + half
    far_q = 2 - half
    edge_q = 3 * half
    place = half * (quarter - 2) + (1 - half) * (1 - quarter)
    inner = place == 0
    member = lane * ka_n + col
    planes = wide.reshape(2 * hidden, PITCH, col_count)

    barrier = pltpu.get_barrier_semaphore()

    def hail(to_row, to_col):
        pl.semaphore_signal(barrier, inc=1, device_id=(to_row, to_col), device_id_type=MESH)

    def greet(step, carry):
        hail(half * group_rows + (spot + step % group_rows) % group_rows, (col + step // group_rows) % ka_n)
        return carry

    def greet_far(step, carry):
        hail(far_q * zone + step % zone, (col + step // zone) % ka_n)
        return carry

    def chunk_rows(chunk):
        return pl.ds(pl.multiple_of(chunk * CHUNK, CHUNK), CHUNK)

    def load(chunk):
        rows = chunk_rows(chunk)
        return pltpu.make_async_copy(pair_hbm.at[rows], pair_ref.at[rows], load_sem.at[chunk])

    smalls = [
        pltpu.make_async_copy(there, here, small_sem.at[at])
        for at, (there, here) in enumerate([
            (w_gate_hbm, w_gate_ref), (w_proj_hbm, w_proj_ref), (ln_gain_hbm, ln_gain_ref),
            (ln_bias_hbm, ln_bias_ref), (mask_hbm, mask_ref), (w_out_gate_hbm, w_out_gate_ref),
            (out_gain_hbm, out_gain_ref), (out_bias_hbm, out_bias_ref), (w_out_hbm, w_out_ref),
        ])
    ]
    smalls[0].start()
    smalls[1].start()
    load(0).start()
    for small in smalls[2:]:
        small.start()
    for chunk in range(1, chunks):
        load(chunk).start()

    @pl.when(inner)
    def _():
        lax.fori_loop(0, hubs, greet_far, 0)

    lax.fori_loop(1, members, greet, 0)

    def turned(ref):
        return ref[...].astype(jnp.float32).T.astype(jnp.bfloat16)

    smalls[0].wait()
    smalls[1].wait()
    gate_rows, proj_rows = turned(w_gate_ref), turned(w_proj_ref)
    w_cat[:hidden, :] = gate_rows[hidden:]
    w_cat[hidden : 2 * hidden, :] = proj_rows[hidden:]
    w_cat[2 * hidden : 3 * hidden, :] = gate_rows[:hidden]
    w_cat[3 * hidden :, :] = proj_rows[:hidden]

    own_cols = pl.ds(pl.multiple_of(col * col_count, 128), col_count)

    def left_ends(chan, count, first, size, to_member):
        return (
            edges.at[pl.ds(to_member * share + chan, count), pl.ds(first, size), :],
            left.at[pl.ds(chan, count), pl.ds(spot * row_count + first, size), own_cols],
        )

    def right_ends(chan, count, first, size, to_member):
        return (
            edges.at[pl.ds(hidden + to_member * share + chan, count), pl.ds(first, size), :],
            right.at[pl.ds(chan, count), pl.ds(row * row_count + first, size), own_cols],
        )

    def send_edges(ends, chan, count, first, size, sent, landed, to_q=None):
        def start(to_lane, to_col):
            here, there = ends(chan, count, first, size, to_lane * ka_n + to_col)
            pltpu.make_async_remote_copy(
                src_ref=here, dst_ref=there, send_sem=sent, recv_sem=landed,
                device_id=((quarter if to_q is None else to_q) * zone + to_lane, to_col), device_id_type=MESH,
            ).start()

        def other(step, carry):
            start((lane + step % zone) % zone, (col + step // zone) % ka_n)
            return carry

        if to_q is not None:
            lax.fori_loop(0, hubs, other, 0)
            return
        lax.fori_loop(1, hubs, other, 0)
        here, there = ends(chan, count, first, size, member)
        pltpu.make_async_copy(here, there, landed).start()

    def make_side(at, local, plain, first_row, first_chan):
        both = lax.dot_general(
            w_cat[first_row : first_row + 2 * hidden], plain, (((1,), (1,)), ((), ())),
            preferred_element_type=jnp.float32,
        )
        mask_row = mask_ref[pl.ds(at, 1), :].astype(jnp.float32)
        made = sigmoid(both[:hidden]) * both[hidden:] * mask_row
        wide[pl.ds(local + first_chan * PITCH, hidden, stride=PITCH), :] = made

    def normalise(at):
        values = pair_ref[at].astype(jnp.float32)
        plain = layer_norm(values, ln_gain_ref[...], ln_bias_ref[...]).astype(jnp.bfloat16)
        normed[at] = plain
        return plain

    def round_side(chunk, first_chan, count):
        some = pl.ds(first_chan, count)
        edges[some, chunk_rows(chunk), :] = planes[some, :CHUNK, :].astype(jnp.bfloat16)

    def make_first():
        load(0).wait()

        def right_row(at, carry):
            make_side(at, at, normalise(at), 0, hidden)
            return carry

        lax.fori_loop(0, CHUNK, right_row, 0, unroll=MAKE_UNROLL)
        round_side(0, hidden, hidden)

    def make_first_left():
        def left_row(at, carry):
            make_side(at, at, normed[at], 2 * hidden, 0)
            return carry

        lax.fori_loop(0, CHUNK, left_row, 0, unroll=MAKE_UNROLL)
        round_side(0, 0, hidden)

    def make_chunk(chunk):
        load(chunk).wait()

        def one_row(local, carry):
            at = chunk * CHUNK + local
            plain = normalise(at)
            make_side(at, local, plain, 0, hidden)
            make_side(at, local, plain, 2 * hidden, 0)
            return carry

        lax.fori_loop(0, CHUNK, one_row, 0, unroll=MAKE_UNROLL)
        round_side(chunk, 0, 2 * hidden)

    def send_early_right(chunk):
        first = pl.multiple_of(chunk * CHUNK, CHUNK)

        @pl.when(inner)
        def _():
            send_edges(right_ends, 0, early, first, CHUNK, send_far, recv_far.at[0], far_q)

        @pl.when((place == 1) & (chunk > 0))
        def _():
            send_edges(right_ends, 0, early, first, CHUNK, send_right, recv_first.at[0, chunk])

    def send_early_left(chunk):
        first = pl.multiple_of(chunk * CHUNK, CHUNK)

        @pl.when(place == 1)
        def _():
            send_edges(left_ends, 0, early, first, CHUNK, send_left, recv_first.at[1, chunk])

    def send_right_late(group):
        send_edges(right_ends, early + group, 1, 0, row_count, send_right, recv_right.at[0, group])

    def send_left_late(group):
        send_edges(left_ends, early + group, 1, 0, row_count, send_left, recv_left.at[0, 1 + group])

    def send_both(group, lead):
        send_right_late(group + lead)
        send_left_late(group)

    def await_part(part, landed):
        pltpu.make_async_copy(part, part, landed).wait()

    def pass_on(part, to_q, landed):
        pltpu.make_async_remote_copy(
            src_ref=part, dst_ref=part, send_sem=send_far, recv_sem=landed,
            device_id=(to_q * zone + lane, col), device_id_type=MESH,
        ).start()

    def right_rows(chan, count, first, size):
        return right.at[pl.ds(chan, count), pl.ds(pl.multiple_of(first, CHUNK), size), :]

    def left_rows(chan, count, from_q):
        first = pl.multiple_of(from_q % 2 * zone * row_count, CHUNK)
        return left.at[pl.ds(chan, count), pl.ds(first, zone * row_count), :]

    def pass_early(from_q, chunk, to_q, landed):
        for to_lane in range(zone):
            first = (from_q * zone + to_lane) * row_count + chunk * CHUNK
            pass_on(right_rows(0, early, first, CHUNK), to_q, landed)

    def pass_late(from_q, group, to_q, came, landed):
        part = right_rows(early + group, 1, from_q * zone * row_count, zone * row_count)
        await_part(part, came)
        pass_on(part, to_q, landed)

    def pass_left(chan, count, group):
        part = left_rows(chan, count, quarter)
        await_part(part, recv_left.at[0, group])
        pass_on(part, hub_q, recv_left.at[1, group])

    def climb_early(chunk):
        sizer = right_rows(0, early, 0, zone * CHUNK)

        @pl.when(chunk > 0)
        def _():
            await_part(sizer, recv_first.at[0, chunk])
            pass_early(quarter, chunk, hub_q, recv_early.at[chunk])

        await_part(sizer, recv_first.at[1, chunk])
        for to_lane in range(zone):
            first = (quarter % 2 * zone + to_lane) * row_count + chunk * CHUNK
            rows = pl.ds(pl.multiple_of(first, CHUNK), CHUNK)
            pass_on(left.at[pl.ds(shared, early - shared), rows, :], hub_q, recv_left.at[1, 0])

    def cross_early(chunk):
        await_part(right_rows(0, early, 0, zone * CHUNK), recv_early.at[chunk])
        pass_early(edge_q, chunk, far_q, recv_far.at[0])

    def cross_near(group):
        pass_late(hub_q, group, far_q, recv_right.at[0, group], recv_far.at[1 + group])

    def cross_edge(group):
        pass_late(edge_q, group, far_q, recv_right.at[1, group], recv_far.at[1 + group])

    def climb_right(group):
        pass_late(edge_q, group, hub_q, recv_right.at[0, group], recv_right.at[1, group])

    def climb_left(group):
        pass_left(early + group, 1, 1 + group)

    def climb(group, carry):
        climb_right(group)
        climb_left(group - 1)
        return carry

    far_first = (1 - half) * group_rows * row_count
    own_first = pl.multiple_of(quarter % 2 * zone * row_count, CHUNK)

    j_half = group_rows * row_count
    col_half = ka_n // 2

    def multiply(chan, count, first, size, j_first, j_size):
        j_rows = pl.ds(pl.multiple_of(j_first, 128), j_size)

        def one_channel(at, carry):
            tri[at, pl.ds(first, size), j_rows] = lax.dot_general(
                left[at, pl.ds(first, size), :], right[at, j_rows, :], (((1,), (1,)), ((), ())),
                preferred_element_type=jnp.float32,
            ).astype(jnp.bfloat16)
            return carry

        lax.fori_loop(chan, chan + count, one_channel, 0)

    def give_all(chan, count, base, spots, me, side, landed):
        slot = back.at[pl.ds(member * share + chan, count)]

        def part(to_spot, to_col):
            first = (base - half * group_rows + to_spot) * row_count
            return tri.at[
                pl.ds(chan, count),
                pl.ds(pl.multiple_of(first, CHUNK), row_count),
                pl.ds(pl.multiple_of(to_col * col_count, 128), col_count),
            ]

        def give(step, carry):
            to_spot = (me + step % spots) % spots
            to_col = side * col_half + (col + step // spots) % col_half
            pltpu.make_async_remote_copy(
                src_ref=part(to_spot, to_col), dst_ref=slot, send_sem=send_tri, recv_sem=landed,
                device_id=(base + to_spot, to_col), device_id_type=MESH,
            ).start()
            return carry

        @pl.when(col // col_half == side)
        def _():
            pltpu.make_async_copy(part(me, col), slot, landed).start()

        @pl.when(col // col_half != side)
        def _():
            give(0, 0)

        lax.fori_loop(1, spots * col_half, give, 0)

    def side_triangle(chan, count, side, landed):
        multiply(chan, count, 0, group_rows * row_count, side * j_half, j_half)
        give_all(chan, count, half * group_rows, group_rows, spot, side, landed)

    def triangle(chan, count, group, landed):
        await_part(left_rows(chan, count, hub_q), recv_left.at[0, group])
        await_part(left_rows(chan, count, edge_q), recv_left.at[1, group])
        side_triangle(chan, count, half, landed)
        await_part(right_rows(chan, count, far_first, group_rows * row_count), recv_far.at[group])
        side_triangle(chan, count, 1 - half, landed)

    def own_triangle():
        for side in range(2):
            multiply(0, shared, own_first, zone * row_count, side * j_half, j_half)
            give_all(0, shared, quarter * zone, zone, lane, side, recv_tri.at[0])

    for small in smalls[2:]:
        small.wait()
    make_first()
    pl.semaphore_wait(barrier, members - 1 + hubs * (1 - place))

    @pl.when(place == 1)
    def _():
        send_edges(right_ends, 0, early, 0, CHUNK, send_far, recv_early.at[0], hub_q)
        send_edges(right_ends, 0, shared, 0, CHUNK, send_right, recv_first.at[0, 0])

    send_early_right(0)
    make_first_left()
    send_early_left(0)

    def rest(chunk, carry):
        make_chunk(chunk)
        send_early_right(chunk)
        send_early_left(chunk)

        @pl.when(place == 1)
        def _():
            climb_early(chunk - 1)

        return carry

    lax.fori_loop(1, chunks, rest, 0)

    @pl.when(place == 1)
    def _():
        climb_early(chunks - 1)
        send_right_late(0)

        def both(group, carry):
            send_both(group, 1)
            return carry

        lax.fori_loop(0, late - 1, both, 0)
        send_left_late(late - 1)
        climb_right(0)
        climb(1, 0)

    @pl.when(inner)
    def _():
        for group in range(ahead):
            send_right_late(group)
        send_edges(right_ends, 0, early, 0, row_count, send_right, recv_own)
        send_edges(left_ends, 0, early, 0, row_count, send_left, recv_left.at[0, 0])
        for chunk in range(chunks):
            cross_early(chunk)

            def both(group, carry):
                send_both(group, ahead)
                return carry

            span = late - ahead
            lax.fori_loop(span * chunk // chunks, span * (chunk + 1) // chunks, both, 0)
            if chunk < ahead:
                cross_near(chunk)
        for group in range(late - ahead, late):
            send_left_late(group)
        own_rows = hub_q * zone * row_count
        await_part(right_rows(0, early, own_rows, zone * row_count), recv_own)
        pass_on(right_rows(0, shared, own_rows, zone * row_count), edge_q, recv_down)

    weights = w_out_ref[...].astype(jnp.float32)
    gain_col = jnp.broadcast_to(out_gain_ref[...], (chans, hidden)).T
    bias_col = jnp.broadcast_to(out_bias_ref[...], (chans, hidden)).T
    w_scaled[...] = (weights * gain_col).astype(jnp.bfloat16)
    bias_row[...] = jnp.sum(weights * bias_col, axis=0, keepdims=True)

    def gate_row(at, carry):
        gates[at] = sigmoid(
            jnp.dot(normed[at], w_out_gate_ref[...], preferred_element_type=jnp.float32)
        )
        return carry

    lax.fori_loop(0, row_count, gate_row, 0, unroll=GATE_UNROLL)

    @pl.when(place == 1)
    def _():
        lax.fori_loop(2, late, climb, 0)
        climb_left(late - 1)
        await_part(right_rows(0, shared, 0, zone * CHUNK), recv_first.at[0, 0])
        await_part(right_rows(0, shared, 0, 3 * zone * row_count), recv_down)
        own_triangle()

    @pl.when(inner)
    def _():
        for group in range(min(chunks, ahead), ahead + 1):
            cross_near(group)
        cross_edge(0)
        await_part(left_rows(0, early, hub_q), recv_left.at[0, 0])
        await_part(left_rows(shared, early - shared, edge_q), recv_left.at[1, 0])
        await_part(right_rows(0, early, 0, group_rows * row_count), recv_far.at[0])
        pass_on(right_rows(0, shared, far_first, group_rows * row_count), edge_q, recv_down)
        own_triangle()
        for side in range(2):
            side_triangle(shared, early - shared, side, recv_tri.at[0])

        def stage(group, carry):
            @pl.when(group + ahead < late)
            def _():
                cross_near(group + ahead)

            cross_edge(group)
            triangle(early + group - 1, 1, group, recv_tri.at[0])
            return carry

        lax.fori_loop(1, late, stage, 0)
        triangle(share - 1, 1, late, recv_tri.at[1])

    await_part(back.at[pl.ds(0, hidden - hubs)], recv_tri.at[0])
    known = hidden - hubs

    def by_member(chunk):
        sums = back[:, chunk_rows(chunk), :].astype(jnp.float32)
        return sums.reshape(hubs, share, CHUNK, col_count)

    def gather_stats(chunk, carry):
        rows = chunk_rows(chunk)
        some = [back[at * share : at * share + share - 1, rows, :].astype(jnp.float32) for at in range(hubs)]
        center = sum(jnp.sum(sums, axis=0) for sums in some) / known
        mean_part[rows, :] = center
        square_part[rows, :] = sum(jnp.sum((sums - center) * (sums - center), axis=0) for sums in some)
        return carry

    lax.fori_loop(0, chunks, gather_stats, 0)
    await_part(back.at[pl.ds(0, hubs)], recv_tri.at[1])

    def finish(chunk, carry):
        first = pl.multiple_of(chunk * CHUNK, CHUNK)
        sums = by_member(chunk)
        last = sums[:, share - 1]
        part = mean_part[chunk_rows(chunk), :]
        center = (part * known + jnp.sum(last, axis=0)) / hidden
        moved = part - center
        left_over = last - center
        squares = square_part[chunk_rows(chunk), :] + known * moved * moved
        squares = squares + jnp.sum(left_over * left_over, axis=0)
        scale = lax.rsqrt(squares / hidden + 1e-05)
        planes[:hidden, :CHUNK, :] = ((sums - center) * scale).reshape(hidden, CHUNK, col_count)

        def one_row(local, inner_carry):
            at = first + local
            tri_normed = wide[pl.ds(local, hidden, stride=PITCH), :].astype(jnp.bfloat16)
            projected = lax.dot_general(
                tri_normed, w_scaled[...], (((0,), (0,)), ((), ())), preferred_element_type=jnp.float32
            )
            out_ref[at] = (gates[at] * (projected + bias_row[...])).astype(jnp.bfloat16)
            return inner_carry

        lax.fori_loop(0, CHUNK, one_row, 0, unroll=FINISH_UNROLL)
        pltpu.make_async_copy(
            out_ref.at[chunk_rows(chunk)], out_hbm.at[chunk_rows(chunk)], store_sem
        ).start()
        return carry

    lax.fori_loop(0, chunks, finish, 0)
    pltpu.make_async_copy(out_ref, out_hbm, store_sem).wait()

    def sent_all(first, count, rows, sem):
        part = edges.at[pl.ds(0, count), pl.ds(first, rows), :]
        await_part(part, sem)

    sent_all(0, (hubs - 1) * share, row_count, send_left)
    sent_all(0, (hubs - 1) * late, row_count, send_right)
    sent_all(CHUNK, (hubs - 1) * early, row_count - CHUNK, send_right)

    @pl.when(place == 1)
    def _():
        sent_all(0, (hubs - 1) * shared, CHUNK, send_right)

    @pl.when(inner)
    def _():
        sent_all(0, (hubs - 1) * early, CHUNK, send_right)

    def given_all(count, spots):
        if spots > 1:
            await_part(tri.at[pl.ds(0, count), pl.ds(0, (spots - 1) * row_count), :], send_tri)
        await_part(tri.at[pl.ds(0, count), pl.ds(0, row_count), pl.ds(0, (ka_n - 1) * col_count)], send_tri)

    plane = zone * row_count
    await_part(right.at[:, pl.ds(0, plane), :], send_far)
    await_part(right.at[pl.ds(0, share - shared), pl.ds(0, plane), :], send_far)
    given_all(shared, zone)

    @pl.when(inner)
    def _():
        await_part(right.at[pl.ds(0, shared), pl.ds(0, 2 * plane), :], send_far)
        await_part(right.at[pl.ds(0, shared), pl.ds(0, 2 * plane), :], send_far)
        given_all(share - shared, group_rows)


def fused(rows_n, ka_n, args):
    pair_repr, pair_mask, ln_gain, ln_bias, w_proj, w_gate, w_out_gate, out_gain, out_bias, w_out = args
    row_count, col_count, chans = pair_repr.shape
    hidden = w_out.shape[0]
    share = hidden // (rows_n // 4 * ka_n)
    late = share - EARLY
    chunks = row_count // CHUNK
    half = jnp.bfloat16
    return pl.pallas_call(
        functools.partial(kernel, rows_n, ka_n, EARLY),
        out_shape=jax.ShapeDtypeStruct(pair_repr.shape, half),
        in_specs=[pl.BlockSpec(memory_space=pltpu.HBM)] * 10,
        out_specs=pl.BlockSpec(memory_space=pl.ANY),
        scratch_shapes=[
            pltpu.VMEM((row_count, col_count), jnp.int32),
            pltpu.VMEM((1, chans), jnp.float32),
            pltpu.VMEM((1, chans), jnp.float32),
            pltpu.VMEM((chans, 2 * hidden), half),
            pltpu.VMEM((chans, 2 * hidden), half),
            pltpu.VMEM((chans, chans), half),
            pltpu.VMEM((1, hidden), jnp.float32),
            pltpu.VMEM((1, hidden), jnp.float32),
            pltpu.VMEM((hidden, chans), half),
            pltpu.VMEM((row_count, col_count, chans), half),
            pltpu.VMEM((row_count, col_count, chans), half),
            pltpu.VMEM((2 * hidden, row_count, col_count), half),
            pltpu.VMEM((2 * hidden * PITCH, col_count), jnp.float32),
            pltpu.VMEM((row_count, col_count, chans), half),
            pltpu.VMEM((row_count, col_count, chans), jnp.float32),
            pltpu.VMEM((share, rows_n // 2 * row_count, ka_n * col_count), half),
            pltpu.VMEM((share, rows_n * row_count, ka_n * col_count), half),
            pltpu.VMEM((share, rows_n // 2 * row_count, ka_n * col_count), half),
            pltpu.VMEM((hidden, row_count, col_count), half),
            pltpu.VMEM((4 * hidden, chans), half),
            pltpu.VMEM((hidden, chans), half),
            pltpu.VMEM((1, chans), jnp.float32),
            pltpu.VMEM((row_count, col_count), jnp.float32),
            pltpu.VMEM((row_count, col_count), jnp.float32),
            pltpu.SemaphoreType.DMA((9,)),
            pltpu.SemaphoreType.DMA((chunks,)),
            pltpu.SemaphoreType.DMA,
            pltpu.SemaphoreType.DMA((2, 1 + late)),
            pltpu.SemaphoreType.DMA((2, chunks)),
            pltpu.SemaphoreType.DMA((chunks,)),
            pltpu.SemaphoreType.DMA,
            pltpu.SemaphoreType.DMA,
            pltpu.SemaphoreType.DMA((2, late)),
            pltpu.SemaphoreType.DMA((1 + late,)),
            pltpu.SemaphoreType.DMA((2,)),
            pltpu.SemaphoreType.DMA,
            pltpu.SemaphoreType.DMA,
            pltpu.SemaphoreType.DMA,
            pltpu.SemaphoreType.DMA,
        ],
        compiler_params=pltpu.CompilerParams(
            collective_id=0, has_side_effects=True, vmem_limit_bytes=42 * 2**20
        ),
    )(*[
        pltpu.with_memory_space_constraint(array, pltpu.HBM)
        for array in (
            pair_repr, pair_mask, ln_gain[None], ln_bias[None], w_proj, w_gate, w_out_gate,
            out_gain[None], out_bias[None], w_out,
        )
    ])


def plain(args):
    pair_repr, pair_mask, ln_gain, ln_bias, w_proj, w_gate, w_out_gate, out_gain, out_bias, w_out = args
    row_count, col_count, chans = pair_repr.shape
    hidden = w_out.shape[0]
    normed = layer_norm(pair_repr.astype(jnp.float32), ln_gain, ln_bias).astype(jnp.bfloat16)
    flat_rows = normed.reshape(row_count * col_count, chans)
    projected = jnp.dot(flat_rows, w_proj, preferred_element_type=jnp.float32)
    gate_logits = jnp.dot(flat_rows, w_gate, preferred_element_type=jnp.float32)
    mask_col = pair_mask.reshape(row_count * col_count, 1).astype(jnp.float32)
    edges = (jax.nn.sigmoid(gate_logits) * projected * mask_col).astype(jnp.bfloat16)
    edges = edges.reshape(row_count, col_count, 2 * hidden)
    partial_sums = jnp.einsum(
        "ikh,jkh->ijh",
        edges[:, :, :hidden],
        lax.all_gather(edges[:, :, hidden:], "rows", axis=0, tiled=True),
        preferred_element_type=jnp.float32,
    )
    triangle = lax.psum_scatter(
        partial_sums.astype(jnp.bfloat16), "ka", scatter_dimension=1, tiled=True
    ).astype(jnp.float32)
    tri_normed = layer_norm(triangle, out_gain, out_bias).astype(jnp.bfloat16)
    out_gate = jax.nn.sigmoid(jnp.dot(flat_rows, w_out_gate, preferred_element_type=jnp.float32))
    projected_out = jnp.dot(
        tri_normed.reshape(row_count * col_count, hidden), w_out, preferred_element_type=jnp.float32
    )
    return (out_gate * projected_out).astype(jnp.bfloat16).reshape(row_count, col_count, chans)


def body(rows_n, ka_n, *args):
    row_count, col_count, chans = args[0].shape
    hidden = args[-1].shape[0]
    hubs = rows_n // 4 * ka_n
    aligned = row_count % CHUNK == 0 and col_count % 128 == 0 and chans % 128 == 0 and hidden % 128 == 0
    if aligned and rows_n % 4 == 0 and ka_n % 2 == 0 and hidden % hubs == 0 and col_count == hidden:
        if hidden // hubs - EARLY > AHEAD and row_count > CHUNK:
            return fused(rows_n, ka_n, args)
    return plain(args)


def solution(mesh):
    placed = (P("rows", "ka", None), P("rows", "ka"), P(), P(), P(), P(), P(), P(), P(), P())
    return jax.shard_map(
        functools.partial(body, mesh.shape["rows"], mesh.shape["ka"]),
        mesh=mesh, in_specs=placed, out_specs=P("rows", "ka", None), check_vma=False,
    )
```

```python
import functools

import jax
import jax.numpy as jnp
from jax import lax
from jax.experimental import pallas as pl
from jax.experimental.pallas import tpu as pltpu
from jax.sharding import PartitionSpec as P

MESH = pl.DeviceIdType.MESH
CHUNK = 16
PITCH = 24
EARLY = 4
SHARED = 2
AHEAD = 3
MAKE_UNROLL = 8
GATE_UNROLL = 8
FINISH_UNROLL = 16


def layer_norm(values, gain_vec, bias_vec):
    center = jnp.mean(values, axis=-1, keepdims=True)
    deviate = values - center
    spread = jnp.mean(deviate * deviate, axis=-1, keepdims=True)
    return deviate * lax.rsqrt(spread + 1e-05) * gain_vec + bias_vec


def sigmoid(logits):
    return 0.5 + 0.5 * jnp.tanh(0.5 * logits)


def kernel(
    rows_n, ka_n, early,
    pair_hbm, mask_hbm, ln_gain_hbm, ln_bias_hbm, w_proj_hbm, w_gate_hbm, w_out_gate_hbm,
    out_gain_hbm, out_bias_hbm, w_out_hbm,
    out_hbm,
    mask_ref, ln_gain_ref, ln_bias_ref, w_proj_ref, w_gate_ref, w_out_gate_ref,
    out_gain_ref, out_bias_ref, w_out_ref,
    pair_ref, out_ref, edges, wide, normed, gates, left, right, tri, back, w_cat, w_scaled, bias_row,
    mean_part, square_part,
    small_sem, load_sem, store_sem, recv_left, recv_first, recv_early, recv_own, recv_down, recv_right, recv_far, recv_tri,
    send_left, send_right, send_far, send_tri,
):
    row = lax.axis_index("rows")
    col = lax.axis_index("ka")
    row_count, col_count, chans = pair_ref.shape
    hidden = w_out_hbm.shape[0]
    zone = rows_n // 4
    group_rows = 2 * zone
    members = group_rows * ka_n
    hubs = zone * ka_n
    share = hidden // hubs
    late = share - early
    chunks = row_count // CHUNK
    ahead = AHEAD
    shared = SHARED

    quarter = row // zone
    lane = row % zone
    half = quarter // 2
    spot = row % group_rows
    hub_q = 1 + half
    far_q = 2 - half
    edge_q = 3 * half
    place = half * (quarter - 2) + (1 - half) * (1 - quarter)
    inner = place == 0
    member = lane * ka_n + col
    planes = wide.reshape(2 * hidden, PITCH, col_count)

    barrier = pltpu.get_barrier_semaphore()

    def hail(to_row, to_col):
        pl.semaphore_signal(barrier, inc=1, device_id=(to_row, to_col), device_id_type=MESH)

    def greet(step, carry):
        hail(half * group_rows + (spot + step % group_rows) % group_rows, (col + step // group_rows) % ka_n)
        return carry

    def greet_far(step, carry):
        hail(far_q * zone + step % zone, (col + step // zone) % ka_n)
        return carry

    def chunk_rows(chunk):
        return pl.ds(pl.multiple_of(chunk * CHUNK, CHUNK), CHUNK)

    def load(chunk):
        rows = chunk_rows(chunk)
        return pltpu.make_async_copy(pair_hbm.at[rows], pair_ref.at[rows], load_sem.at[chunk])

    smalls = [
        pltpu.make_async_copy(there, here, small_sem.at[at])
        for at, (there, here) in enumerate([
            (w_gate_hbm, w_gate_ref), (w_proj_hbm, w_proj_ref), (ln_gain_hbm, ln_gain_ref),
            (ln_bias_hbm, ln_bias_ref), (mask_hbm, mask_ref), (w_out_gate_hbm, w_out_gate_ref),
            (out_gain_hbm, out_gain_ref), (out_bias_hbm, out_bias_ref), (w_out_hbm, w_out_ref),
        ])
    ]
    smalls[0].start()
    smalls[1].start()
    load(0).start()
    for small in smalls[2:]:
        small.start()
    for chunk in range(1, chunks):
        load(chunk).start()

    @pl.when(inner)
    def _():
        lax.fori_loop(0, hubs, greet_far, 0)

    lax.fori_loop(1, members, greet, 0)

    def turned(ref):
        return ref[...].astype(jnp.float32).T.astype(jnp.bfloat16)

    smalls[0].wait()
    smalls[1].wait()
    gate_rows, proj_rows = turned(w_gate_ref), turned(w_proj_ref)
    w_cat[:hidden, :] = gate_rows[hidden:]
    w_cat[hidden : 2 * hidden, :] = proj_rows[hidden:]
    w_cat[2 * hidden : 3 * hidden, :] = gate_rows[:hidden]
    w_cat[3 * hidden :, :] = proj_rows[:hidden]

    own_cols = pl.ds(pl.multiple_of(col * col_count, 128), col_count)

    def left_ends(chan, count, first, size, to_member):
        return (
            edges.at[pl.ds(to_member * share + chan, count), pl.ds(first, size), :],
            left.at[pl.ds(chan, count), pl.ds(spot * row_count + first, size), own_cols],
        )

    def right_ends(chan, count, first, size, to_member):
        return (
            edges.at[pl.ds(hidden + to_member * share + chan, count), pl.ds(first, size), :],
            right.at[pl.ds(chan, count), pl.ds(row * row_count + first, size), own_cols],
        )

    def send_edges(ends, chan, count, first, size, sent, landed, to_q=None):
        def start(to_lane, to_col):
            here, there = ends(chan, count, first, size, to_lane * ka_n + to_col)
            pltpu.make_async_remote_copy(
                src_ref=here, dst_ref=there, send_sem=sent, recv_sem=landed,
                device_id=((quarter if to_q is None else to_q) * zone + to_lane, to_col), device_id_type=MESH,
            ).start()

        def other(step, carry):
            start((lane + step % zone) % zone, (col + step // zone) % ka_n)
            return carry

        if to_q is not None:
            lax.fori_loop(0, hubs, other, 0)
            return
        lax.fori_loop(1, hubs, other, 0)
        here, there = ends(chan, count, first, size, member)
        pltpu.make_async_copy(here, there, landed).start()

    def make_side(at, local, plain, first_row, first_chan):
        both = lax.dot_general(
            w_cat[first_row : first_row + 2 * hidden], plain, (((1,), (1,)), ((), ())),
            preferred_element_type=jnp.float32,
        )
        mask_row = mask_ref[pl.ds(at, 1), :].astype(jnp.float32)
        made = sigmoid(both[:hidden]) * both[hidden:] * mask_row
        wide[pl.ds(local + first_chan * PITCH, hidden, stride=PITCH), :] = made

    def normalise(at):
        values = pair_ref[at].astype(jnp.float32)
        plain = layer_norm(values, ln_gain_ref[...], ln_bias_ref[...]).astype(jnp.bfloat16)
        normed[at] = plain
        return plain

    def round_side(chunk, first_chan, count):
        some = pl.ds(first_chan, count)
        edges[some, chunk_rows(chunk), :] = planes[some, :CHUNK, :].astype(jnp.bfloat16)

    def make_first():
        load(0).wait()

        def right_row(at, carry):
            make_side(at, at, normalise(at), 0, hidden)
            return carry

        lax.fori_loop(0, CHUNK, right_row, 0, unroll=CHUNK)
        round_side(0, hidden, hidden)

    def make_first_left():
        def left_row(at, carry):
            make_side(at, at, normed[at], 2 * hidden, 0)
            return carry

        lax.fori_loop(0, CHUNK, left_row, 0, unroll=MAKE_UNROLL)
        round_side(0, 0, hidden)

    def make_chunk(chunk):
        load(chunk).wait()

        def one_row(local, carry):
            at = chunk * CHUNK + local
            plain = normalise(at)
            make_side(at, local, plain, 0, hidden)
            make_side(at, local, plain, 2 * hidden, 0)
            return carry

        lax.fori_loop(0, CHUNK, one_row, 0, unroll=MAKE_UNROLL)
        round_side(chunk, 0, 2 * hidden)

    def send_early_right(chunk):
        first = pl.multiple_of(chunk * CHUNK, CHUNK)

        @pl.when(inner)
        def _():
            send_edges(right_ends, 0, early, first, CHUNK, send_far, recv_far.at[0, 0], far_q)

        @pl.when((place == 1) & (chunk > 0))
        def _():
            send_edges(right_ends, 0, early, first, CHUNK, send_right, recv_first.at[0, chunk])

    def send_early_left(chunk):
        first = pl.multiple_of(chunk * CHUNK, CHUNK)

        @pl.when(place == 1)
        def _():
            send_edges(left_ends, 0, early, first, CHUNK, send_left, recv_first.at[1, chunk])

    def send_right_late(group):
        send_edges(right_ends, early + group, 1, 0, row_count, send_right, recv_right.at[0, group])

    def send_left_late(group):
        send_edges(left_ends, early + group, 1, 0, row_count, send_left, recv_left.at[0, 1 + group])

    def send_both(group, lead):
        send_right_late(group + lead)
        send_left_late(group)

    def await_part(part, landed):
        pltpu.make_async_copy(part, part, landed).wait()

    def pass_on(part, to_q, landed):
        pltpu.make_async_remote_copy(
            src_ref=part, dst_ref=part, send_sem=send_far, recv_sem=landed,
            device_id=(to_q * zone + lane, col), device_id_type=MESH,
        ).start()

    def right_rows(chan, count, first, size):
        return right.at[pl.ds(chan, count), pl.ds(pl.multiple_of(first, CHUNK), size), :]

    def left_rows(chan, count, from_q):
        first = pl.multiple_of(from_q % 2 * zone * row_count, CHUNK)
        return left.at[pl.ds(chan, count), pl.ds(first, zone * row_count), :]

    def pass_early(from_q, chunk, to_q, landed):
        for to_lane in range(zone):
            first = (from_q * zone + to_lane) * row_count + chunk * CHUNK
            pass_on(right_rows(0, early, first, CHUNK), to_q, landed)

    def pass_late(from_q, group, to_q, came, landed):
        part = right_rows(early + group, 1, from_q * zone * row_count, zone * row_count)
        await_part(part, came)
        pass_on(part, to_q, landed)

    def pass_left(chan, count, group):
        part = left_rows(chan, count, quarter)
        await_part(part, recv_left.at[0, group])
        pass_on(part, hub_q, recv_left.at[1, group])

    def climb_early(chunk):
        sizer = right_rows(0, early, 0, zone * CHUNK)

        @pl.when(chunk > 0)
        def _():
            await_part(sizer, recv_first.at[0, chunk])
            pass_early(quarter, chunk, hub_q, recv_early.at[chunk])

        await_part(sizer, recv_first.at[1, chunk])
        for to_lane in range(zone):
            first = (quarter % 2 * zone + to_lane) * row_count + chunk * CHUNK
            rows = pl.ds(pl.multiple_of(first, CHUNK), CHUNK)
            pass_on(left.at[pl.ds(shared, early - shared), rows, :], hub_q, recv_left.at[1, 0])

    def cross_early(chunk):
        await_part(right_rows(0, early, 0, zone * CHUNK), recv_early.at[chunk])
        pass_early(edge_q, chunk, far_q, recv_far.at[1, 0])

    def cross_near(group):
        pass_late(hub_q, group, far_q, recv_right.at[0, group], recv_far.at[0, 1 + group])

    def cross_edge(group):
        pass_late(edge_q, group, far_q, recv_right.at[1, group], recv_far.at[1, 1 + group])

    def climb_right(group):
        pass_late(edge_q, group, hub_q, recv_right.at[0, group], recv_right.at[1, group])

    def climb_left(group):
        pass_left(early + group, 1, 1 + group)

    def climb(group, carry):
        climb_right(group)
        climb_left(group - 1)
        return carry

    far_first = (1 - half) * group_rows * row_count
    own_first = pl.multiple_of(quarter % 2 * zone * row_count, CHUNK)

    j_block = zone * row_count
    col_block = ka_n // 4

    def multiply(chan, count, first, size, j_first, j_size):
        j_rows = pl.ds(pl.multiple_of(j_first, 128), j_size)

        def one_channel(at, carry):
            tri[at, pl.ds(first, size), j_rows] = lax.dot_general(
                left[at, pl.ds(first, size), :], right[at, j_rows, :], (((1,), (1,)), ((), ())),
                preferred_element_type=jnp.float32,
            ).astype(jnp.bfloat16)
            return carry

        lax.fori_loop(chan, chan + count, one_channel, 0)

    def give_all(chan, count, base, spots, me, col_first, col_size, landed):
        slot = back.at[pl.ds(member * share + chan, count)]

        def part(to_spot, to_col):
            first = (base - half * group_rows + to_spot) * row_count
            return tri.at[
                pl.ds(chan, count),
                pl.ds(pl.multiple_of(first, CHUNK), row_count),
                pl.ds(pl.multiple_of(to_col * col_count, 128), col_count),
            ]

        def give(step, carry):
            to_spot = (me + step % spots) % spots
            to_col = col_first + (col + step // spots) % col_size
            pltpu.make_async_remote_copy(
                src_ref=part(to_spot, to_col), dst_ref=slot, send_sem=send_tri, recv_sem=landed,
                device_id=(base + to_spot, to_col), device_id_type=MESH,
            ).start()
            return carry

        mine = (col >= col_first) & (col < col_first + col_size)

        @pl.when(mine)
        def _():
            pltpu.make_async_copy(part(me, col), slot, landed).start()

        @pl.when(jnp.logical_not(mine))
        def _():
            give(0, 0)

        lax.fori_loop(1, spots * col_size, give, 0)

    def block(chan, count, from_q, quarters, landed):
        multiply(chan, count, 0, group_rows * row_count, from_q * j_block, quarters * j_block)
        give_all(
            chan, count, half * group_rows, group_rows, spot, from_q * col_block, quarters * col_block, landed
        )

    def near_block(chan, count, group, landed):
        await_part(left_rows(chan, count, hub_q), recv_left.at[0, group])
        await_part(left_rows(chan, count, edge_q), recv_left.at[1, group])
        block(chan, count, 2 * half, 2, landed)

    def far_block(chan, count, group, landed):
        for where in range(2):
            far_part(where, chan, count, group, landed)

    def far_part(where, chan, count, group, landed):
        from_q = far_q if where == 0 else 3 * (1 - half)
        part = right_rows(chan, count, from_q * zone * row_count, zone * row_count)
        await_part(part, recv_far.at[where, group])
        block(chan, count, from_q, 1, landed)

    def own_triangle():
        multiply(0, shared, own_first, zone * row_count, 0, rows_n * row_count)
        give_all(0, shared, quarter * zone, zone, lane, 0, ka_n, recv_tri.at[0])

    known = hidden - hubs

    def gather_stats():
        await_part(back.at[pl.ds(0, known)], recv_tri.at[0])

        def one_chunk(chunk, carry):
            rows = chunk_rows(chunk)
            some = [
                back[at * share : at * share + share - 1, rows, :].astype(jnp.float32) for at in range(hubs)
            ]
            center = sum(jnp.sum(sums, axis=0) for sums in some) / known
            mean_part[rows, :] = center
            square_part[rows, :] = sum(
                jnp.sum((sums - center) * (sums - center), axis=0) for sums in some
            )
            return carry

        lax.fori_loop(0, chunks, one_chunk, 0)

    for small in smalls[2:]:
        small.wait()
    make_first()
    pl.semaphore_wait(barrier, members - 1 + hubs * (1 - place))

    @pl.when(place == 1)
    def _():
        send_edges(right_ends, 0, early, 0, CHUNK, send_far, recv_early.at[0], hub_q)
        send_edges(right_ends, 0, shared, 0, CHUNK, send_right, recv_first.at[0, 0])

    send_early_right(0)
    make_first_left()
    send_early_left(0)

    def rest(chunk, carry):
        make_chunk(chunk)
        send_early_right(chunk)
        send_early_left(chunk)

        @pl.when(place == 1)
        def _():
            climb_early(chunk - 1)

        return carry

    lax.fori_loop(1, chunks, rest, 0)

    @pl.when(place == 1)
    def _():
        climb_early(chunks - 1)
        send_right_late(0)

        def both(group, carry):
            send_both(group, 1)
            return carry

        lax.fori_loop(0, late - 1, both, 0)
        send_left_late(late - 1)
        climb_right(0)
        climb(1, 0)

    @pl.when(inner)
    def _():
        for group in range(ahead):
            send_right_late(group)
        send_edges(right_ends, 0, early, 0, row_count, send_right, recv_own)
        send_edges(left_ends, 0, early, 0, row_count, send_left, recv_left.at[0, 0])
        for chunk in range(chunks):
            cross_early(chunk)

            def both(group, carry):
                send_both(group, ahead)
                return carry

            span = late - ahead
            lax.fori_loop(span * chunk // chunks, span * (chunk + 1) // chunks, both, 0)
            if chunk < ahead:
                cross_near(chunk)
        for group in range(late - ahead, late):
            send_left_late(group)
        own_rows = hub_q * zone * row_count
        await_part(right_rows(0, early, own_rows, zone * row_count), recv_own)
        pass_on(right_rows(0, shared, own_rows, zone * row_count), edge_q, recv_down)

    weights = w_out_ref[...].astype(jnp.float32)
    gain_col = jnp.broadcast_to(out_gain_ref[...], (chans, hidden)).T
    bias_col = jnp.broadcast_to(out_bias_ref[...], (chans, hidden)).T
    w_scaled[...] = (weights * gain_col).astype(jnp.bfloat16)
    bias_row[...] = jnp.sum(weights * bias_col, axis=0, keepdims=True)

    def gate_row(at, carry):
        gates[at] = sigmoid(
            jnp.dot(normed[at], w_out_gate_ref[...], preferred_element_type=jnp.float32)
        )
        return carry

    lax.fori_loop(0, row_count, gate_row, 0, unroll=GATE_UNROLL)

    @pl.when(place == 1)
    def _():
        lax.fori_loop(2, late, climb, 0)
        climb_left(late - 1)
        await_part(right_rows(0, shared, 0, zone * CHUNK), recv_first.at[0, 0])
        await_part(right_rows(0, shared, 0, 3 * zone * row_count), recv_down)
        own_triangle()

    @pl.when(inner)
    def _():
        for group in range(min(chunks, ahead), ahead + 1):
            cross_near(group)
        cross_edge(0)
        await_part(left_rows(0, early, hub_q), recv_left.at[0, 0])
        await_part(left_rows(shared, early - shared, edge_q), recv_left.at[1, 0])
        for where, from_q in ((0, far_q), (1, 3 * (1 - half))):
            await_part(right_rows(0, early, from_q * zone * row_count, zone * row_count), recv_far.at[where, 0])
        pass_on(right_rows(0, shared, far_first, group_rows * row_count), edge_q, recv_down)
        own_triangle()
        block(shared, early - shared, 0, 4, recv_tri.at[0])

        def near_upto(group):
            return ahead + 1 + (late - ahead - 1) * group // (late - 1)

        def near_one(group, carry):
            cross_near(group)
            return carry

        def stage(group, carry):
            lax.fori_loop(near_upto(group - 1), near_upto(group), near_one, 0)
            cross_edge(group)
            near_block(early + group - 1, 1, group, recv_tri.at[0])
            far_block(early + group - 1, 1, group, recv_tri.at[0])
            return carry

        lax.fori_loop(1, late, stage, 0)
        near_block(share - 1, 1, late, recv_tri.at[1])
        far_part(0, share - 1, 1, late, recv_tri.at[1])
        gather_stats()
        far_part(1, share - 1, 1, late, recv_tri.at[1])

    @pl.when(place == 1)
    def _():
        gather_stats()

    await_part(back.at[pl.ds(0, hubs)], recv_tri.at[1])

    def by_member(chunk):
        sums = back[:, chunk_rows(chunk), :].astype(jnp.float32)
        return sums.reshape(hubs, share, CHUNK, col_count)

    def finish(chunk, carry):
        first = pl.multiple_of(chunk * CHUNK, CHUNK)
        sums = by_member(chunk)
        last = sums[:, share - 1 :]
        part = mean_part[chunk_rows(chunk), :]
        center = (part * known + jnp.sum(last, axis=(0, 1))) / hidden
        moved = part - center
        left_over = last - center
        squares = square_part[chunk_rows(chunk), :] + known * moved * moved
        squares = squares + jnp.sum(left_over * left_over, axis=(0, 1))
        scale = lax.rsqrt(squares / hidden + 1e-05)
        planes[:hidden, :CHUNK, :] = ((sums - center) * scale).reshape(hidden, CHUNK, col_count)

        def one_row(local, inner_carry):
            at = first + local
            tri_normed = wide[pl.ds(local, hidden, stride=PITCH), :].astype(jnp.bfloat16)
            projected = lax.dot_general(
                tri_normed, w_scaled[...], (((0,), (0,)), ((), ())), preferred_element_type=jnp.float32
            )
            out_ref[at] = (gates[at] * (projected + bias_row[...])).astype(jnp.bfloat16)
            return inner_carry

        lax.fori_loop(0, CHUNK, one_row, 0, unroll=FINISH_UNROLL)
        pltpu.make_async_copy(
            out_ref.at[chunk_rows(chunk)], out_hbm.at[chunk_rows(chunk)], store_sem
        ).start()
        return carry

    lax.fori_loop(0, chunks, finish, 0)
    pltpu.make_async_copy(out_ref, out_hbm, store_sem).wait()

    def sent_all(first, count, rows, sem):
        part = edges.at[pl.ds(0, count), pl.ds(first, rows), :]
        await_part(part, sem)

    sent_all(0, (hubs - 1) * share, row_count, send_left)
    sent_all(0, (hubs - 1) * late, row_count, send_right)
    sent_all(CHUNK, (hubs - 1) * early, row_count - CHUNK, send_right)

    @pl.when(place == 1)
    def _():
        sent_all(0, (hubs - 1) * shared, CHUNK, send_right)

    @pl.when(inner)
    def _():
        sent_all(0, (hubs - 1) * early, CHUNK, send_right)

    def given_all(count, spots):
        if spots > 1:
            await_part(tri.at[pl.ds(0, count), pl.ds(0, (spots - 1) * row_count), :], send_tri)
        await_part(tri.at[pl.ds(0, count), pl.ds(0, row_count), pl.ds(0, (ka_n - 1) * col_count)], send_tri)

    plane = zone * row_count
    await_part(right.at[:, pl.ds(0, plane), :], send_far)
    await_part(right.at[pl.ds(0, share - shared), pl.ds(0, plane), :], send_far)
    given_all(shared, zone)

    @pl.when(inner)
    def _():
        await_part(right.at[pl.ds(0, shared), pl.ds(0, 2 * plane), :], send_far)
        await_part(right.at[pl.ds(0, shared), pl.ds(0, 2 * plane), :], send_far)
        given_all(share - shared, group_rows)


def fused(rows_n, ka_n, args):
    pair_repr, pair_mask, ln_gain, ln_bias, w_proj, w_gate, w_out_gate, out_gain, out_bias, w_out = args
    row_count, col_count, chans = pair_repr.shape
    hidden = w_out.shape[0]
    share = hidden // (rows_n // 4 * ka_n)
    late = share - EARLY
    chunks = row_count // CHUNK
    half = jnp.bfloat16
    return pl.pallas_call(
        functools.partial(kernel, rows_n, ka_n, EARLY),
        out_shape=jax.ShapeDtypeStruct(pair_repr.shape, half),
        in_specs=[pl.BlockSpec(memory_space=pltpu.HBM)] * 10,
        out_specs=pl.BlockSpec(memory_space=pl.ANY),
        scratch_shapes=[
            pltpu.VMEM((row_count, col_count), jnp.int32),
            pltpu.VMEM((1, chans), jnp.float32),
            pltpu.VMEM((1, chans), jnp.float32),
            pltpu.VMEM((chans, 2 * hidden), half),
            pltpu.VMEM((chans, 2 * hidden), half),
            pltpu.VMEM((chans, chans), half),
            pltpu.VMEM((1, hidden), jnp.float32),
            pltpu.VMEM((1, hidden), jnp.float32),
            pltpu.VMEM((hidden, chans), half),
            pltpu.VMEM((row_count, col_count, chans), half),
            pltpu.VMEM((row_count, col_count, chans), half),
            pltpu.VMEM((2 * hidden, row_count, col_count), half),
            pltpu.VMEM((2 * hidden * PITCH, col_count), jnp.float32),
            pltpu.VMEM((row_count, col_count, chans), half),
            pltpu.VMEM((row_count, col_count, chans), jnp.float32),
            pltpu.VMEM((share, rows_n // 2 * row_count, ka_n * col_count), half),
            pltpu.VMEM((share, rows_n * row_count, ka_n * col_count), half),
            pltpu.VMEM((share, rows_n // 2 * row_count, ka_n * col_count), half),
            pltpu.VMEM((hidden, row_count, col_count), half),
            pltpu.VMEM((4 * hidden, chans), half),
            pltpu.VMEM((hidden, chans), half),
            pltpu.VMEM((1, chans), jnp.float32),
            pltpu.VMEM((row_count, col_count), jnp.float32),
            pltpu.VMEM((row_count, col_count), jnp.float32),
            pltpu.SemaphoreType.DMA((9,)),
            pltpu.SemaphoreType.DMA((chunks,)),
            pltpu.SemaphoreType.DMA,
            pltpu.SemaphoreType.DMA((2, 1 + late)),
            pltpu.SemaphoreType.DMA((2, chunks)),
            pltpu.SemaphoreType.DMA((chunks,)),
            pltpu.SemaphoreType.DMA,
            pltpu.SemaphoreType.DMA,
            pltpu.SemaphoreType.DMA((2, late)),
            pltpu.SemaphoreType.DMA((2, 1 + late)),
            pltpu.SemaphoreType.DMA((2,)),
            pltpu.SemaphoreType.DMA,
            pltpu.SemaphoreType.DMA,
            pltpu.SemaphoreType.DMA,
            pltpu.SemaphoreType.DMA,
        ],
        compiler_params=pltpu.CompilerParams(
            collective_id=0, has_side_effects=True, vmem_limit_bytes=42 * 2**20
        ),
    )(*[
        pltpu.with_memory_space_constraint(array, pltpu.HBM)
        for array in (
            pair_repr, pair_mask, ln_gain[None], ln_bias[None], w_proj, w_gate, w_out_gate,
            out_gain[None], out_bias[None], w_out,
        )
    ])


def plain(args):
    pair_repr, pair_mask, ln_gain, ln_bias, w_proj, w_gate, w_out_gate, out_gain, out_bias, w_out = args
    row_count, col_count, chans = pair_repr.shape
    hidden = w_out.shape[0]
    normed = layer_norm(pair_repr.astype(jnp.float32), ln_gain, ln_bias).astype(jnp.bfloat16)
    flat_rows = normed.reshape(row_count * col_count, chans)
    projected = jnp.dot(flat_rows, w_proj, preferred_element_type=jnp.float32)
    gate_logits = jnp.dot(flat_rows, w_gate, preferred_element_type=jnp.float32)
    mask_col = pair_mask.reshape(row_count * col_count, 1).astype(jnp.float32)
    edges = (jax.nn.sigmoid(gate_logits) * projected * mask_col).astype(jnp.bfloat16)
    edges = edges.reshape(row_count, col_count, 2 * hidden)
    partial_sums = jnp.einsum(
        "ikh,jkh->ijh",
        edges[:, :, :hidden],
        lax.all_gather(edges[:, :, hidden:], "rows", axis=0, tiled=True),
        preferred_element_type=jnp.float32,
    )
    triangle = lax.psum_scatter(
        partial_sums.astype(jnp.bfloat16), "ka", scatter_dimension=1, tiled=True
    ).astype(jnp.float32)
    tri_normed = layer_norm(triangle, out_gain, out_bias).astype(jnp.bfloat16)
    out_gate = jax.nn.sigmoid(jnp.dot(flat_rows, w_out_gate, preferred_element_type=jnp.float32))
    projected_out = jnp.dot(
        tri_normed.reshape(row_count * col_count, hidden), w_out, preferred_element_type=jnp.float32
    )
    return (out_gate * projected_out).astype(jnp.bfloat16).reshape(row_count, col_count, chans)


def body(rows_n, ka_n, *args):
    row_count, col_count, chans = args[0].shape
    hidden = args[-1].shape[0]
    hubs = rows_n // 4 * ka_n
    aligned = row_count % CHUNK == 0 and col_count % 128 == 0 and chans % 128 == 0 and hidden % 128 == 0
    if aligned and rows_n % 4 == 0 and ka_n % 4 == 0 and hidden % hubs == 0 and col_count == hidden:
        if hidden // hubs - EARLY > AHEAD and row_count > CHUNK:
            return fused(rows_n, ka_n, args)
    return plain(args)


def solution(mesh):
    placed = (P("rows", "ka", None), P("rows", "ka"), P(), P(), P(), P(), P(), P(), P(), P())
    return jax.shard_map(
        functools.partial(body, mesh.shape["rows"], mesh.shape["ka"]),
        mesh=mesh, in_specs=placed, out_specs=P("rows", "ka", None), check_vma=False,
    )
```

```python
import functools

import jax
import jax.numpy as jnp
from jax import lax
from jax.experimental import pallas as pl
from jax.experimental.pallas import tpu as pltpu
from jax.sharding import PartitionSpec as P

MESH = pl.DeviceIdType.MESH
CHUNK = 16
PITCH = 24
EARLY = 4
SHARED = 2
AHEAD = 3
MAKE_UNROLL = 8
GATE_UNROLL = 8
FINISH_UNROLL = 16


def layer_norm(values, gain_vec, bias_vec):
    center = jnp.mean(values, axis=-1, keepdims=True)
    deviate = values - center
    spread = jnp.mean(deviate * deviate, axis=-1, keepdims=True)
    return deviate * lax.rsqrt(spread + 1e-05) * gain_vec + bias_vec


def sigmoid(logits):
    return 0.5 + 0.5 * jnp.tanh(0.5 * logits)


def kernel(
    rows_n, ka_n, early,
    pair_hbm, mask_hbm, ln_gain_hbm, ln_bias_hbm, w_proj_hbm, w_gate_hbm, w_out_gate_hbm,
    out_gain_hbm, out_bias_hbm, w_out_hbm,
    out_ref,
    mask_ref, ln_gain_ref, ln_bias_ref, w_proj_ref, w_gate_ref, w_out_gate_ref,
    out_gain_ref, out_bias_ref, w_out_ref,
    pair_ref, edges, wide, normed, gates, left, right, tri, back, w_cat, w_scaled, bias_row,
    mean_part, square_part,
    small_sem, load_sem, recv_left, recv_first, recv_early, recv_own, recv_down, recv_right, recv_far, recv_tri,
    send_left, send_right, send_far, send_tri,
):
    row = lax.axis_index("rows")
    col = lax.axis_index("ka")
    row_count, col_count, chans = pair_ref.shape
    hidden = w_out_hbm.shape[0]
    zone = rows_n // 4
    group_rows = 2 * zone
    members = group_rows * ka_n
    hubs = zone * ka_n
    share = hidden // hubs
    late = share - early
    chunks = row_count // CHUNK
    ahead = AHEAD
    shared = SHARED

    quarter = row // zone
    lane = row % zone
    half = quarter // 2
    spot = row % group_rows
    hub_q = 1 + half
    far_q = 2 - half
    edge_q = 3 * half
    place = half * (quarter - 2) + (1 - half) * (1 - quarter)
    inner = place == 0
    member = lane * ka_n + col
    planes = wide.reshape(2 * hidden, PITCH, col_count)

    barrier = pltpu.get_barrier_semaphore()

    def hail(to_row, to_col):
        pl.semaphore_signal(barrier, inc=1, device_id=(to_row, to_col), device_id_type=MESH)

    def greet(step, carry):
        hail(half * group_rows + (spot + step % group_rows) % group_rows, (col + step // group_rows) % ka_n)
        return carry

    def greet_far(step, carry):
        hail(far_q * zone + step % zone, (col + step // zone) % ka_n)
        return carry

    def chunk_rows(chunk):
        return pl.ds(pl.multiple_of(chunk * CHUNK, CHUNK), CHUNK)

    def load(chunk):
        rows = chunk_rows(chunk)
        return pltpu.make_async_copy(pair_hbm.at[rows], pair_ref.at[rows], load_sem.at[chunk])

    smalls = [
        pltpu.make_async_copy(there, here, small_sem.at[at])
        for at, (there, here) in enumerate([
            (w_gate_hbm, w_gate_ref), (w_proj_hbm, w_proj_ref), (ln_gain_hbm, ln_gain_ref),
            (ln_bias_hbm, ln_bias_ref), (mask_hbm, mask_ref), (w_out_gate_hbm, w_out_gate_ref),
            (out_gain_hbm, out_gain_ref), (out_bias_hbm, out_bias_ref), (w_out_hbm, w_out_ref),
        ])
    ]
    smalls[0].start()
    smalls[1].start()
    load(0).start()
    for small in smalls[2:]:
        small.start()
    for chunk in range(1, chunks):
        load(chunk).start()

    @pl.when(inner)
    def _():
        lax.fori_loop(0, hubs, greet_far, 0)

    lax.fori_loop(1, members, greet, 0)

    def turned(ref):
        return ref[...].astype(jnp.float32).T.astype(jnp.bfloat16)

    smalls[0].wait()
    smalls[1].wait()
    gate_rows, proj_rows = turned(w_gate_ref), turned(w_proj_ref)
    w_cat[:hidden, :] = gate_rows[hidden:]
    w_cat[hidden : 2 * hidden, :] = proj_rows[hidden:]
    w_cat[2 * hidden : 3 * hidden, :] = gate_rows[:hidden]
    w_cat[3 * hidden :, :] = proj_rows[:hidden]

    own_cols = pl.ds(pl.multiple_of(col * col_count, 128), col_count)

    def left_ends(chan, count, first, size, to_member):
        return (
            edges.at[pl.ds(to_member * share + chan, count), pl.ds(first, size), :],
            left.at[pl.ds(chan, count), pl.ds(spot * row_count + first, size), own_cols],
        )

    def right_ends(chan, count, first, size, to_member):
        return (
            edges.at[pl.ds(hidden + to_member * share + chan, count), pl.ds(first, size), :],
            right.at[pl.ds(chan, count), pl.ds(row * row_count + first, size), own_cols],
        )

    def send_edges(ends, chan, count, first, size, sent, landed, to_q=None):
        def start(to_lane, to_col):
            here, there = ends(chan, count, first, size, to_lane * ka_n + to_col)
            pltpu.make_async_remote_copy(
                src_ref=here, dst_ref=there, send_sem=sent, recv_sem=landed,
                device_id=((quarter if to_q is None else to_q) * zone + to_lane, to_col), device_id_type=MESH,
            ).start()

        def other(step, carry):
            start((lane + step % zone) % zone, (col + step // zone) % ka_n)
            return carry

        if to_q is not None:
            lax.fori_loop(0, hubs, other, 0)
            return
        lax.fori_loop(1, hubs, other, 0)
        here, there = ends(chan, count, first, size, member)
        pltpu.make_async_copy(here, there, landed).start()

    def make_side(at, local, plain, first_row, first_chan):
        both = lax.dot_general(
            w_cat[first_row : first_row + 2 * hidden], plain, (((1,), (1,)), ((), ())),
            preferred_element_type=jnp.float32,
        )
        mask_row = mask_ref[pl.ds(at, 1), :].astype(jnp.float32)
        made = sigmoid(both[:hidden]) * both[hidden:] * mask_row
        wide[pl.ds(local + first_chan * PITCH, hidden, stride=PITCH), :] = made

    def normalise(at):
        values = pair_ref[at].astype(jnp.float32)
        plain = layer_norm(values, ln_gain_ref[...], ln_bias_ref[...]).astype(jnp.bfloat16)
        normed[at] = plain
        return plain

    def round_side(chunk, first_chan, count):
        some = pl.ds(first_chan, count)
        edges[some, chunk_rows(chunk), :] = planes[some, :CHUNK, :].astype(jnp.bfloat16)

    def make_first():
        load(0).wait()

        def right_row(at, carry):
            make_side(at, at, normalise(at), 0, hidden)
            return carry

        lax.fori_loop(0, CHUNK, right_row, 0, unroll=CHUNK)
        round_side(0, hidden, hidden)

    def make_first_left():
        def left_row(at, carry):
            make_side(at, at, normed[at], 2 * hidden, 0)
            return carry

        lax.fori_loop(0, CHUNK, left_row, 0, unroll=MAKE_UNROLL)
        round_side(0, 0, hidden)

    def make_chunk(chunk):
        load(chunk).wait()

        def one_row(local, carry):
            at = chunk * CHUNK + local
            plain = normalise(at)
            make_side(at, local, plain, 0, hidden)
            make_side(at, local, plain, 2 * hidden, 0)
            return carry

        lax.fori_loop(0, CHUNK, one_row, 0, unroll=MAKE_UNROLL)
        round_side(chunk, 0, 2 * hidden)

    def send_early_right(chunk):
        first = pl.multiple_of(chunk * CHUNK, CHUNK)

        @pl.when(inner)
        def _():
            send_edges(right_ends, 0, early, first, CHUNK, send_far, recv_far.at[0, 0], far_q)

        @pl.when((place == 1) & (chunk > 0))
        def _():
            send_edges(right_ends, 0, early, first, CHUNK, send_right, recv_first.at[0, chunk])

    def send_early_left(chunk):
        first = pl.multiple_of(chunk * CHUNK, CHUNK)

        @pl.when(place == 1)
        def _():
            send_edges(left_ends, 0, early, first, CHUNK, send_left, recv_first.at[1, chunk])

    def send_right_late(group):
        send_edges(right_ends, early + group, 1, 0, row_count, send_right, recv_right.at[0, group])

    def send_left_late(group):
        send_edges(left_ends, early + group, 1, 0, row_count, send_left, recv_left.at[0, 1 + group])

    def send_both(group, lead):
        send_right_late(group + lead)
        send_left_late(group)

    def await_part(part, landed):
        pltpu.make_async_copy(part, part, landed).wait()

    def pass_on(part, to_q, landed):
        pltpu.make_async_remote_copy(
            src_ref=part, dst_ref=part, send_sem=send_far, recv_sem=landed,
            device_id=(to_q * zone + lane, col), device_id_type=MESH,
        ).start()

    def right_rows(chan, count, first, size):
        return right.at[pl.ds(chan, count), pl.ds(pl.multiple_of(first, CHUNK), size), :]

    def left_rows(chan, count, from_q):
        first = pl.multiple_of(from_q % 2 * zone * row_count, CHUNK)
        return left.at[pl.ds(chan, count), pl.ds(first, zone * row_count), :]

    def pass_early(from_q, chunk, to_q, landed):
        for to_lane in range(zone):
            first = (from_q * zone + to_lane) * row_count + chunk * CHUNK
            pass_on(right_rows(0, early, first, CHUNK), to_q, landed)

    def pass_late(from_q, group, to_q, came, landed):
        part = right_rows(early + group, 1, from_q * zone * row_count, zone * row_count)
        await_part(part, came)
        pass_on(part, to_q, landed)

    def pass_left(chan, count, group):
        part = left_rows(chan, count, quarter)
        await_part(part, recv_left.at[0, group])
        pass_on(part, hub_q, recv_left.at[1, group])

    def climb_early(chunk):
        sizer = right_rows(0, early, 0, zone * CHUNK)

        @pl.when(chunk > 0)
        def _():
            await_part(sizer, recv_first.at[0, chunk])
            pass_early(quarter, chunk, hub_q, recv_early.at[chunk])

        await_part(sizer, recv_first.at[1, chunk])
        for to_lane in range(zone):
            first = (quarter % 2 * zone + to_lane) * row_count + chunk * CHUNK
            rows = pl.ds(pl.multiple_of(first, CHUNK), CHUNK)
            pass_on(left.at[pl.ds(shared, early - shared), rows, :], hub_q, recv_left.at[1, 0])

    def cross_early(chunk):
        await_part(right_rows(0, early, 0, zone * CHUNK), recv_early.at[chunk])
        pass_early(edge_q, chunk, far_q, recv_far.at[1, 0])

    def cross_near(group):
        pass_late(hub_q, group, far_q, recv_right.at[0, group], recv_far.at[0, 1 + group])

    def cross_edge(group):
        pass_late(edge_q, group, far_q, recv_right.at[1, group], recv_far.at[1, 1 + group])

    def climb_right(group):
        pass_late(edge_q, group, hub_q, recv_right.at[0, group], recv_right.at[1, group])

    def climb_left(group):
        pass_left(early + group, 1, 1 + group)

    def climb(group, carry):
        climb_right(group)
        climb_left(group - 1)
        return carry

    far_first = (1 - half) * group_rows * row_count
    own_first = pl.multiple_of(quarter % 2 * zone * row_count, CHUNK)

    j_block = zone * row_count
    col_block = ka_n // 4

    def multiply(chan, count, first, size, j_first, j_size):
        j_rows = pl.ds(pl.multiple_of(j_first, 128), j_size)

        def one_channel(at, carry):
            tri[at, pl.ds(first, size), j_rows] = lax.dot_general(
                left[at, pl.ds(first, size), :], right[at, j_rows, :], (((1,), (1,)), ((), ())),
                preferred_element_type=jnp.float32,
            ).astype(jnp.bfloat16)
            return carry

        lax.fori_loop(chan, chan + count, one_channel, 0)

    def give_all(chan, count, base, spots, me, col_first, col_size, landed):
        slot = back.at[pl.ds(member * share + chan, count)]

        def part(to_spot, to_col):
            first = (base - half * group_rows + to_spot) * row_count
            return tri.at[
                pl.ds(chan, count),
                pl.ds(pl.multiple_of(first, CHUNK), row_count),
                pl.ds(pl.multiple_of(to_col * col_count, 128), col_count),
            ]

        def give(step, carry):
            to_spot = (me + step % spots) % spots
            to_col = col_first + (col + step // spots) % col_size
            pltpu.make_async_remote_copy(
                src_ref=part(to_spot, to_col), dst_ref=slot, send_sem=send_tri, recv_sem=landed,
                device_id=(base + to_spot, to_col), device_id_type=MESH,
            ).start()
            return carry

        mine = (col >= col_first) & (col < col_first + col_size)

        @pl.when(mine)
        def _():
            pltpu.make_async_copy(part(me, col), slot, landed).start()

        @pl.when(jnp.logical_not(mine))
        def _():
            give(0, 0)

        lax.fori_loop(1, spots * col_size, give, 0)

    def block(chan, count, from_q, quarters, landed):
        multiply(chan, count, 0, group_rows * row_count, from_q * j_block, quarters * j_block)
        give_all(
            chan, count, half * group_rows, group_rows, spot, from_q * col_block, quarters * col_block, landed
        )

    def near_block(chan, count, group, landed):
        await_part(left_rows(chan, count, hub_q), recv_left.at[0, group])
        await_part(left_rows(chan, count, edge_q), recv_left.at[1, group])
        block(chan, count, 2 * half, 2, landed)

    def far_block(chan, count, group, landed):
        for where in range(2):
            far_part(where, chan, count, group, landed)

    def far_part(where, chan, count, group, landed):
        from_q = far_q if where == 0 else 3 * (1 - half)
        part = right_rows(chan, count, from_q * zone * row_count, zone * row_count)
        await_part(part, recv_far.at[where, group])
        block(chan, count, from_q, 1, landed)

    def own_triangle():
        multiply(0, shared, own_first, zone * row_count, 0, rows_n * row_count)
        give_all(0, shared, quarter * zone, zone, lane, 0, ka_n, recv_tri.at[0])

    known = hidden - hubs

    def gather_stats():
        await_part(back.at[pl.ds(0, known)], recv_tri.at[0])

        def one_chunk(chunk, carry):
            rows = chunk_rows(chunk)
            some = [
                back[at * share : at * share + share - 1, rows, :].astype(jnp.float32) for at in range(hubs)
            ]
            center = sum(jnp.sum(sums, axis=0) for sums in some) / known
            mean_part[rows, :] = center
            square_part[rows, :] = sum(
                jnp.sum((sums - center) * (sums - center), axis=0) for sums in some
            )
            return carry

        lax.fori_loop(0, chunks, one_chunk, 0)

    for small in smalls[2:]:
        small.wait()
    make_first()
    pl.semaphore_wait(barrier, members - 1 + hubs * (1 - place))

    @pl.when(place == 1)
    def _():
        send_edges(right_ends, 0, early, 0, CHUNK, send_far, recv_early.at[0], hub_q)
        send_edges(right_ends, 0, shared, 0, CHUNK, send_right, recv_first.at[0, 0])

    send_early_right(0)
    make_first_left()
    send_early_left(0)

    def rest(chunk, carry):
        make_chunk(chunk)
        send_early_right(chunk)
        send_early_left(chunk)

        @pl.when(place == 1)
        def _():
            climb_early(chunk - 1)

        return carry

    lax.fori_loop(1, chunks, rest, 0)

    @pl.when(place == 1)
    def _():
        send_right_late(0)
        send_both(0, 1)
        send_both(1, 1)
        climb_early(chunks - 1)
        send_both(2, 1)
        climb_right(0)
        send_both(3, 1)
        climb(1, 0)

        def both(group, carry):
            send_both(group, 1)
            return carry

        lax.fori_loop(4, late - 1, both, 0)
        send_left_late(late - 1)
        climb(2, 0)

    @pl.when(inner)
    def _():
        for group in range(ahead):
            send_right_late(group)
        send_edges(right_ends, 0, early, 0, row_count, send_right, recv_own)
        send_edges(left_ends, 0, early, 0, row_count, send_left, recv_left.at[0, 0])
        for chunk in range(chunks):
            cross_early(chunk)

            def both(group, carry):
                send_both(group, ahead)
                return carry

            span = late - ahead
            lax.fori_loop(span * chunk // chunks, span * (chunk + 1) // chunks, both, 0)
            if chunk < ahead:
                cross_near(chunk)
        for group in range(late - ahead, late):
            send_left_late(group)
        own_rows = hub_q * zone * row_count
        await_part(right_rows(0, early, own_rows, zone * row_count), recv_own)
        pass_on(right_rows(0, shared, own_rows, zone * row_count), edge_q, recv_down)

    weights = w_out_ref[...].astype(jnp.float32)
    gain_col = jnp.broadcast_to(out_gain_ref[...], (chans, hidden)).T
    bias_col = jnp.broadcast_to(out_bias_ref[...], (chans, hidden)).T
    w_scaled[...] = (weights * gain_col).astype(jnp.bfloat16)
    bias_row[...] = jnp.sum(weights * bias_col, axis=0, keepdims=True)

    def gate_row(at, carry):
        gates[at] = sigmoid(
            jnp.dot(normed[at], w_out_gate_ref[...], preferred_element_type=jnp.float32)
        )
        return carry

    lax.fori_loop(0, row_count, gate_row, 0, unroll=GATE_UNROLL)

    @pl.when(place == 1)
    def _():
        lax.fori_loop(3, late, climb, 0)
        climb_left(late - 1)
        await_part(right_rows(0, shared, 0, zone * CHUNK), recv_first.at[0, 0])
        await_part(right_rows(0, shared, 0, 3 * zone * row_count), recv_down)
        own_triangle()

    @pl.when(inner)
    def _():
        for group in range(min(chunks, ahead), ahead + 1):
            cross_near(group)
        cross_edge(0)
        await_part(left_rows(0, early, hub_q), recv_left.at[0, 0])
        await_part(left_rows(shared, early - shared, edge_q), recv_left.at[1, 0])
        for where, from_q in ((0, far_q), (1, 3 * (1 - half))):
            await_part(right_rows(0, early, from_q * zone * row_count, zone * row_count), recv_far.at[where, 0])
        pass_on(right_rows(0, shared, far_first, group_rows * row_count), edge_q, recv_down)
        own_triangle()
        block(shared, early - shared, 0, 4, recv_tri.at[0])

        def near_upto(group):
            return ahead + 1 + (late - ahead - 1) * group // (late - 1)

        def near_one(group, carry):
            cross_near(group)
            return carry

        def stage(group, carry):
            lax.fori_loop(near_upto(group - 1), near_upto(group), near_one, 0)
            cross_edge(group)
            near_block(early + group - 1, 1, group, recv_tri.at[0])
            far_block(early + group - 1, 1, group, recv_tri.at[0])
            return carry

        lax.fori_loop(1, late, stage, 0)
        near_block(share - 1, 1, late, recv_tri.at[1])
        far_part(0, share - 1, 1, late, recv_tri.at[1])
        gather_stats()
        far_part(1, share - 1, 1, late, recv_tri.at[1])

    @pl.when(place == 1)
    def _():
        gather_stats()

    await_part(back.at[pl.ds(0, hubs)], recv_tri.at[1])

    def by_member(chunk):
        sums = back[:, chunk_rows(chunk), :].astype(jnp.float32)
        return sums.reshape(hubs, share, CHUNK, col_count)

    def scale_chunk(chunk, first_plane):
        sums = by_member(chunk)
        last = sums[:, share - 1 :]
        part = mean_part[chunk_rows(chunk), :]
        center = (part * known + jnp.sum(last, axis=(0, 1))) / hidden
        moved = part - center
        left_over = last - center
        squares = square_part[chunk_rows(chunk), :] + known * moved * moved
        squares = squares + jnp.sum(left_over * left_over, axis=(0, 1))
        scale = lax.rsqrt(squares / hidden + 1e-05)
        planes[first_plane : first_plane + hidden, :CHUNK, :] = ((sums - center) * scale).reshape(hidden, CHUNK, col_count)

    def project_chunk(chunk, first_plane):
        def one_row(local, inner_carry):
            at = chunk * CHUNK + local
            tri_normed = wide[pl.ds(local + first_plane * PITCH, hidden, stride=PITCH), :].astype(jnp.bfloat16)
            projected = lax.dot_general(
                tri_normed, w_scaled[...], (((0,), (0,)), ((), ())), preferred_element_type=jnp.float32
            )
            out_ref[at] = (gates[at] * (projected + bias_row[...])).astype(jnp.bfloat16)
            return inner_carry

        lax.fori_loop(0, CHUNK, one_row, 0, unroll=FINISH_UNROLL)

    scale_chunk(0, 0)

    for chunk in range(chunks):
        if chunk + 1 < chunks:
            scale_chunk(chunk + 1, (chunk + 1) % 2 * hidden)
        project_chunk(chunk, chunk % 2 * hidden)

    def sent_all(first, count, rows, sem):
        part = edges.at[pl.ds(0, count), pl.ds(first, rows), :]
        await_part(part, sem)

    sent_all(0, (hubs - 1) * share, row_count, send_left)
    sent_all(0, (hubs - 1) * late, row_count, send_right)
    sent_all(CHUNK, (hubs - 1) * early, row_count - CHUNK, send_right)

    @pl.when(place == 1)
    def _():
        sent_all(0, (hubs - 1) * shared, CHUNK, send_right)

    @pl.when(inner)
    def _():
        sent_all(0, (hubs - 1) * early, CHUNK, send_right)

    def given_all(count, spots):
        if spots > 1:
            await_part(tri.at[pl.ds(0, count), pl.ds(0, (spots - 1) * row_count), :], send_tri)
        await_part(tri.at[pl.ds(0, count), pl.ds(0, row_count), pl.ds(0, (ka_n - 1) * col_count)], send_tri)

    plane = zone * row_count
    await_part(right.at[:, pl.ds(0, plane), :], send_far)
    await_part(right.at[pl.ds(0, share - shared), pl.ds(0, plane), :], send_far)
    given_all(shared, zone)

    @pl.when(inner)
    def _():
        await_part(right.at[pl.ds(0, shared), pl.ds(0, 2 * plane), :], send_far)
        await_part(right.at[pl.ds(0, shared), pl.ds(0, 2 * plane), :], send_far)
        given_all(share - shared, group_rows)


def fused(rows_n, ka_n, args):
    pair_repr, pair_mask, ln_gain, ln_bias, w_proj, w_gate, w_out_gate, out_gain, out_bias, w_out = args
    row_count, col_count, chans = pair_repr.shape
    hidden = w_out.shape[0]
    share = hidden // (rows_n // 4 * ka_n)
    late = share - EARLY
    chunks = row_count // CHUNK
    half = jnp.bfloat16
    return pl.pallas_call(
        functools.partial(kernel, rows_n, ka_n, EARLY),
        out_shape=jax.ShapeDtypeStruct(pair_repr.shape, half),
        in_specs=[pl.BlockSpec(memory_space=pltpu.HBM)] * 10,
        out_specs=pl.BlockSpec(memory_space=pltpu.VMEM),
        scratch_shapes=[
            pltpu.VMEM((row_count, col_count), jnp.int32),
            pltpu.VMEM((1, chans), jnp.float32),
            pltpu.VMEM((1, chans), jnp.float32),
            pltpu.VMEM((chans, 2 * hidden), half),
            pltpu.VMEM((chans, 2 * hidden), half),
            pltpu.VMEM((chans, chans), half),
            pltpu.VMEM((1, hidden), jnp.float32),
            pltpu.VMEM((1, hidden), jnp.float32),
            pltpu.VMEM((hidden, chans), half),
            pltpu.VMEM((row_count, col_count, chans), half),
            pltpu.VMEM((2 * hidden, row_count, col_count), half),
            pltpu.VMEM((2 * hidden * PITCH, col_count), jnp.float32),
            pltpu.VMEM((row_count, col_count, chans), half),
            pltpu.VMEM((row_count, col_count, chans), jnp.float32),
            pltpu.VMEM((share, rows_n // 2 * row_count, ka_n * col_count), half),
            pltpu.VMEM((share, rows_n * row_count, ka_n * col_count), half),
            pltpu.VMEM((share, rows_n // 2 * row_count, ka_n * col_count), half),
            pltpu.VMEM((hidden, row_count, col_count), half),
            pltpu.VMEM((4 * hidden, chans), half),
            pltpu.VMEM((hidden, chans), half),
            pltpu.VMEM((1, chans), jnp.float32),
            pltpu.VMEM((row_count, col_count), jnp.float32),
            pltpu.VMEM((row_count, col_count), jnp.float32),
            pltpu.SemaphoreType.DMA((9,)),
            pltpu.SemaphoreType.DMA((chunks,)),
            pltpu.SemaphoreType.DMA((2, 1 + late)),
            pltpu.SemaphoreType.DMA((2, chunks)),
            pltpu.SemaphoreType.DMA((chunks,)),
            pltpu.SemaphoreType.DMA,
            pltpu.SemaphoreType.DMA,
            pltpu.SemaphoreType.DMA((2, late)),
            pltpu.SemaphoreType.DMA((2, 1 + late)),
            pltpu.SemaphoreType.DMA((2,)),
            pltpu.SemaphoreType.DMA,
            pltpu.SemaphoreType.DMA,
            pltpu.SemaphoreType.DMA,
            pltpu.SemaphoreType.DMA,
        ],
        compiler_params=pltpu.CompilerParams(
            collective_id=0, has_side_effects=True, vmem_limit_bytes=42 * 2**20
        ),
    )(*[
        pltpu.with_memory_space_constraint(array, pltpu.HBM)
        for array in (
            pair_repr, pair_mask, ln_gain[None], ln_bias[None], w_proj, w_gate, w_out_gate,
            out_gain[None], out_bias[None], w_out,
        )
    ])


def plain(args):
    pair_repr, pair_mask, ln_gain, ln_bias, w_proj, w_gate, w_out_gate, out_gain, out_bias, w_out = args
    row_count, col_count, chans = pair_repr.shape
    hidden = w_out.shape[0]
    normed = layer_norm(pair_repr.astype(jnp.float32), ln_gain, ln_bias).astype(jnp.bfloat16)
    flat_rows = normed.reshape(row_count * col_count, chans)
    projected = jnp.dot(flat_rows, w_proj, preferred_element_type=jnp.float32)
    gate_logits = jnp.dot(flat_rows, w_gate, preferred_element_type=jnp.float32)
    mask_col = pair_mask.reshape(row_count * col_count, 1).astype(jnp.float32)
    edges = (jax.nn.sigmoid(gate_logits) * projected * mask_col).astype(jnp.bfloat16)
    edges = edges.reshape(row_count, col_count, 2 * hidden)
    partial_sums = jnp.einsum(
        "ikh,jkh->ijh",
        edges[:, :, :hidden],
        lax.all_gather(edges[:, :, hidden:], "rows", axis=0, tiled=True),
        preferred_element_type=jnp.float32,
    )
    triangle = lax.psum_scatter(
        partial_sums.astype(jnp.bfloat16), "ka", scatter_dimension=1, tiled=True
    ).astype(jnp.float32)
    tri_normed = layer_norm(triangle, out_gain, out_bias).astype(jnp.bfloat16)
    out_gate = jax.nn.sigmoid(jnp.dot(flat_rows, w_out_gate, preferred_element_type=jnp.float32))
    projected_out = jnp.dot(
        tri_normed.reshape(row_count * col_count, hidden), w_out, preferred_element_type=jnp.float32
    )
    return (out_gate * projected_out).astype(jnp.bfloat16).reshape(row_count, col_count, chans)


def body(rows_n, ka_n, *args):
    row_count, col_count, chans = args[0].shape
    hidden = args[-1].shape[0]
    hubs = rows_n // 4 * ka_n
    aligned = row_count % CHUNK == 0 and col_count % 128 == 0 and chans % 128 == 0 and hidden % 128 == 0
    if aligned and rows_n % 4 == 0 and ka_n % 4 == 0 and hidden % hubs == 0 and col_count == hidden:
        if hidden // hubs - EARLY > max(AHEAD, 5) and row_count > CHUNK:
            return fused(rows_n, ka_n, args)
    return plain(args)


def solution(mesh):
    placed = (P("rows", "ka", None), P("rows", "ka"), P(), P(), P(), P(), P(), P(), P(), P())
    return jax.shard_map(
        functools.partial(body, mesh.shape["rows"], mesh.shape["ka"]),
        mesh=mesh, in_specs=placed, out_specs=P("rows", "ka", None), check_vma=False,
    )
```

```python
import functools

import jax
import jax.numpy as jnp
from jax import lax
from jax.experimental import pallas as pl
from jax.experimental.pallas import tpu as pltpu
from jax.sharding import PartitionSpec as P

MESH = pl.DeviceIdType.MESH
CHUNK = 16
PITCH = 24
EARLY = 4
SHARED = 2
AHEAD = 3
MAKE_UNROLL = 8
GATE_UNROLL = 8
FINISH_UNROLL = 16


def layer_norm(values, gain_vec, bias_vec):
    center = jnp.mean(values, axis=-1, keepdims=True)
    deviate = values - center
    spread = jnp.mean(deviate * deviate, axis=-1, keepdims=True)
    return deviate * lax.rsqrt(spread + 1e-05) * gain_vec + bias_vec


def sigmoid(logits):
    return 0.5 + 0.5 * jnp.tanh(0.5 * logits)


def kernel(
    rows_n, ka_n, early,
    pair_hbm, mask_hbm, ln_gain_hbm, ln_bias_hbm, w_proj_hbm, w_gate_hbm, w_out_gate_hbm,
    out_gain_hbm, out_bias_hbm, w_out_hbm,
    out_ref,
    mask_ref, ln_gain_ref, ln_bias_ref, w_proj_ref, w_gate_ref, w_out_gate_ref,
    out_gain_ref, out_bias_ref, w_out_ref,
    pair_ref, edges, wide, normed, gates, left, right, tri, back, w_cat, w_scaled, bias_row, w_tail, acc,
    mean_part, square_part,
    small_sem, load_sem, recv_left, recv_first, recv_early, recv_own, recv_down, recv_right, recv_far, recv_tri,
    send_left, send_right, send_far, send_tri,
):
    row = lax.axis_index("rows")
    col = lax.axis_index("ka")
    row_count, col_count, chans = pair_ref.shape
    hidden = w_out_hbm.shape[0]
    zone = rows_n // 4
    group_rows = 2 * zone
    members = group_rows * ka_n
    hubs = zone * ka_n
    share = hidden // hubs
    late = share - early
    chunks = row_count // CHUNK
    ahead = AHEAD
    shared = SHARED

    quarter = row // zone
    lane = row % zone
    half = quarter // 2
    spot = row % group_rows
    hub_q = 1 + half
    far_q = 2 - half
    edge_q = 3 * half
    place = half * (quarter - 2) + (1 - half) * (1 - quarter)
    inner = place == 0
    member = lane * ka_n + col
    planes = wide.reshape(2 * hidden, PITCH, col_count)

    barrier = pltpu.get_barrier_semaphore()

    def hail(to_row, to_col):
        pl.semaphore_signal(barrier, inc=1, device_id=(to_row, to_col), device_id_type=MESH)

    def greet(step, carry):
        hail(half * group_rows + (spot + step % group_rows) % group_rows, (col + step // group_rows) % ka_n)
        return carry

    def greet_far(step, carry):
        hail(far_q * zone + step % zone, (col + step // zone) % ka_n)
        return carry

    def chunk_rows(chunk):
        return pl.ds(pl.multiple_of(chunk * CHUNK, CHUNK), CHUNK)

    def load(chunk):
        rows = chunk_rows(chunk)
        return pltpu.make_async_copy(pair_hbm.at[rows], pair_ref.at[rows], load_sem.at[chunk])

    smalls = [
        pltpu.make_async_copy(there, here, small_sem.at[at])
        for at, (there, here) in enumerate([
            (w_gate_hbm, w_gate_ref), (w_proj_hbm, w_proj_ref), (ln_gain_hbm, ln_gain_ref),
            (ln_bias_hbm, ln_bias_ref), (mask_hbm, mask_ref), (w_out_gate_hbm, w_out_gate_ref),
            (out_gain_hbm, out_gain_ref), (out_bias_hbm, out_bias_ref), (w_out_hbm, w_out_ref),
        ])
    ]
    smalls[0].start()
    smalls[1].start()
    load(0).start()
    for small in smalls[2:]:
        small.start()
    for chunk in range(1, chunks):
        load(chunk).start()

    @pl.when(inner)
    def _():
        lax.fori_loop(0, hubs, greet_far, 0)

    lax.fori_loop(1, members, greet, 0)

    def turned(ref):
        return ref[...].astype(jnp.float32).T.astype(jnp.bfloat16)

    smalls[0].wait()
    smalls[1].wait()
    gate_rows, proj_rows = turned(w_gate_ref), turned(w_proj_ref)
    w_cat[:hidden, :] = gate_rows[hidden:]
    w_cat[hidden : 2 * hidden, :] = proj_rows[hidden:]
    w_cat[2 * hidden : 3 * hidden, :] = gate_rows[:hidden]
    w_cat[3 * hidden :, :] = proj_rows[:hidden]

    own_cols = pl.ds(pl.multiple_of(col * col_count, 128), col_count)

    def left_ends(chan, count, first, size, to_member):
        return (
            edges.at[pl.ds(to_member * share + chan, count), pl.ds(first, size), :],
            left.at[pl.ds(chan, count), pl.ds(spot * row_count + first, size), own_cols],
        )

    def right_ends(chan, count, first, size, to_member):
        return (
            edges.at[pl.ds(hidden + to_member * share + chan, count), pl.ds(first, size), :],
            right.at[pl.ds(chan, count), pl.ds(row * row_count + first, size), own_cols],
        )

    def send_edges(ends, chan, count, first, size, sent, landed, to_q=None):
        def start(to_lane, to_col):
            here, there = ends(chan, count, first, size, to_lane * ka_n + to_col)
            pltpu.make_async_remote_copy(
                src_ref=here, dst_ref=there, send_sem=sent, recv_sem=landed,
                device_id=((quarter if to_q is None else to_q) * zone + to_lane, to_col), device_id_type=MESH,
            ).start()

        def other(step, carry):
            start((lane + step % zone) % zone, (col + step // zone) % ka_n)
            return carry

        if to_q is not None:
            lax.fori_loop(0, hubs, other, 0)
            return
        lax.fori_loop(1, hubs, other, 0)
        here, there = ends(chan, count, first, size, member)
        pltpu.make_async_copy(here, there, landed).start()

    def make_side(at, local, plain, first_row, first_chan):
        both = lax.dot_general(
            w_cat[first_row : first_row + 2 * hidden], plain, (((1,), (1,)), ((), ())),
            preferred_element_type=jnp.float32,
        )
        mask_row = mask_ref[pl.ds(at, 1), :].astype(jnp.float32)
        made = sigmoid(both[:hidden]) * both[hidden:] * mask_row
        wide[pl.ds(local + first_chan * PITCH, hidden, stride=PITCH), :] = made

    def normalise(at):
        values = pair_ref[at].astype(jnp.float32)
        plain = layer_norm(values, ln_gain_ref[...], ln_bias_ref[...]).astype(jnp.bfloat16)
        normed[at] = plain
        return plain

    def round_side(chunk, first_chan, count):
        some = pl.ds(first_chan, count)
        edges[some, chunk_rows(chunk), :] = planes[some, :CHUNK, :].astype(jnp.bfloat16)

    def make_first():
        load(0).wait()

        def right_row(at, carry):
            make_side(at, at, normalise(at), 0, hidden)
            return carry

        lax.fori_loop(0, CHUNK, right_row, 0, unroll=CHUNK)
        round_side(0, hidden, hidden)

    def make_first_left():
        def left_row(at, carry):
            make_side(at, at, normed[at], 2 * hidden, 0)
            return carry

        lax.fori_loop(0, CHUNK, left_row, 0, unroll=MAKE_UNROLL)
        round_side(0, 0, hidden)

    def make_chunk(chunk):
        load(chunk).wait()

        def one_row(local, carry):
            at = chunk * CHUNK + local
            plain = normalise(at)
            make_side(at, local, plain, 0, hidden)
            make_side(at, local, plain, 2 * hidden, 0)
            return carry

        lax.fori_loop(0, CHUNK, one_row, 0, unroll=MAKE_UNROLL)
        round_side(chunk, 0, 2 * hidden)

    def send_early_right(chunk):
        first = pl.multiple_of(chunk * CHUNK, CHUNK)

        @pl.when(inner)
        def _():
            send_edges(right_ends, 0, early, first, CHUNK, send_far, recv_far.at[0, 0], far_q)

        @pl.when((place == 1) & (chunk > 0))
        def _():
            send_edges(right_ends, 0, early, first, CHUNK, send_right, recv_first.at[0, chunk])

    def send_early_left(chunk):
        first = pl.multiple_of(chunk * CHUNK, CHUNK)

        @pl.when(place == 1)
        def _():
            send_edges(left_ends, 0, early, first, CHUNK, send_left, recv_first.at[1, chunk])

    def send_right_late(group):
        send_edges(right_ends, early + group, 1, 0, row_count, send_right, recv_right.at[0, group])

    def send_left_late(group):
        send_edges(left_ends, early + group, 1, 0, row_count, send_left, recv_left.at[0, 1 + group])

    def send_both(group, lead):
        send_right_late(group + lead)
        send_left_late(group)

    def await_part(part, landed):
        pltpu.make_async_copy(part, part, landed).wait()

    def pass_on(part, to_q, landed):
        pltpu.make_async_remote_copy(
            src_ref=part, dst_ref=part, send_sem=send_far, recv_sem=landed,
            device_id=(to_q * zone + lane, col), device_id_type=MESH,
        ).start()

    def right_rows(chan, count, first, size):
        return right.at[pl.ds(chan, count), pl.ds(pl.multiple_of(first, CHUNK), size), :]

    def left_rows(chan, count, from_q):
        first = pl.multiple_of(from_q % 2 * zone * row_count, CHUNK)
        return left.at[pl.ds(chan, count), pl.ds(first, zone * row_count), :]

    def pass_early(from_q, chunk, to_q, landed):
        for to_lane in range(zone):
            first = (from_q * zone + to_lane) * row_count + chunk * CHUNK
            pass_on(right_rows(0, early, first, CHUNK), to_q, landed)

    def pass_late(from_q, group, to_q, came, landed):
        part = right_rows(early + group, 1, from_q * zone * row_count, zone * row_count)
        await_part(part, came)
        pass_on(part, to_q, landed)

    def pass_left(chan, count, group):
        part = left_rows(chan, count, quarter)
        await_part(part, recv_left.at[0, group])
        pass_on(part, hub_q, recv_left.at[1, group])

    def climb_early(chunk):
        sizer = right_rows(0, early, 0, zone * CHUNK)

        @pl.when(chunk > 0)
        def _():
            await_part(sizer, recv_first.at[0, chunk])
            pass_early(quarter, chunk, hub_q, recv_early.at[chunk])

        await_part(sizer, recv_first.at[1, chunk])
        for to_lane in range(zone):
            first = (quarter % 2 * zone + to_lane) * row_count + chunk * CHUNK
            rows = pl.ds(pl.multiple_of(first, CHUNK), CHUNK)
            pass_on(left.at[pl.ds(shared, early - shared), rows, :], hub_q, recv_left.at[1, 0])

    def cross_early(chunk):
        await_part(right_rows(0, early, 0, zone * CHUNK), recv_early.at[chunk])
        pass_early(edge_q, chunk, far_q, recv_far.at[1, 0])

    def cross_near(group):
        pass_late(hub_q, group, far_q, recv_right.at[0, group], recv_far.at[0, 1 + group])

    def cross_edge(group):
        pass_late(edge_q, group, far_q, recv_right.at[1, group], recv_far.at[1, 1 + group])

    def climb_right(group):
        pass_late(edge_q, group, hub_q, recv_right.at[0, group], recv_right.at[1, group])

    def climb_left(group):
        pass_left(early + group, 1, 1 + group)

    def climb(group, carry):
        climb_right(group)
        climb_left(group - 1)
        return carry

    far_first = (1 - half) * group_rows * row_count
    own_first = pl.multiple_of(quarter % 2 * zone * row_count, CHUNK)

    j_block = zone * row_count
    col_block = ka_n // 4

    def multiply(chan, count, first, size, j_first, j_size):
        j_rows = pl.ds(pl.multiple_of(j_first, 128), j_size)

        def one_channel(at, carry):
            tri[at, pl.ds(first, size), j_rows] = lax.dot_general(
                left[at, pl.ds(first, size), :], right[at, j_rows, :], (((1,), (1,)), ((), ())),
                preferred_element_type=jnp.float32,
            ).astype(jnp.bfloat16)
            return carry

        lax.fori_loop(chan, chan + count, one_channel, 0)

    def give_all(chan, count, base, spots, me, col_first, col_size, landed):
        slot = back.at[pl.ds(member * share + chan, count)]

        def part(to_spot, to_col):
            first = (base - half * group_rows + to_spot) * row_count
            return tri.at[
                pl.ds(chan, count),
                pl.ds(pl.multiple_of(first, CHUNK), row_count),
                pl.ds(pl.multiple_of(to_col * col_count, 128), col_count),
            ]

        def give(step, carry):
            to_spot = (me + step % spots) % spots
            to_col = col_first + (col + step // spots) % col_size
            pltpu.make_async_remote_copy(
                src_ref=part(to_spot, to_col), dst_ref=slot, send_sem=send_tri, recv_sem=landed,
                device_id=(base + to_spot, to_col), device_id_type=MESH,
            ).start()
            return carry

        mine = (col >= col_first) & (col < col_first + col_size)

        @pl.when(mine)
        def _():
            pltpu.make_async_copy(part(me, col), slot, landed).start()

        @pl.when(jnp.logical_not(mine))
        def _():
            give(0, 0)

        lax.fori_loop(1, spots * col_size, give, 0)

    def block(chan, count, from_q, quarters, landed):
        multiply(chan, count, 0, group_rows * row_count, from_q * j_block, quarters * j_block)
        give_all(
            chan, count, half * group_rows, group_rows, spot, from_q * col_block, quarters * col_block, landed
        )

    def near_block(chan, count, group, landed):
        await_part(left_rows(chan, count, hub_q), recv_left.at[0, group])
        await_part(left_rows(chan, count, edge_q), recv_left.at[1, group])
        block(chan, count, 2 * half, 2, landed)

    def far_block(chan, count, group, landed):
        for where in range(2):
            far_part(where, chan, count, group, landed)

    def far_part(where, chan, count, group, landed):
        from_q = far_q if where == 0 else 3 * (1 - half)
        part = right_rows(chan, count, from_q * zone * row_count, zone * row_count)
        await_part(part, recv_far.at[where, group])
        block(chan, count, from_q, 1, landed)

    def own_triangle():
        multiply(0, shared, own_first, zone * row_count, 0, rows_n * row_count)
        give_all(0, shared, quarter * zone, zone, lane, 0, ka_n, recv_tri.at[0])

    known = hidden - hubs

    def gather_stats():
        await_part(back.at[pl.ds(0, known)], recv_tri.at[0])

        def one_chunk(chunk, carry):
            rows = chunk_rows(chunk)
            some = [
                back[at * share : at * share + share - 1, rows, :].astype(jnp.float32) for at in range(hubs)
            ]
            center = sum(jnp.sum(sums, axis=0) for sums in some) / known
            mean_part[rows, :] = center
            square_part[rows, :] = sum(
                jnp.sum((sums - center) * (sums - center), axis=0) for sums in some
            )
            return carry

        lax.fori_loop(0, chunks, one_chunk, 0)

    for small in smalls[2:]:
        small.wait()
    make_first()
    pl.semaphore_wait(barrier, members - 1 + hubs * (1 - place))

    @pl.when(place == 1)
    def _():
        send_edges(right_ends, 0, early, 0, CHUNK, send_far, recv_early.at[0], hub_q)
        send_edges(right_ends, 0, shared, 0, CHUNK, send_right, recv_first.at[0, 0])

    send_early_right(0)
    make_first_left()
    send_early_left(0)

    def rest(chunk, carry):
        make_chunk(chunk)
        send_early_right(chunk)
        send_early_left(chunk)

        @pl.when(place == 1)
        def _():
            climb_early(chunk - 1)

        return carry

    lax.fori_loop(1, chunks, rest, 0)

    @pl.when(place == 1)
    def _():
        send_right_late(0)
        send_both(0, 1)
        send_both(1, 1)
        climb_early(chunks - 1)
        send_both(2, 1)
        climb_right(0)
        send_both(3, 1)
        climb(1, 0)

        def both(group, carry):
            send_both(group, 1)
            return carry

        lax.fori_loop(4, late - 1, both, 0)
        send_left_late(late - 1)
        climb(2, 0)

    @pl.when(inner)
    def _():
        for group in range(ahead):
            send_right_late(group)
        send_edges(right_ends, 0, early, 0, row_count, send_right, recv_own)
        send_edges(left_ends, 0, early, 0, row_count, send_left, recv_left.at[0, 0])
        for chunk in range(chunks):
            cross_early(chunk)

            def both(group, carry):
                send_both(group, ahead)
                return carry

            span = late - ahead
            lax.fori_loop(span * chunk // chunks, span * (chunk + 1) // chunks, both, 0)
            if chunk < ahead:
                cross_near(chunk)
        for group in range(late - ahead, late):
            send_left_late(group)
        own_rows = hub_q * zone * row_count
        await_part(right_rows(0, early, own_rows, zone * row_count), recv_own)
        pass_on(right_rows(0, shared, own_rows, zone * row_count), edge_q, recv_down)

    weights = w_out_ref[...].astype(jnp.float32)
    gain_col = jnp.broadcast_to(out_gain_ref[...], (chans, hidden)).T
    bias_col = jnp.broadcast_to(out_bias_ref[...], (chans, hidden)).T
    w_scaled[...] = (weights * gain_col).astype(jnp.bfloat16)
    bias_row[...] = jnp.sum(weights * bias_col, axis=0, keepdims=True)

    def parts_of(values):
        high = values.astype(jnp.bfloat16).astype(jnp.float32)
        middle = (values - high).astype(jnp.bfloat16).astype(jnp.float32)
        return high, middle, values - high - middle

    rounded = w_scaled[...].astype(jnp.float32)
    high, middle, low = parts_of(-jnp.sum(rounded, axis=0, keepdims=True))
    none, one = jnp.zeros_like(high), jnp.ones_like(high)
    late_rows = [rounded[at * share + share - 1 : at * share + share] for at in range(hubs)]
    rows_plain = late_rows + [high, middle, low, high, middle, high, none, none]
    rows_scale = [none] * (hubs + 6) + [one, one]
    w_tail[...] = jnp.concatenate(
        [jnp.concatenate(rows_plain, axis=0), jnp.concatenate(rows_scale, axis=0)], axis=1
    ).astype(jnp.bfloat16)

    def gate_row(at, carry):
        gates[at] = sigmoid(
            jnp.dot(normed[at], w_out_gate_ref[...], preferred_element_type=jnp.float32)
        )
        return carry

    lax.fori_loop(0, row_count, gate_row, 0, unroll=GATE_UNROLL)

    @pl.when(place == 1)
    def _():
        lax.fori_loop(3, late, climb, 0)
        climb_left(late - 1)
        await_part(right_rows(0, shared, 0, zone * CHUNK), recv_first.at[0, 0])
        await_part(right_rows(0, shared, 0, 3 * zone * row_count), recv_down)
        own_triangle()

    @pl.when(inner)
    def _():
        for group in range(min(chunks, ahead), ahead + 1):
            cross_near(group)
        cross_edge(0)
        await_part(left_rows(0, early, hub_q), recv_left.at[0, 0])
        await_part(left_rows(shared, early - shared, edge_q), recv_left.at[1, 0])
        for where, from_q in ((0, far_q), (1, 3 * (1 - half))):
            await_part(right_rows(0, early, from_q * zone * row_count, zone * row_count), recv_far.at[where, 0])
        pass_on(right_rows(0, shared, far_first, group_rows * row_count), edge_q, recv_down)
        own_triangle()
        block(shared, early - shared, 0, 4, recv_tri.at[0])

        def near_upto(group):
            return ahead + 1 + (late - ahead - 1) * group // (late - 1)

        def near_one(group, carry):
            cross_near(group)
            return carry

        def stage(group, carry):
            lax.fori_loop(near_upto(group - 1), near_upto(group), near_one, 0)
            cross_edge(group)
            near_block(early + group - 1, 1, group, recv_tri.at[0])
            far_block(early + group - 1, 1, group, recv_tri.at[0])
            return carry

        lax.fori_loop(1, late, stage, 0)
        near_block(share - 1, 1, late, recv_tri.at[1])
        far_part(0, share - 1, 1, late, recv_tri.at[1])
        gather_stats()
        far_part(1, share - 1, 1, late, recv_tri.at[1])

    @pl.when(place == 1)
    def _():
        gather_stats()

    def lay_known(chunk, base):
        for at in range(hubs):
            first, size = at * share, share - 1
            planes[base + first : base + first + size, :CHUNK, :] = (
                back[first : first + size, chunk_rows(chunk), :].astype(jnp.float32)
            )
            planes[base + first + size, :CHUNK, :] = jnp.zeros((CHUNK, col_count), jnp.float32)

    def project_known(chunk, base):
        def one_row(local, carry):
            sums = wide[pl.ds(local + base * PITCH, hidden, stride=PITCH), :].astype(jnp.bfloat16)
            acc[chunk * CHUNK + local] = lax.dot_general(
                sums, w_scaled[...], (((0,), (0,)), ((), ())), preferred_element_type=jnp.float32
            )
            return carry

        lax.fori_loop(0, CHUNK, one_row, 0, unroll=FINISH_UNROLL)

    def lay_last(chunk, base):
        rows = chunk_rows(chunk)
        last = [back[at * share + share - 1, rows, :].astype(jnp.float32) for at in range(hubs)]
        part = mean_part[rows, :]
        center = (part * known + sum(last)) / hidden
        moved = part - center
        squares = square_part[rows, :] + known * moved * moved
        squares = squares + sum((sums - center) * (sums - center) for sums in last)
        high, middle, low = parts_of(center)
        scale, scale_rest, _ = parts_of(lax.rsqrt(squares / hidden + 1e-05))
        stack = last + [high, high, high, middle, middle, low, scale, scale_rest]
        for at, plane in enumerate(stack):
            planes[base + at, :CHUNK, :] = plane

    def project_last(chunk, base):
        def one_row(local, carry):
            at = chunk * CHUNK + local
            stack = wide[pl.ds(local + base * PITCH, hubs + 8, stride=PITCH), :].astype(jnp.bfloat16)
            tail = lax.dot_general(
                stack, w_tail[...], (((0,), (0,)), ((), ())), preferred_element_type=jnp.float32
            )
            projected = (acc[at] + tail[:, :chans]) * tail[:, chans:] + bias_row[...]
            out_ref[at] = (gates[at] * projected).astype(jnp.bfloat16)
            return carry

        lax.fori_loop(0, CHUNK, one_row, 0, unroll=FINISH_UNROLL)

    def in_turns(lay, project):
        lay(0, 0)
        for chunk in range(chunks):
            if chunk + 1 < chunks:
                lay(chunk + 1, (chunk + 1) % 2 * hidden)
            project(chunk, chunk % 2 * hidden)

    in_turns(lay_known, project_known)
    await_part(back.at[pl.ds(0, hubs)], recv_tri.at[1])
    in_turns(lay_last, project_last)

    def sent_all(first, count, rows, sem):
        part = edges.at[pl.ds(0, count), pl.ds(first, rows), :]
        await_part(part, sem)

    sent_all(0, (hubs - 1) * share, row_count, send_left)
    sent_all(0, (hubs - 1) * late, row_count, send_right)
    sent_all(CHUNK, (hubs - 1) * early, row_count - CHUNK, send_right)

    @pl.when(place == 1)
    def _():
        sent_all(0, (hubs - 1) * shared, CHUNK, send_right)

    @pl.when(inner)
    def _():
        sent_all(0, (hubs - 1) * early, CHUNK, send_right)

    def given_all(count, spots):
        if spots > 1:
            await_part(tri.at[pl.ds(0, count), pl.ds(0, (spots - 1) * row_count), :], send_tri)
        await_part(tri.at[pl.ds(0, count), pl.ds(0, row_count), pl.ds(0, (ka_n - 1) * col_count)], send_tri)

    plane = zone * row_count
    await_part(right.at[:, pl.ds(0, plane), :], send_far)
    await_part(right.at[pl.ds(0, share - shared), pl.ds(0, plane), :], send_far)
    given_all(shared, zone)

    @pl.when(inner)
    def _():
        await_part(right.at[pl.ds(0, shared), pl.ds(0, 2 * plane), :], send_far)
        await_part(right.at[pl.ds(0, shared), pl.ds(0, 2 * plane), :], send_far)
        given_all(share - shared, group_rows)


def fused(rows_n, ka_n, args):
    pair_repr, pair_mask, ln_gain, ln_bias, w_proj, w_gate, w_out_gate, out_gain, out_bias, w_out = args
    row_count, col_count, chans = pair_repr.shape
    hidden = w_out.shape[0]
    share = hidden // (rows_n // 4 * ka_n)
    late = share - EARLY
    chunks = row_count // CHUNK
    half = jnp.bfloat16
    return pl.pallas_call(
        functools.partial(kernel, rows_n, ka_n, EARLY),
        out_shape=jax.ShapeDtypeStruct(pair_repr.shape, half),
        in_specs=[pl.BlockSpec(memory_space=pltpu.HBM)] * 10,
        out_specs=pl.BlockSpec(memory_space=pltpu.VMEM),
        scratch_shapes=[
            pltpu.VMEM((row_count, col_count), jnp.int32),
            pltpu.VMEM((1, chans), jnp.float32),
            pltpu.VMEM((1, chans), jnp.float32),
            pltpu.VMEM((chans, 2 * hidden), half),
            pltpu.VMEM((chans, 2 * hidden), half),
            pltpu.VMEM((chans, chans), half),
            pltpu.VMEM((1, hidden), jnp.float32),
            pltpu.VMEM((1, hidden), jnp.float32),
            pltpu.VMEM((hidden, chans), half),
            pltpu.VMEM((row_count, col_count, chans), half),
            pltpu.VMEM((2 * hidden, row_count, col_count), half),
            pltpu.VMEM((2 * hidden * PITCH, col_count), jnp.float32),
            pltpu.VMEM((row_count, col_count, chans), half),
            pltpu.VMEM((row_count, col_count, chans), jnp.float32),
            pltpu.VMEM((share, rows_n // 2 * row_count, ka_n * col_count), half),
            pltpu.VMEM((share, rows_n * row_count, ka_n * col_count), half),
            pltpu.VMEM((share, rows_n // 2 * row_count, ka_n * col_count), half),
            pltpu.VMEM((hidden, row_count, col_count), half),
            pltpu.VMEM((4 * hidden, chans), half),
            pltpu.VMEM((hidden, chans), half),
            pltpu.VMEM((1, chans), jnp.float32),
            pltpu.VMEM((hidden // share + 8, 2 * chans), half),
            pltpu.VMEM((row_count, col_count, chans), jnp.float32),
            pltpu.VMEM((row_count, col_count), jnp.float32),
            pltpu.VMEM((row_count, col_count), jnp.float32),
            pltpu.SemaphoreType.DMA((9,)),
            pltpu.SemaphoreType.DMA((chunks,)),
            pltpu.SemaphoreType.DMA((2, 1 + late)),
            pltpu.SemaphoreType.DMA((2, chunks)),
            pltpu.SemaphoreType.DMA((chunks,)),
            pltpu.SemaphoreType.DMA,
            pltpu.SemaphoreType.DMA,
            pltpu.SemaphoreType.DMA((2, late)),
            pltpu.SemaphoreType.DMA((2, 1 + late)),
            pltpu.SemaphoreType.DMA((2,)),
            pltpu.SemaphoreType.DMA,
            pltpu.SemaphoreType.DMA,
            pltpu.SemaphoreType.DMA,
            pltpu.SemaphoreType.DMA,
        ],
        compiler_params=pltpu.CompilerParams(
            collective_id=0, has_side_effects=True, vmem_limit_bytes=42 * 2**20
        ),
    )(*[
        pltpu.with_memory_space_constraint(array, pltpu.HBM)
        for array in (
            pair_repr, pair_mask, ln_gain[None], ln_bias[None], w_proj, w_gate, w_out_gate,
            out_gain[None], out_bias[None], w_out,
        )
    ])


def plain(args):
    pair_repr, pair_mask, ln_gain, ln_bias, w_proj, w_gate, w_out_gate, out_gain, out_bias, w_out = args
    row_count, col_count, chans = pair_repr.shape
    hidden = w_out.shape[0]
    normed = layer_norm(pair_repr.astype(jnp.float32), ln_gain, ln_bias).astype(jnp.bfloat16)
    flat_rows = normed.reshape(row_count * col_count, chans)
    projected = jnp.dot(flat_rows, w_proj, preferred_element_type=jnp.float32)
    gate_logits = jnp.dot(flat_rows, w_gate, preferred_element_type=jnp.float32)
    mask_col = pair_mask.reshape(row_count * col_count, 1).astype(jnp.float32)
    edges = (jax.nn.sigmoid(gate_logits) * projected * mask_col).astype(jnp.bfloat16)
    edges = edges.reshape(row_count, col_count, 2 * hidden)
    partial_sums = jnp.einsum(
        "ikh,jkh->ijh",
        edges[:, :, :hidden],
        lax.all_gather(edges[:, :, hidden:], "rows", axis=0, tiled=True),
        preferred_element_type=jnp.float32,
    )
    triangle = lax.psum_scatter(
        partial_sums.astype(jnp.bfloat16), "ka", scatter_dimension=1, tiled=True
    ).astype(jnp.float32)
    tri_normed = layer_norm(triangle, out_gain, out_bias).astype(jnp.bfloat16)
    out_gate = jax.nn.sigmoid(jnp.dot(flat_rows, w_out_gate, preferred_element_type=jnp.float32))
    projected_out = jnp.dot(
        tri_normed.reshape(row_count * col_count, hidden), w_out, preferred_element_type=jnp.float32
    )
    return (out_gate * projected_out).astype(jnp.bfloat16).reshape(row_count, col_count, chans)


def body(rows_n, ka_n, *args):
    row_count, col_count, chans = args[0].shape
    hidden = args[-1].shape[0]
    hubs = rows_n // 4 * ka_n
    aligned = row_count % CHUNK == 0 and col_count % 128 == 0 and chans % 128 == 0 and hidden % 128 == 0
    if aligned and rows_n % 4 == 0 and ka_n % 4 == 0 and hidden % hubs == 0 and col_count == hidden:
        if hidden // hubs - EARLY > max(AHEAD, 5) and row_count > CHUNK:
            return fused(rows_n, ka_n, args)
    return plain(args)


def solution(mesh):
    placed = (P("rows", "ka", None), P("rows", "ka"), P(), P(), P(), P(), P(), P(), P(), P())
    return jax.shard_map(
        functools.partial(body, mesh.shape["rows"], mesh.shape["ka"]),
        mesh=mesh, in_specs=placed, out_specs=P("rows", "ka", None), check_vma=False,
    )
```

```python
import functools

import jax
import jax.numpy as jnp
from jax import lax
from jax.experimental import pallas as pl
from jax.experimental.pallas import tpu as pltpu
from jax.sharding import PartitionSpec as P

MESH = pl.DeviceIdType.MESH
CHUNK = 16
PITCH = 24
EARLY = 4
SHARED = 2
AHEAD = 3
MAKE_UNROLL = 8
GATE_UNROLL = 8
FINISH_UNROLL = 16


def layer_norm(values, gain_vec, bias_vec):
    center = jnp.mean(values, axis=-1, keepdims=True)
    deviate = values - center
    spread = jnp.mean(deviate * deviate, axis=-1, keepdims=True)
    return deviate * lax.rsqrt(spread + 1e-05) * gain_vec + bias_vec


def sigmoid(logits):
    return 0.5 + 0.5 * jnp.tanh(0.5 * logits)


def kernel(
    rows_n, ka_n, early,
    pair_hbm, mask_hbm, ln_gain_hbm, ln_bias_hbm, w_proj_hbm, w_gate_hbm, w_out_gate_hbm,
    out_gain_hbm, out_bias_hbm, w_out_hbm,
    out_ref,
    mask_ref, ln_gain_ref, ln_bias_ref, w_proj_ref, w_gate_ref, w_out_gate_ref,
    out_gain_ref, out_bias_ref, w_out_ref,
    pair_ref, edges, wide, normed, gates, left, right, tri, back, w_cat, w_scaled, bias_row, w_tail, acc,
    mean_part, square_part,
    small_sem, load_sem, recv_left, recv_first, recv_early, recv_own, recv_down, recv_right, recv_far, recv_tri,
    send_left, send_right, send_far, send_tri,
):
    row = lax.axis_index("rows")
    col = lax.axis_index("ka")
    row_count, col_count, chans = pair_ref.shape
    hidden = w_out_hbm.shape[0]
    zone = rows_n // 4
    group_rows = 2 * zone
    members = group_rows * ka_n
    hubs = zone * ka_n
    share = hidden // hubs
    late = share - early
    chunks = row_count // CHUNK
    ahead = AHEAD
    shared = SHARED

    quarter = row // zone
    lane = row % zone
    half = quarter // 2
    spot = row % group_rows
    hub_q = 1 + half
    far_q = 2 - half
    edge_q = 3 * half
    place = half * (quarter - 2) + (1 - half) * (1 - quarter)
    inner = place == 0
    member = lane * ka_n + col
    planes = wide.reshape(2 * hidden, PITCH, col_count)

    barrier = pltpu.get_barrier_semaphore()

    def hail(to_row, to_col):
        pl.semaphore_signal(barrier, inc=1, device_id=(to_row, to_col), device_id_type=MESH)

    def greet(step, carry):
        hail(half * group_rows + (spot + step % group_rows) % group_rows, (col + step // group_rows) % ka_n)
        return carry

    def greet_far(step, carry):
        hail(far_q * zone + step % zone, (col + step // zone) % ka_n)
        return carry

    def chunk_rows(chunk):
        return pl.ds(pl.multiple_of(chunk * CHUNK, CHUNK), CHUNK)

    def load(chunk):
        rows = chunk_rows(chunk)
        return pltpu.make_async_copy(pair_hbm.at[rows], pair_ref.at[rows], load_sem.at[chunk])

    smalls = [
        pltpu.make_async_copy(there, here, small_sem.at[at])
        for at, (there, here) in enumerate([
            (w_gate_hbm, w_gate_ref), (w_proj_hbm, w_proj_ref), (ln_gain_hbm, ln_gain_ref),
            (ln_bias_hbm, ln_bias_ref), (mask_hbm, mask_ref), (w_out_gate_hbm, w_out_gate_ref),
            (out_gain_hbm, out_gain_ref), (out_bias_hbm, out_bias_ref), (w_out_hbm, w_out_ref),
        ])
    ]
    smalls[0].start()
    smalls[1].start()
    load(0).start()
    for small in smalls[2:]:
        small.start()
    for chunk in range(1, chunks):
        load(chunk).start()

    @pl.when(inner)
    def _():
        lax.fori_loop(0, hubs, greet_far, 0)

    lax.fori_loop(1, members, greet, 0)

    def turned(ref):
        return ref[...].astype(jnp.float32).T.astype(jnp.bfloat16)

    smalls[0].wait()
    smalls[1].wait()
    gate_rows, proj_rows = turned(w_gate_ref), turned(w_proj_ref)
    w_cat[:hidden, :] = gate_rows[hidden:]
    w_cat[hidden : 2 * hidden, :] = proj_rows[hidden:]
    w_cat[2 * hidden : 3 * hidden, :] = gate_rows[:hidden]
    w_cat[3 * hidden :, :] = proj_rows[:hidden]

    own_cols = pl.ds(pl.multiple_of(col * col_count, 128), col_count)

    def left_ends(chan, count, first, size, to_member):
        return (
            edges.at[pl.ds(to_member * share + chan, count), pl.ds(first, size), :],
            left.at[pl.ds(chan, count), pl.ds(spot * row_count + first, size), own_cols],
        )

    def right_ends(chan, count, first, size, to_member):
        return (
            edges.at[pl.ds(hidden + to_member * share + chan, count), pl.ds(first, size), :],
            right.at[pl.ds(chan, count), pl.ds(row * row_count + first, size), own_cols],
        )

    def send_edges(ends, chan, count, first, size, sent, landed, to_q=None):
        def start(to_lane, to_col):
            here, there = ends(chan, count, first, size, to_lane * ka_n + to_col)
            pltpu.make_async_remote_copy(
                src_ref=here, dst_ref=there, send_sem=sent, recv_sem=landed,
                device_id=((quarter if to_q is None else to_q) * zone + to_lane, to_col), device_id_type=MESH,
            ).start()

        def other(step, carry):
            start((lane + step % zone) % zone, (col + step // zone) % ka_n)
            return carry

        if to_q is not None:
            lax.fori_loop(0, hubs, other, 0)
            return
        lax.fori_loop(1, hubs, other, 0)
        here, there = ends(chan, count, first, size, member)
        pltpu.make_async_copy(here, there, landed).start()

    def make_side(at, local, plain, first_row, first_chan):
        both = lax.dot_general(
            w_cat[first_row : first_row + 2 * hidden], plain, (((1,), (1,)), ((), ())),
            preferred_element_type=jnp.float32,
        )
        mask_row = mask_ref[pl.ds(at, 1), :].astype(jnp.float32)
        made = sigmoid(both[:hidden]) * both[hidden:] * mask_row
        wide[pl.ds(local + first_chan * PITCH, hidden, stride=PITCH), :] = made

    def normalise(at):
        values = pair_ref[at].astype(jnp.float32)
        plain = layer_norm(values, ln_gain_ref[...], ln_bias_ref[...]).astype(jnp.bfloat16)
        normed[at] = plain
        return plain

    def round_side(chunk, first_chan, count):
        some = pl.ds(first_chan, count)
        edges[some, chunk_rows(chunk), :] = planes[some, :CHUNK, :].astype(jnp.bfloat16)

    def make_first():
        load(0).wait()

        def right_row(at, carry):
            make_side(at, at, normalise(at), 0, hidden)
            return carry

        lax.fori_loop(0, CHUNK, right_row, 0, unroll=CHUNK)
        round_side(0, hidden, hidden)

    def make_first_left():
        def left_row(at, carry):
            make_side(at, at, normed[at], 2 * hidden, 0)
            return carry

        lax.fori_loop(0, CHUNK, left_row, 0, unroll=MAKE_UNROLL)
        round_side(0, 0, hidden)

    def make_chunk(chunk):
        load(chunk).wait()

        def one_row(local, carry):
            at = chunk * CHUNK + local
            plain = normalise(at)
            both = lax.dot_general(
                w_cat[...], plain, (((1,), (1,)), ((), ())), preferred_element_type=jnp.float32
            )
            mask_row = mask_ref[pl.ds(at, 1), :].astype(jnp.float32)
            right_made = sigmoid(both[:hidden]) * both[hidden : 2 * hidden] * mask_row
            left_made = sigmoid(both[2 * hidden : 3 * hidden]) * both[3 * hidden :] * mask_row
            wide[pl.ds(local + hidden * PITCH, hidden, stride=PITCH), :] = right_made
            wide[pl.ds(local, hidden, stride=PITCH), :] = left_made
            return carry

        lax.fori_loop(0, CHUNK, one_row, 0, unroll=MAKE_UNROLL)
        round_side(chunk, 0, 2 * hidden)

    def send_early_right(chunk):
        first = pl.multiple_of(chunk * CHUNK, CHUNK)

        @pl.when(inner)
        def _():
            send_edges(right_ends, 0, early, first, CHUNK, send_far, recv_far.at[0], far_q)

        @pl.when((place == 1) & (chunk > 0))
        def _():
            send_edges(right_ends, 0, early, first, CHUNK, send_right, recv_first.at[0, chunk])

    def send_early_left(chunk):
        first = pl.multiple_of(chunk * CHUNK, CHUNK)

        @pl.when(place == 1)
        def _():
            send_edges(left_ends, 0, early, first, CHUNK, send_left, recv_first.at[1, chunk])

    def send_right_late(group):
        send_edges(right_ends, early + group, 1, 0, row_count, send_right, recv_right.at[0, group])

    def send_left_late(group):
        send_edges(left_ends, early + group, 1, 0, row_count, send_left, recv_left.at[0, 1 + group])

    def send_both(group, lead):
        send_right_late(group + lead)
        send_left_late(group)

    def await_part(part, landed):
        pltpu.make_async_copy(part, part, landed).wait()

    def pass_on(part, to_q, landed):
        pltpu.make_async_remote_copy(
            src_ref=part, dst_ref=part, send_sem=send_far, recv_sem=landed,
            device_id=(to_q * zone + lane, col), device_id_type=MESH,
        ).start()

    def right_rows(chan, count, first, size):
        return right.at[pl.ds(chan, count), pl.ds(pl.multiple_of(first, CHUNK), size), :]

    def left_rows(chan, count, from_q):
        first = pl.multiple_of(from_q % 2 * zone * row_count, CHUNK)
        return left.at[pl.ds(chan, count), pl.ds(first, zone * row_count), :]

    def pass_early(from_q, chunk, to_q, landed):
        for to_lane in range(zone):
            first = (from_q * zone + to_lane) * row_count + chunk * CHUNK
            pass_on(right_rows(0, early, first, CHUNK), to_q, landed)

    def pass_late(from_q, group, to_q, came, landed):
        part = right_rows(early + group, 1, from_q * zone * row_count, zone * row_count)
        await_part(part, came)
        pass_on(part, to_q, landed)

    def pass_left(chan, count, group):
        part = left_rows(chan, count, quarter)
        await_part(part, recv_left.at[0, group])
        pass_on(part, hub_q, recv_left.at[1, group])

    def climb_early(chunk):
        sizer = right_rows(0, early, 0, zone * CHUNK)

        @pl.when(chunk > 0)
        def _():
            await_part(sizer, recv_first.at[0, chunk])
            pass_early(quarter, chunk, hub_q, recv_early.at[chunk])

        await_part(sizer, recv_first.at[1, chunk])
        for to_lane in range(zone):
            first = (quarter % 2 * zone + to_lane) * row_count + chunk * CHUNK
            rows = pl.ds(pl.multiple_of(first, CHUNK), CHUNK)
            pass_on(left.at[pl.ds(shared, early - shared), rows, :], hub_q, recv_left.at[1, 0])

    def cross_early(chunk):
        await_part(right_rows(0, early, 0, zone * CHUNK), recv_early.at[chunk])
        pass_early(edge_q, chunk, far_q, recv_far.at[0])

    def cross_near(group):
        pass_late(hub_q, group, far_q, recv_right.at[0, group], recv_far.at[1 + group])

    def cross_edge(group):
        pass_late(edge_q, group, far_q, recv_right.at[1, group], recv_far.at[1 + group + group // (late - 1)])

    def climb_right(group):
        pass_late(edge_q, group, hub_q, recv_right.at[0, group], recv_right.at[1, group])

    def climb_left(group):
        pass_left(early + group, 1, 1 + group)

    def climb(group, carry):
        climb_right(group)
        climb_left(group - 1)
        return carry

    far_first = (1 - half) * group_rows * row_count
    own_first = pl.multiple_of(quarter % 2 * zone * row_count, CHUNK)

    j_block = zone * row_count
    col_block = ka_n // 4

    def multiply(chan, count, first, size, j_first, j_size):
        j_rows = pl.ds(pl.multiple_of(j_first, 128), j_size)

        def one_channel(at, carry):
            tri[at, pl.ds(first, size), j_rows] = lax.dot_general(
                left[at, pl.ds(first, size), :], right[at, j_rows, :], (((1,), (1,)), ((), ())),
                preferred_element_type=jnp.float32,
            ).astype(jnp.bfloat16)
            return carry

        lax.fori_loop(chan, chan + count, one_channel, 0)

    def give_all(chan, count, base, spots, me, col_first, col_size, landed):
        slot = back.at[pl.ds(member * share + chan, count)]

        def part(to_spot, to_col):
            first = (base - half * group_rows + to_spot) * row_count
            return tri.at[
                pl.ds(chan, count),
                pl.ds(pl.multiple_of(first, CHUNK), row_count),
                pl.ds(pl.multiple_of(to_col * col_count, 128), col_count),
            ]

        def give(step, carry):
            to_spot = (me + step % spots) % spots
            to_col = col_first + (col + step // spots) % col_size
            pltpu.make_async_remote_copy(
                src_ref=part(to_spot, to_col), dst_ref=slot, send_sem=send_tri, recv_sem=landed,
                device_id=(base + to_spot, to_col), device_id_type=MESH,
            ).start()
            return carry

        mine = (col >= col_first) & (col < col_first + col_size)

        @pl.when(mine)
        def _():
            pltpu.make_async_copy(part(me, col), slot, landed).start()

        @pl.when(jnp.logical_not(mine))
        def _():
            give(0, 0)

        lax.fori_loop(1, spots * col_size, give, 0)

    def block(chan, count, from_q, quarters, landed):
        multiply(chan, count, 0, group_rows * row_count, from_q * j_block, quarters * j_block)
        give_all(
            chan, count, half * group_rows, group_rows, spot, from_q * col_block, quarters * col_block, landed
        )

    def near_block(chan, count, group, landed):
        await_part(left_rows(chan, count, hub_q), recv_left.at[0, group])
        await_part(left_rows(chan, count, edge_q), recv_left.at[1, group])
        block(chan, count, 2 * half, 2, landed)

    def far_block(chan, count, group, landed):
        await_part(right_rows(chan, count, far_first, group_rows * row_count), recv_far.at[group])
        block(chan, count, 2 * (1 - half), 2, landed)

    def far_part(where, chan, count, group, landed):
        from_q = far_q if where == 0 else 3 * (1 - half)
        part = right_rows(chan, count, from_q * zone * row_count, zone * row_count)
        await_part(part, recv_far.at[group])
        block(chan, count, from_q, 1, landed)

    def own_triangle():
        multiply(0, shared, own_first, zone * row_count, 0, rows_n * row_count)
        give_all(0, shared, quarter * zone, zone, lane, 0, ka_n, recv_tri.at[0])

    known = hidden - hubs

    def gather_stats():
        await_part(back.at[pl.ds(0, known)], recv_tri.at[0])

        def one_chunk(chunk, carry):
            rows = chunk_rows(chunk)
            some = [
                back[at * share : at * share + share - 1, rows, :].astype(jnp.float32) for at in range(hubs)
            ]
            center = sum(jnp.sum(sums, axis=0) for sums in some) / known
            mean_part[rows, :] = center
            square_part[rows, :] = sum(
                jnp.sum((sums - center) * (sums - center), axis=0) for sums in some
            )
            return carry

        lax.fori_loop(0, chunks, one_chunk, 0)

    for small in smalls[2:]:
        small.wait()
    make_first()
    pl.semaphore_wait(barrier, members - 1 + hubs * (1 - place))

    @pl.when(place == 1)
    def _():
        send_edges(right_ends, 0, early, 0, CHUNK, send_far, recv_early.at[0], hub_q)
        send_edges(right_ends, 0, shared, 0, CHUNK, send_right, recv_first.at[0, 0])

    send_early_right(0)
    make_first_left()
    send_early_left(0)

    def rest(chunk, carry):
        make_chunk(chunk)
        send_early_right(chunk)
        send_early_left(chunk)

        @pl.when(place == 1)
        def _():
            climb_early(chunk - 1)

        return carry

    lax.fori_loop(1, chunks, rest, 0)

    @pl.when(place == 1)
    def _():
        send_right_late(0)
        send_both(0, 1)
        send_both(1, 1)
        climb_early(chunks - 1)
        send_both(2, 1)
        climb_right(0)
        send_both(3, 1)
        climb(1, 0)

        def both(group, carry):
            send_both(group, 1)
            return carry

        lax.fori_loop(4, late - 1, both, 0)
        send_left_late(late - 1)
        climb(2, 0)

    @pl.when(inner)
    def _():
        for group in range(ahead):
            send_right_late(group)
        send_edges(right_ends, 0, early, 0, row_count, send_right, recv_own)
        send_edges(left_ends, 0, early, 0, row_count, send_left, recv_left.at[0, 0])
        for chunk in range(chunks):
            cross_early(chunk)

            def both(group, carry):
                send_both(group, ahead)
                return carry

            span = late - ahead
            lax.fori_loop(span * chunk // chunks, span * (chunk + 1) // chunks, both, 0)
            if chunk < ahead:
                cross_near(chunk)
        for group in range(late - ahead, late):
            send_left_late(group)
        own_rows = hub_q * zone * row_count
        await_part(right_rows(0, early, own_rows, zone * row_count), recv_own)
        pass_on(right_rows(0, shared, own_rows, zone * row_count), edge_q, recv_down)

    weights = w_out_ref[...].astype(jnp.float32)
    gain_col = jnp.broadcast_to(out_gain_ref[...], (chans, hidden)).T
    bias_col = jnp.broadcast_to(out_bias_ref[...], (chans, hidden)).T
    w_scaled[...] = (weights * gain_col).astype(jnp.bfloat16)
    bias_row[...] = jnp.sum(weights * bias_col, axis=0, keepdims=True)

    def parts_of(values):
        high = values.astype(jnp.bfloat16).astype(jnp.float32)
        middle = (values - high).astype(jnp.bfloat16).astype(jnp.float32)
        return high, middle, values - high - middle

    rounded = w_scaled[...].astype(jnp.float32)
    high, middle, low = parts_of(-jnp.sum(rounded, axis=0, keepdims=True))
    none, one = jnp.zeros_like(high), jnp.ones_like(high)
    late_rows = [rounded[at * share + share - 1 : at * share + share] for at in range(hubs)]
    rows_plain = late_rows + [high, middle, low, high, middle, high, none, none]
    rows_scale = [none] * (hubs + 6) + [one, one]
    w_tail[...] = jnp.concatenate(
        [jnp.concatenate(rows_plain, axis=0), jnp.concatenate(rows_scale, axis=0)], axis=1
    ).astype(jnp.bfloat16)

    def gate_row(at, carry):
        gates[at] = sigmoid(
            jnp.dot(normed[at], w_out_gate_ref[...], preferred_element_type=jnp.float32)
        )
        return carry

    lax.fori_loop(0, row_count, gate_row, 0, unroll=GATE_UNROLL)

    @pl.when(place == 1)
    def _():
        lax.fori_loop(3, late, climb, 0)
        climb_left(late - 1)
        await_part(right_rows(0, shared, 0, zone * CHUNK), recv_first.at[0, 0])
        await_part(right_rows(0, shared, 0, 3 * zone * row_count), recv_down)
        own_triangle()

    @pl.when(inner)
    def _():
        for group in range(min(chunks, ahead), ahead + 1):
            cross_near(group)
        cross_edge(0)
        await_part(left_rows(0, early, hub_q), recv_left.at[0, 0])
        await_part(left_rows(shared, early - shared, edge_q), recv_left.at[1, 0])
        await_part(right_rows(0, early, far_first, group_rows * row_count), recv_far.at[0])
        pass_on(right_rows(0, shared, far_first, group_rows * row_count), edge_q, recv_down)
        own_triangle()
        block(shared, early - shared, 0, 4, recv_tri.at[0])

        def near_upto(group):
            return ahead + 1 + (late - ahead - 1) * group // (late - 1)

        def near_one(group, carry):
            cross_near(group)
            return carry

        def stage(group, carry):
            lax.fori_loop(near_upto(group - 1), near_upto(group), near_one, 0)
            cross_edge(group)
            near_block(early + group - 1, 1, group, recv_tri.at[0])
            far_block(early + group - 1, 1, group, recv_tri.at[0])
            return carry

        lax.fori_loop(1, late, stage, 0)
        near_block(share - 1, 1, late, recv_tri.at[1])
        far_part(0, share - 1, 1, late, recv_tri.at[1])
        gather_stats()
        far_part(1, share - 1, 1, late + 1, recv_tri.at[1])

    @pl.when(place == 1)
    def _():
        gather_stats()

    def lay_known(chunk, base):
        for at in range(hubs):
            first, size = at * share, share - 1
            planes[base + first : base + first + size, :CHUNK, :] = (
                back[first : first + size, chunk_rows(chunk), :].astype(jnp.float32)
            )
            planes[base + first + size, :CHUNK, :] = jnp.zeros((CHUNK, col_count), jnp.float32)

    def project_known(chunk, base):
        def one_row(local, carry):
            sums = wide[pl.ds(local + base * PITCH, hidden, stride=PITCH), :].astype(jnp.bfloat16)
            acc[chunk * CHUNK + local] = lax.dot_general(
                sums, w_scaled[...], (((0,), (0,)), ((), ())), preferred_element_type=jnp.float32
            )
            return carry

        lax.fori_loop(0, CHUNK, one_row, 0, unroll=FINISH_UNROLL)

    def lay_last(chunk, base):
        rows = chunk_rows(chunk)
        last = [back[at * share + share - 1, rows, :].astype(jnp.float32) for at in range(hubs)]
        part = mean_part[rows, :]
        center = (part * known + sum(last)) / hidden
        moved = part - center
        squares = square_part[rows, :] + known * moved * moved
        squares = squares + sum((sums - center) * (sums - center) for sums in last)
        high, middle, low = parts_of(center)
        scale, scale_rest, _ = parts_of(lax.rsqrt(squares / hidden + 1e-05))
        stack = last + [high, high, high, middle, middle, low, scale, scale_rest]
        for at, plane in enumerate(stack):
            planes[base + at, :CHUNK, :] = plane

    def project_last(chunk, base):
        def one_row(local, carry):
            at = chunk * CHUNK + local
            stack = wide[pl.ds(local + base * PITCH, hubs + 8, stride=PITCH), :].astype(jnp.bfloat16)
            tail = lax.dot_general(
                stack, w_tail[...], (((0,), (0,)), ((), ())), preferred_element_type=jnp.float32
            )
            projected = (acc[at] + tail[:, :chans]) * tail[:, chans:] + bias_row[...]
            out_ref[at] = (gates[at] * projected).astype(jnp.bfloat16)
            return carry

        lax.fori_loop(0, CHUNK, one_row, 0, unroll=FINISH_UNROLL)

    def in_turns(lay, project):
        lay(0, 0)
        for chunk in range(chunks):
            if chunk + 1 < chunks:
                lay(chunk + 1, (chunk + 1) % 2 * hidden)
            project(chunk, chunk % 2 * hidden)

    in_turns(lay_known, project_known)
    await_part(back.at[pl.ds(0, hubs)], recv_tri.at[1])
    in_turns(lay_last, project_last)

    def sent_all(first, count, rows, sem):
        part = edges.at[pl.ds(0, count), pl.ds(first, rows), :]
        await_part(part, sem)

    sent_all(0, (hubs - 1) * share, row_count, send_left)
    sent_all(0, (hubs - 1) * late, row_count, send_right)
    sent_all(CHUNK, (hubs - 1) * early, row_count - CHUNK, send_right)

    @pl.when(place == 1)
    def _():
        sent_all(0, (hubs - 1) * shared, CHUNK, send_right)

    @pl.when(inner)
    def _():
        sent_all(0, (hubs - 1) * early, CHUNK, send_right)

    def given_all(count, spots):
        if spots > 1:
            await_part(tri.at[pl.ds(0, count), pl.ds(0, (spots - 1) * row_count), :], send_tri)
        await_part(tri.at[pl.ds(0, count), pl.ds(0, row_count), pl.ds(0, (ka_n - 1) * col_count)], send_tri)

    plane = zone * row_count
    await_part(right.at[:, pl.ds(0, plane), :], send_far)
    await_part(right.at[pl.ds(0, share - shared), pl.ds(0, plane), :], send_far)
    given_all(shared, zone)

    @pl.when(inner)
    def _():
        await_part(right.at[pl.ds(0, shared), pl.ds(0, 2 * plane), :], send_far)
        await_part(right.at[pl.ds(0, shared), pl.ds(0, 2 * plane), :], send_far)
        given_all(share - shared, group_rows)


def fused(rows_n, ka_n, args):
    pair_repr, pair_mask, ln_gain, ln_bias, w_proj, w_gate, w_out_gate, out_gain, out_bias, w_out = args
    row_count, col_count, chans = pair_repr.shape
    hidden = w_out.shape[0]
    share = hidden // (rows_n // 4 * ka_n)
    late = share - EARLY
    chunks = row_count // CHUNK
    half = jnp.bfloat16
    return pl.pallas_call(
        functools.partial(kernel, rows_n, ka_n, EARLY),
        out_shape=jax.ShapeDtypeStruct(pair_repr.shape, half),
        in_specs=[pl.BlockSpec(memory_space=pltpu.HBM)] * 10,
        out_specs=pl.BlockSpec(memory_space=pltpu.VMEM),
        scratch_shapes=[
            pltpu.VMEM((row_count, col_count), jnp.int32),
            pltpu.VMEM((1, chans), jnp.float32),
            pltpu.VMEM((1, chans), jnp.float32),
            pltpu.VMEM((chans, 2 * hidden), half),
            pltpu.VMEM((chans, 2 * hidden), half),
            pltpu.VMEM((chans, chans), half),
            pltpu.VMEM((1, hidden), jnp.float32),
            pltpu.VMEM((1, hidden), jnp.float32),
            pltpu.VMEM((hidden, chans), half),
            pltpu.VMEM((row_count, col_count, chans), half),
            pltpu.VMEM((2 * hidden, row_count, col_count), half),
            pltpu.VMEM((2 * hidden * PITCH, col_count), jnp.float32),
            pltpu.VMEM((row_count, col_count, chans), half),
            pltpu.VMEM((row_count, col_count, chans), jnp.float32),
            pltpu.VMEM((share, rows_n // 2 * row_count, ka_n * col_count), half),
            pltpu.VMEM((share, rows_n * row_count, ka_n * col_count), half),
            pltpu.VMEM((share, rows_n // 2 * row_count, ka_n * col_count), half),
            pltpu.VMEM((hidden, row_count, col_count), half),
            pltpu.VMEM((4 * hidden, chans), half),
            pltpu.VMEM((hidden, chans), half),
            pltpu.VMEM((1, chans), jnp.float32),
            pltpu.VMEM((hidden // share + 8, 2 * chans), half),
            pltpu.VMEM((row_count, col_count, chans), jnp.float32),
            pltpu.VMEM((row_count, col_count), jnp.float32),
            pltpu.VMEM((row_count, col_count), jnp.float32),
            pltpu.SemaphoreType.DMA((9,)),
            pltpu.SemaphoreType.DMA((chunks,)),
            pltpu.SemaphoreType.DMA((2, 1 + late)),
            pltpu.SemaphoreType.DMA((2, chunks)),
            pltpu.SemaphoreType.DMA((chunks,)),
            pltpu.SemaphoreType.DMA,
            pltpu.SemaphoreType.DMA,
            pltpu.SemaphoreType.DMA((2, late)),
            pltpu.SemaphoreType.DMA((2 + late,)),
            pltpu.SemaphoreType.DMA((2,)),
            pltpu.SemaphoreType.DMA,
            pltpu.SemaphoreType.DMA,
            pltpu.SemaphoreType.DMA,
            pltpu.SemaphoreType.DMA,
        ],
        compiler_params=pltpu.CompilerParams(
            collective_id=0, has_side_effects=True, vmem_limit_bytes=42 * 2**20
        ),
    )(*[
        pltpu.with_memory_space_constraint(array, pltpu.HBM)
        for array in (
            pair_repr, pair_mask, ln_gain[None], ln_bias[None], w_proj, w_gate, w_out_gate,
            out_gain[None], out_bias[None], w_out,
        )
    ])


def plain(args):
    pair_repr, pair_mask, ln_gain, ln_bias, w_proj, w_gate, w_out_gate, out_gain, out_bias, w_out = args
    row_count, col_count, chans = pair_repr.shape
    hidden = w_out.shape[0]
    normed = layer_norm(pair_repr.astype(jnp.float32), ln_gain, ln_bias).astype(jnp.bfloat16)
    flat_rows = normed.reshape(row_count * col_count, chans)
    projected = jnp.dot(flat_rows, w_proj, preferred_element_type=jnp.float32)
    gate_logits = jnp.dot(flat_rows, w_gate, preferred_element_type=jnp.float32)
    mask_col = pair_mask.reshape(row_count * col_count, 1).astype(jnp.float32)
    edges = (jax.nn.sigmoid(gate_logits) * projected * mask_col).astype(jnp.bfloat16)
    edges = edges.reshape(row_count, col_count, 2 * hidden)
    partial_sums = jnp.einsum(
        "ikh,jkh->ijh",
        edges[:, :, :hidden],
        lax.all_gather(edges[:, :, hidden:], "rows", axis=0, tiled=True),
        preferred_element_type=jnp.float32,
    )
    triangle = lax.psum_scatter(
        partial_sums.astype(jnp.bfloat16), "ka", scatter_dimension=1, tiled=True
    ).astype(jnp.float32)
    tri_normed = layer_norm(triangle, out_gain, out_bias).astype(jnp.bfloat16)
    out_gate = jax.nn.sigmoid(jnp.dot(flat_rows, w_out_gate, preferred_element_type=jnp.float32))
    projected_out = jnp.dot(
        tri_normed.reshape(row_count * col_count, hidden), w_out, preferred_element_type=jnp.float32
    )
    return (out_gate * projected_out).astype(jnp.bfloat16).reshape(row_count, col_count, chans)


def body(rows_n, ka_n, *args):
    row_count, col_count, chans = args[0].shape
    hidden = args[-1].shape[0]
    hubs = rows_n // 4 * ka_n
    aligned = row_count % CHUNK == 0 and col_count % 128 == 0 and chans % 128 == 0 and hidden % 128 == 0
    if aligned and rows_n % 4 == 0 and ka_n % 4 == 0 and hidden % hubs == 0 and col_count == hidden:
        if hidden // hubs - EARLY > max(AHEAD, 5) and row_count > CHUNK:
            return fused(rows_n, ka_n, args)
    return plain(args)


def solution(mesh):
    placed = (P("rows", "ka", None), P("rows", "ka"), P(), P(), P(), P(), P(), P(), P(), P())
    return jax.shard_map(
        functools.partial(body, mesh.shape["rows"], mesh.shape["ka"]),
        mesh=mesh, in_specs=placed, out_specs=P("rows", "ka", None), check_vma=False,
    )
```

```python
import functools

import jax
import jax.numpy as jnp
from jax import lax
from jax.experimental import pallas as pl
from jax.experimental.pallas import tpu as pltpu
from jax.sharding import PartitionSpec as P

MESH = pl.DeviceIdType.MESH
CHUNK = 16
PITCH = 24
EARLY = 4
SHARED = 2
AHEAD = 3
MAKE_UNROLL = 8
GATE_UNROLL = 8
FINISH_UNROLL = 16


def layer_norm(values, gain_vec, bias_vec):
    center = jnp.mean(values, axis=-1, keepdims=True)
    deviate = values - center
    spread = jnp.mean(deviate * deviate, axis=-1, keepdims=True)
    return deviate * lax.rsqrt(spread + 1e-05) * gain_vec + bias_vec


def sigmoid(logits):
    return 0.5 + 0.5 * jnp.tanh(0.5 * logits)


def kernel(
    rows_n, ka_n, early,
    pair_hbm, mask_hbm, ln_gain_hbm, ln_bias_hbm, w_proj_hbm, w_gate_hbm, w_out_gate_hbm,
    out_gain_hbm, out_bias_hbm, w_out_hbm,
    out_ref,
    mask_ref, ln_gain_ref, ln_bias_ref, w_proj_ref, w_gate_ref, w_out_gate_ref,
    out_gain_ref, out_bias_ref, w_out_ref,
    pair_ref, edges, wide, normed, gates, left, right, tri, back, w_cat, w_scaled, bias_row, w_tail, acc,
    mean_part, square_part,
    small_sem, load_sem, recv_left, recv_first, recv_early, recv_own, recv_down, recv_right, recv_far, recv_tri,
    send_left, send_right, send_far, send_tri,
):
    row = lax.axis_index("rows")
    col = lax.axis_index("ka")
    row_count, col_count, chans = pair_ref.shape
    hidden = w_out_hbm.shape[0]
    zone = rows_n // 4
    group_rows = 2 * zone
    members = group_rows * ka_n
    hubs = zone * ka_n
    share = hidden // hubs
    late = share - early
    chunks = row_count // CHUNK
    ahead = AHEAD
    shared = SHARED

    quarter = row // zone
    lane = row % zone
    half = quarter // 2
    spot = row % group_rows
    hub_q = 1 + half
    far_q = 2 - half
    edge_q = 3 * half
    place = half * (quarter - 2) + (1 - half) * (1 - quarter)
    inner = place == 0
    member = lane * ka_n + col
    planes = wide.reshape(2 * hidden, PITCH, col_count)

    barrier = pltpu.get_barrier_semaphore()

    def hail(to_row, to_col):
        pl.semaphore_signal(barrier, inc=1, device_id=(to_row, to_col), device_id_type=MESH)

    def greet(step, carry):
        hail(half * group_rows + (spot + step % group_rows) % group_rows, (col + step // group_rows) % ka_n)
        return carry

    def greet_far(step, carry):
        hail(far_q * zone + step % zone, (col + step // zone) % ka_n)
        return carry

    def chunk_rows(chunk):
        return pl.ds(pl.multiple_of(chunk * CHUNK, CHUNK), CHUNK)

    def load(chunk):
        rows = chunk_rows(chunk)
        return pltpu.make_async_copy(pair_hbm.at[rows], pair_ref.at[rows], load_sem.at[chunk])

    smalls = [
        pltpu.make_async_copy(there, here, small_sem.at[at])
        for at, (there, here) in enumerate([
            (w_gate_hbm, w_gate_ref), (w_proj_hbm, w_proj_ref), (ln_gain_hbm, ln_gain_ref),
            (ln_bias_hbm, ln_bias_ref), (mask_hbm, mask_ref), (w_out_gate_hbm, w_out_gate_ref),
            (out_gain_hbm, out_gain_ref), (out_bias_hbm, out_bias_ref), (w_out_hbm, w_out_ref),
        ])
    ]
    smalls[0].start()
    smalls[1].start()
    load(0).start()
    for small in smalls[2:]:
        small.start()
    for chunk in range(1, chunks):
        load(chunk).start()

    @pl.when(inner)
    def _():
        lax.fori_loop(0, hubs, greet_far, 0)

    lax.fori_loop(1, members, greet, 0)

    def turned(ref):
        return ref[...].astype(jnp.float32).T.astype(jnp.bfloat16)

    smalls[0].wait()
    smalls[1].wait()
    gate_rows, proj_rows = turned(w_gate_ref), turned(w_proj_ref)
    w_cat[:hidden, :] = gate_rows[hidden:]
    w_cat[hidden : 2 * hidden, :] = proj_rows[hidden:]
    w_cat[2 * hidden : 3 * hidden, :] = gate_rows[:hidden]
    w_cat[3 * hidden :, :] = proj_rows[:hidden]

    own_cols = pl.ds(pl.multiple_of(col * col_count, 128), col_count)

    def left_ends(chan, count, first, size, to_member):
        return (
            edges.at[pl.ds(to_member * share + chan, count), pl.ds(first, size), :],
            left.at[pl.ds(chan, count), pl.ds(spot * row_count + first, size), own_cols],
        )

    def right_ends(chan, count, first, size, to_member):
        return (
            edges.at[pl.ds(hidden + to_member * share + chan, count), pl.ds(first, size), :],
            right.at[pl.ds(chan, count), pl.ds(row * row_count + first, size), own_cols],
        )

    def send_edges(ends, chan, count, first, size, sent, landed, to_q=None):
        def start(to_lane, to_col):
            here, there = ends(chan, count, first, size, to_lane * ka_n + to_col)
            pltpu.make_async_remote_copy(
                src_ref=here, dst_ref=there, send_sem=sent, recv_sem=landed,
                device_id=((quarter if to_q is None else to_q) * zone + to_lane, to_col), device_id_type=MESH,
            ).start()

        def other(step, carry):
            start((lane + step % zone) % zone, (col + step // zone) % ka_n)
            return carry

        if to_q is not None:
            lax.fori_loop(0, hubs, other, 0)
            return
        lax.fori_loop(1, hubs, other, 0)
        here, there = ends(chan, count, first, size, member)
        pltpu.make_async_copy(here, there, landed).start()

    def make_side(at, local, plain, first_row, first_chan):
        both = lax.dot_general(
            w_cat[first_row : first_row + 2 * hidden], plain, (((1,), (1,)), ((), ())),
            preferred_element_type=jnp.float32,
        )
        mask_row = mask_ref[pl.ds(at, 1), :].astype(jnp.float32)
        made = sigmoid(both[:hidden]) * both[hidden:] * mask_row
        wide[pl.ds(local + first_chan * PITCH, hidden, stride=PITCH), :] = made

    def normalise(at):
        values = pair_ref[at].astype(jnp.float32)
        plain = layer_norm(values, ln_gain_ref[...], ln_bias_ref[...]).astype(jnp.bfloat16)
        normed[at] = plain
        return plain

    def round_side(chunk, first_chan, count):
        some = pl.ds(first_chan, count)
        edges[some, chunk_rows(chunk), :] = planes[some, :CHUNK, :].astype(jnp.bfloat16)

    def make_first():
        load(0).wait()

        def right_row(at, carry):
            make_side(at, at, normalise(at), 0, hidden)
            return carry

        lax.fori_loop(0, CHUNK, right_row, 0, unroll=CHUNK)
        round_side(0, hidden, hidden)

    def make_first_left():
        def left_row(at, carry):
            make_side(at, at, normed[at], 2 * hidden, 0)
            return carry

        lax.fori_loop(0, CHUNK, left_row, 0, unroll=MAKE_UNROLL)
        round_side(0, 0, hidden)

    def make_chunk(chunk):
        load(chunk).wait()

        def one_row(local, carry):
            at = chunk * CHUNK + local
            plain = normalise(at)
            both = lax.dot_general(
                w_cat[...], plain, (((1,), (1,)), ((), ())), preferred_element_type=jnp.float32
            )
            mask_row = mask_ref[pl.ds(at, 1), :].astype(jnp.float32)
            right_made = sigmoid(both[:hidden]) * both[hidden : 2 * hidden] * mask_row
            left_made = sigmoid(both[2 * hidden : 3 * hidden]) * both[3 * hidden :] * mask_row
            wide[pl.ds(local + hidden * PITCH, hidden, stride=PITCH), :] = right_made
            wide[pl.ds(local, hidden, stride=PITCH), :] = left_made
            return carry

        lax.fori_loop(0, CHUNK, one_row, 0, unroll=MAKE_UNROLL)
        round_side(chunk, 0, 2 * hidden)

    def send_early_right(chunk):
        first = pl.multiple_of(chunk * CHUNK, CHUNK)

        @pl.when(inner)
        def _():
            send_edges(right_ends, 0, early, first, CHUNK, send_far, recv_far.at[0], far_q)

        @pl.when((place == 1) & (chunk > 0))
        def _():
            send_edges(right_ends, 0, early, first, CHUNK, send_right, recv_first.at[0, chunk])

    def send_early_left(chunk):
        first = pl.multiple_of(chunk * CHUNK, CHUNK)

        @pl.when(place == 1)
        def _():
            send_edges(left_ends, 0, early, first, CHUNK, send_left, recv_first.at[1, chunk])

    def send_right_late(group):
        send_edges(right_ends, early + group, 1, 0, row_count, send_right, recv_right.at[0, group])

    def send_left_late(group):
        send_edges(left_ends, early + group, 1, 0, row_count, send_left, recv_left.at[0, 1 + group])

    def send_both(group, lead):
        send_right_late(group + lead)
        send_left_late(group)

    def await_part(part, landed):
        pltpu.make_async_copy(part, part, landed).wait()

    def pass_on(part, to_q, landed):
        pltpu.make_async_remote_copy(
            src_ref=part, dst_ref=part, send_sem=send_far, recv_sem=landed,
            device_id=(to_q * zone + lane, col), device_id_type=MESH,
        ).start()

    def right_rows(chan, count, first, size):
        return right.at[pl.ds(chan, count), pl.ds(pl.multiple_of(first, CHUNK), size), :]

    def left_rows(chan, count, from_q):
        first = pl.multiple_of(from_q % 2 * zone * row_count, CHUNK)
        return left.at[pl.ds(chan, count), pl.ds(first, zone * row_count), :]

    def pass_early(from_q, chunk, to_q, landed):
        for to_lane in range(zone):
            first = (from_q * zone + to_lane) * row_count + chunk * CHUNK
            pass_on(right_rows(0, early, first, CHUNK), to_q, landed)

    def pass_late(from_q, group, to_q, came, landed):
        part = right_rows(early + group, 1, from_q * zone * row_count, zone * row_count)
        await_part(part, came)
        pass_on(part, to_q, landed)

    def pass_left(chan, count, group):
        part = left_rows(chan, count, quarter)
        await_part(part, recv_left.at[0, group])
        pass_on(part, hub_q, recv_left.at[1, group])

    def climb_early(chunk):
        sizer = right_rows(0, early, 0, zone * CHUNK)

        @pl.when(chunk > 0)
        def _():
            await_part(sizer, recv_first.at[0, chunk])
            pass_early(quarter, chunk, hub_q, recv_early.at[chunk])

        await_part(sizer, recv_first.at[1, chunk])
        for to_lane in range(zone):
            first = (quarter % 2 * zone + to_lane) * row_count + chunk * CHUNK
            rows = pl.ds(pl.multiple_of(first, CHUNK), CHUNK)
            pass_on(left.at[pl.ds(shared, early - shared), rows, :], hub_q, recv_left.at[1, 0])

    def cross_early(chunk):
        await_part(right_rows(0, early, 0, zone * CHUNK), recv_early.at[chunk])
        pass_early(edge_q, chunk, far_q, recv_far.at[0])

    def cross_near(group):
        pass_late(hub_q, group, far_q, recv_right.at[0, group], recv_far.at[1 + group])

    def cross_edge(group):
        pass_late(edge_q, group, far_q, recv_right.at[1, group], recv_far.at[1 + group + group // (late - 1)])

    def climb_right(group):
        pass_late(edge_q, group, hub_q, recv_right.at[0, group], recv_right.at[1, group])

    def climb_left(group):
        pass_left(early + group, 1, 1 + group)

    def climb(group, carry):
        climb_right(group)
        climb_left(group - 1)
        return carry

    far_first = (1 - half) * group_rows * row_count
    own_first = pl.multiple_of(quarter % 2 * zone * row_count, CHUNK)

    j_block = zone * row_count
    col_block = ka_n // 4

    def multiply(chan, count, first, size, j_first, j_size):
        j_rows = pl.ds(pl.multiple_of(j_first, 128), j_size)

        def one_channel(at, carry):
            tri[at, pl.ds(first, size), j_rows] = lax.dot_general(
                left[at, pl.ds(first, size), :], right[at, j_rows, :], (((1,), (1,)), ((), ())),
                preferred_element_type=jnp.float32,
            ).astype(jnp.bfloat16)
            return carry

        lax.fori_loop(chan, chan + count, one_channel, 0)

    def give_all(chan, count, base, spots, me, col_first, col_size, landed):
        slot = back.at[pl.ds(member * share + chan, count)]

        def part(to_spot, to_col):
            first = (base - half * group_rows + to_spot) * row_count
            return tri.at[
                pl.ds(chan, count),
                pl.ds(pl.multiple_of(first, CHUNK), row_count),
                pl.ds(pl.multiple_of(to_col * col_count, 128), col_count),
            ]

        def give(step, carry):
            to_spot = (me + step % spots) % spots
            to_col = col_first + (col + step // spots) % col_size
            pltpu.make_async_remote_copy(
                src_ref=part(to_spot, to_col), dst_ref=slot, send_sem=send_tri, recv_sem=landed,
                device_id=(base + to_spot, to_col), device_id_type=MESH,
            ).start()
            return carry

        mine = (col >= col_first) & (col < col_first + col_size)

        @pl.when(mine)
        def _():
            pltpu.make_async_copy(part(me, col), slot, landed).start()

        @pl.when(jnp.logical_not(mine))
        def _():
            give(0, 0)

        lax.fori_loop(1, spots * col_size, give, 0)

    def block(chan, count, from_q, quarters, landed):
        multiply(chan, count, 0, group_rows * row_count, from_q * j_block, quarters * j_block)
        give_all(
            chan, count, half * group_rows, group_rows, spot, from_q * col_block, quarters * col_block, landed
        )

    def near_block(chan, count, group, landed):
        await_part(left_rows(chan, count, hub_q), recv_left.at[0, group])
        await_part(left_rows(chan, count, edge_q), recv_left.at[1, group])
        block(chan, count, 2 * half, 2, landed)

    def far_block(chan, count, group, landed):
        await_part(right_rows(chan, count, far_first, group_rows * row_count), recv_far.at[group])
        block(chan, count, 2 * (1 - half), 2, landed)

    def far_part(where, chan, count, group, landed):
        from_q = far_q if where == 0 else 3 * (1 - half)
        part = right_rows(chan, count, from_q * zone * row_count, zone * row_count)
        await_part(part, recv_far.at[group])
        block(chan, count, from_q, 1, landed)

    def own_triangle():
        multiply(0, shared, own_first, zone * row_count, 0, rows_n * row_count)
        give_all(0, shared, quarter * zone, zone, lane, 0, ka_n, recv_tri.at[0])

    known = hidden - hubs

    def gather_stats():
        await_part(back.at[pl.ds(0, known)], recv_tri.at[0])

        def one_chunk(chunk, carry):
            rows = chunk_rows(chunk)
            some = [
                back[at * share : at * share + share - 1, rows, :].astype(jnp.float32) for at in range(hubs)
            ]
            center = sum(jnp.sum(sums, axis=0) for sums in some) / known
            mean_part[rows, :] = center
            square_part[rows, :] = sum(
                jnp.sum((sums - center) * (sums - center), axis=0) for sums in some
            )
            return carry

        lax.fori_loop(0, chunks, one_chunk, 0)

    for small in smalls[2:5]:
        small.wait()
    make_first()
    pl.semaphore_wait(barrier, members - 1 + hubs * (1 - place))

    @pl.when(place == 1)
    def _():
        send_edges(right_ends, 0, early, 0, CHUNK, send_far, recv_early.at[0], hub_q)
        send_edges(right_ends, 0, shared, 0, CHUNK, send_right, recv_first.at[0, 0])

    send_early_right(0)
    for small in smalls[5:]:
        small.wait()
    make_first_left()
    send_early_left(0)

    def rest(chunk, carry):
        make_chunk(chunk)
        send_early_right(chunk)
        send_early_left(chunk)

        @pl.when(place == 1)
        def _():
            climb_early(chunk - 1)

        return carry

    lax.fori_loop(1, chunks, rest, 0)

    @pl.when(place == 1)
    def _():
        send_right_late(0)
        send_both(0, 1)
        send_both(1, 1)
        climb_early(chunks - 1)
        send_both(2, 1)
        climb_right(0)
        send_both(3, 1)
        climb(1, 0)

        def both(group, carry):
            send_both(group, 1)
            return carry

        lax.fori_loop(4, late - 1, both, 0)
        send_left_late(late - 1)
        climb(2, 0)

    @pl.when(inner)
    def _():
        for group in range(ahead):
            send_right_late(group)
        send_edges(right_ends, 0, early, 0, row_count, send_right, recv_own)
        send_edges(left_ends, 0, early, 0, row_count, send_left, recv_left.at[0, 0])
        for chunk in range(chunks):
            cross_early(chunk)

            def both(group, carry):
                send_both(group, ahead)
                return carry

            span = late - ahead
            lax.fori_loop(span * chunk // chunks, span * (chunk + 1) // chunks, both, 0)
            if chunk < ahead:
                cross_near(chunk)
        for group in range(late - ahead, late):
            send_left_late(group)
        own_rows = hub_q * zone * row_count
        await_part(right_rows(0, early, own_rows, zone * row_count), recv_own)
        pass_on(right_rows(0, shared, own_rows, zone * row_count), edge_q, recv_down)

    weights = w_out_ref[...].astype(jnp.float32)
    gain_col = jnp.broadcast_to(out_gain_ref[...], (chans, hidden)).T
    bias_col = jnp.broadcast_to(out_bias_ref[...], (chans, hidden)).T
    w_scaled[...] = (weights * gain_col).astype(jnp.bfloat16)
    bias_row[...] = jnp.sum(weights * bias_col, axis=0, keepdims=True)

    def parts_of(values):
        high = values.astype(jnp.bfloat16).astype(jnp.float32)
        middle = (values - high).astype(jnp.bfloat16).astype(jnp.float32)
        return high, middle, values - high - middle

    rounded = w_scaled[...].astype(jnp.float32)
    high, middle, low = parts_of(-jnp.sum(rounded, axis=0, keepdims=True))
    none, one = jnp.zeros_like(high), jnp.ones_like(high)
    late_rows = [rounded[at * share + share - 1 : at * share + share] for at in range(hubs)]
    rows_plain = late_rows + [high, middle, low, high, middle, high, none, none]
    rows_scale = [none] * (hubs + 6) + [one, one]
    w_tail[...] = jnp.concatenate(
        [jnp.concatenate(rows_plain, axis=0), jnp.concatenate(rows_scale, axis=0)], axis=1
    ).astype(jnp.bfloat16)

    def gate_row(at, carry):
        gates[at] = sigmoid(
            jnp.dot(normed[at], w_out_gate_ref[...], preferred_element_type=jnp.float32)
        )
        return carry

    lax.fori_loop(0, row_count, gate_row, 0, unroll=GATE_UNROLL)

    @pl.when(place == 1)
    def _():
        lax.fori_loop(3, late, climb, 0)
        climb_left(late - 1)
        await_part(right_rows(0, shared, 0, zone * CHUNK), recv_first.at[0, 0])
        await_part(right_rows(0, shared, 0, 3 * zone * row_count), recv_down)
        own_triangle()

    @pl.when(inner)
    def _():
        for group in range(min(chunks, ahead), ahead + 1):
            cross_near(group)
        cross_edge(0)
        await_part(left_rows(0, early, hub_q), recv_left.at[0, 0])
        await_part(left_rows(shared, early - shared, edge_q), recv_left.at[1, 0])
        await_part(right_rows(0, early, far_first, group_rows * row_count), recv_far.at[0])
        pass_on(right_rows(0, shared, far_first, group_rows * row_count), edge_q, recv_down)
        own_triangle()
        block(shared, early - shared, 0, 4, recv_tri.at[0])

        def near_upto(group):
            return ahead + 1 + (late - ahead - 1) * group // (late - 1)

        def near_one(group, carry):
            cross_near(group)
            return carry

        def stage(group, carry):
            lax.fori_loop(near_upto(group - 1), near_upto(group), near_one, 0)
            cross_edge(group)
            near_block(early + group - 1, 1, group, recv_tri.at[0])
            far_block(early + group - 1, 1, group, recv_tri.at[0])
            return carry

        lax.fori_loop(1, late, stage, 0)
        near_block(share - 1, 1, late, recv_tri.at[1])
        far_part(0, share - 1, 1, late, recv_tri.at[1])
        gather_stats()
        far_part(1, share - 1, 1, late + 1, recv_tri.at[1])

    @pl.when(place == 1)
    def _():
        gather_stats()

    def lay_known(chunk, base):
        for at in range(hubs):
            first, size = at * share, share - 1
            planes[base + first : base + first + size, :CHUNK, :] = (
                back[first : first + size, chunk_rows(chunk), :].astype(jnp.float32)
            )
            planes[base + first + size, :CHUNK, :] = jnp.zeros((CHUNK, col_count), jnp.float32)

    def project_known(chunk, base):
        def one_row(local, carry):
            sums = wide[pl.ds(local + base * PITCH, hidden, stride=PITCH), :].astype(jnp.bfloat16)
            acc[chunk * CHUNK + local] = lax.dot_general(
                sums, w_scaled[...], (((0,), (0,)), ((), ())), preferred_element_type=jnp.float32
            )
            return carry

        lax.fori_loop(0, CHUNK, one_row, 0, unroll=FINISH_UNROLL)

    def lay_last(chunk, base):
        rows = chunk_rows(chunk)
        last = [back[at * share + share - 1, rows, :].astype(jnp.float32) for at in range(hubs)]
        part = mean_part[rows, :]
        center = (part * known + sum(last)) / hidden
        moved = part - center
        squares = square_part[rows, :] + known * moved * moved
        squares = squares + sum((sums - center) * (sums - center) for sums in last)
        high, middle, low = parts_of(center)
        scale, scale_rest, _ = parts_of(lax.rsqrt(squares / hidden + 1e-05))
        stack = last + [high, high, high, middle, middle, low, scale, scale_rest]
        for at, plane in enumerate(stack):
            planes[base + at, :CHUNK, :] = plane

    def project_last(chunk, base):
        def one_row(local, carry):
            at = chunk * CHUNK + local
            stack = wide[pl.ds(local + base * PITCH, hubs + 8, stride=PITCH), :].astype(jnp.bfloat16)
            tail = lax.dot_general(
                stack, w_tail[...], (((0,), (0,)), ((), ())), preferred_element_type=jnp.float32
            )
            projected = (acc[at] + tail[:, :chans]) * tail[:, chans:] + bias_row[...]
            out_ref[at] = (gates[at] * projected).astype(jnp.bfloat16)
            return carry

        lax.fori_loop(0, CHUNK, one_row, 0, unroll=FINISH_UNROLL)

    def in_turns(lay, project):
        lay(0, 0)
        for chunk in range(chunks):
            if chunk + 1 < chunks:
                lay(chunk + 1, (chunk + 1) % 2 * hidden)
            project(chunk, chunk % 2 * hidden)

    in_turns(lay_known, project_known)
    await_part(back.at[pl.ds(0, hubs)], recv_tri.at[1])
    in_turns(lay_last, project_last)

    def sent_all(first, count, rows, sem):
        part = edges.at[pl.ds(0, count), pl.ds(first, rows), :]
        await_part(part, sem)

    sent_all(0, (hubs - 1) * share, row_count, send_left)
    sent_all(0, (hubs - 1) * late, row_count, send_right)
    sent_all(CHUNK, (hubs - 1) * early, row_count - CHUNK, send_right)

    @pl.when(place == 1)
    def _():
        sent_all(0, (hubs - 1) * shared, CHUNK, send_right)

    @pl.when(inner)
    def _():
        sent_all(0, (hubs - 1) * early, CHUNK, send_right)

    def given_all(count, spots):
        if spots > 1:
            await_part(tri.at[pl.ds(0, count), pl.ds(0, (spots - 1) * row_count), :], send_tri)
        await_part(tri.at[pl.ds(0, count), pl.ds(0, row_count), pl.ds(0, (ka_n - 1) * col_count)], send_tri)

    plane = zone * row_count
    await_part(right.at[:, pl.ds(0, plane), :], send_far)
    await_part(right.at[pl.ds(0, share - shared), pl.ds(0, plane), :], send_far)
    given_all(shared, zone)

    @pl.when(inner)
    def _():
        await_part(right.at[pl.ds(0, shared), pl.ds(0, 2 * plane), :], send_far)
        await_part(right.at[pl.ds(0, shared), pl.ds(0, 2 * plane), :], send_far)
        given_all(share - shared, group_rows)


def fused(rows_n, ka_n, args):
    pair_repr, pair_mask, ln_gain, ln_bias, w_proj, w_gate, w_out_gate, out_gain, out_bias, w_out = args
    row_count, col_count, chans = pair_repr.shape
    hidden = w_out.shape[0]
    share = hidden // (rows_n // 4 * ka_n)
    late = share - EARLY
    chunks = row_count // CHUNK
    half = jnp.bfloat16
    return pl.pallas_call(
        functools.partial(kernel, rows_n, ka_n, EARLY),
        out_shape=jax.ShapeDtypeStruct(pair_repr.shape, half),
        in_specs=[pl.BlockSpec(memory_space=pltpu.HBM)] * 10,
        out_specs=pl.BlockSpec(memory_space=pltpu.VMEM),
        scratch_shapes=[
            pltpu.VMEM((row_count, col_count), jnp.int32),
            pltpu.VMEM((1, chans), jnp.float32),
            pltpu.VMEM((1, chans), jnp.float32),
            pltpu.VMEM((chans, 2 * hidden), half),
            pltpu.VMEM((chans, 2 * hidden), half),
            pltpu.VMEM((chans, chans), half),
            pltpu.VMEM((1, hidden), jnp.float32),
            pltpu.VMEM((1, hidden), jnp.float32),
            pltpu.VMEM((hidden, chans), half),
            pltpu.VMEM((row_count, col_count, chans), half),
            pltpu.VMEM((2 * hidden, row_count, col_count), half),
            pltpu.VMEM((2 * hidden * PITCH, col_count), jnp.float32),
            pltpu.VMEM((row_count, col_count, chans), half),
            pltpu.VMEM((row_count, col_count, chans), jnp.float32),
            pltpu.VMEM((share, rows_n // 2 * row_count, ka_n * col_count), half),
            pltpu.VMEM((share, rows_n * row_count, ka_n * col_count), half),
            pltpu.VMEM((share, rows_n // 2 * row_count, ka_n * col_count), half),
            pltpu.VMEM((hidden, row_count, col_count), half),
            pltpu.VMEM((4 * hidden, chans), half),
            pltpu.VMEM((hidden, chans), half),
            pltpu.VMEM((1, chans), jnp.float32),
            pltpu.VMEM((hidden // share + 8, 2 * chans), half),
            pltpu.VMEM((row_count, col_count, chans), jnp.float32),
            pltpu.VMEM((row_count, col_count), jnp.float32),
            pltpu.VMEM((row_count, col_count), jnp.float32),
            pltpu.SemaphoreType.DMA((9,)),
            pltpu.SemaphoreType.DMA((chunks,)),
            pltpu.SemaphoreType.DMA((2, 1 + late)),
            pltpu.SemaphoreType.DMA((2, chunks)),
            pltpu.SemaphoreType.DMA((chunks,)),
            pltpu.SemaphoreType.DMA,
            pltpu.SemaphoreType.DMA,
            pltpu.SemaphoreType.DMA((2, late)),
            pltpu.SemaphoreType.DMA((2 + late,)),
            pltpu.SemaphoreType.DMA((2,)),
            pltpu.SemaphoreType.DMA,
            pltpu.SemaphoreType.DMA,
            pltpu.SemaphoreType.DMA,
            pltpu.SemaphoreType.DMA,
        ],
        compiler_params=pltpu.CompilerParams(
            collective_id=0, has_side_effects=True, vmem_limit_bytes=42 * 2**20
        ),
    )(*[
        pltpu.with_memory_space_constraint(array, pltpu.HBM)
        for array in (
            pair_repr, pair_mask, ln_gain[None], ln_bias[None], w_proj, w_gate, w_out_gate,
            out_gain[None], out_bias[None], w_out,
        )
    ])


def plain(args):
    pair_repr, pair_mask, ln_gain, ln_bias, w_proj, w_gate, w_out_gate, out_gain, out_bias, w_out = args
    row_count, col_count, chans = pair_repr.shape
    hidden = w_out.shape[0]
    normed = layer_norm(pair_repr.astype(jnp.float32), ln_gain, ln_bias).astype(jnp.bfloat16)
    flat_rows = normed.reshape(row_count * col_count, chans)
    projected = jnp.dot(flat_rows, w_proj, preferred_element_type=jnp.float32)
    gate_logits = jnp.dot(flat_rows, w_gate, preferred_element_type=jnp.float32)
    mask_col = pair_mask.reshape(row_count * col_count, 1).astype(jnp.float32)
    edges = (jax.nn.sigmoid(gate_logits) * projected * mask_col).astype(jnp.bfloat16)
    edges = edges.reshape(row_count, col_count, 2 * hidden)
    partial_sums = jnp.einsum(
        "ikh,jkh->ijh",
        edges[:, :, :hidden],
        lax.all_gather(edges[:, :, hidden:], "rows", axis=0, tiled=True),
        preferred_element_type=jnp.float32,
    )
    triangle = lax.psum_scatter(
        partial_sums.astype(jnp.bfloat16), "ka", scatter_dimension=1, tiled=True
    ).astype(jnp.float32)
    tri_normed = layer_norm(triangle, out_gain, out_bias).astype(jnp.bfloat16)
    out_gate = jax.nn.sigmoid(jnp.dot(flat_rows, w_out_gate, preferred_element_type=jnp.float32))
    projected_out = jnp.dot(
        tri_normed.reshape(row_count * col_count, hidden), w_out, preferred_element_type=jnp.float32
    )
    return (out_gate * projected_out).astype(jnp.bfloat16).reshape(row_count, col_count, chans)


def body(rows_n, ka_n, *args):
    row_count, col_count, chans = args[0].shape
    hidden = args[-1].shape[0]
    hubs = rows_n // 4 * ka_n
    aligned = row_count % CHUNK == 0 and col_count % 128 == 0 and chans % 128 == 0 and hidden % 128 == 0
    if aligned and rows_n % 4 == 0 and ka_n % 4 == 0 and hidden % hubs == 0 and col_count == hidden:
        if hidden // hubs - EARLY > max(AHEAD, 5) and row_count > CHUNK:
            return fused(rows_n, ka_n, args)
    return plain(args)


def solution(mesh):
    placed = (P("rows", "ka", None), P("rows", "ka"), P(), P(), P(), P(), P(), P(), P(), P())
    return jax.shard_map(
        functools.partial(body, mesh.shape["rows"], mesh.shape["ka"]),
        mesh=mesh, in_specs=placed, out_specs=P("rows", "ka", None), check_vma=False,
    )
```
